256 devices in a mesh: slab: 32 (over z, y), energy: 8 (over x, core).
Axes of the slice: x: 4, y: 4, z: 8, core: 2. Of those that a mesh axis runs over, the one named last changes fastest.
Arguments:
- green: bfloat16 [8, 32, 3, 2, 384, 384], P('energy', 'slab'), may hold values from -0.3125 to 0.3125
- sigma: bfloat16 [8, 32, 3, 2, 384, 384], P('energy', 'slab'), may hold values from -4 to 4
- phonon: bfloat16 [8, 32, 2, 384, 384], P('energy', 'slab'), may hold values from -4 to 4
- pair_off: int32 [32, 3], replicated, may hold values from -2 to 2, as said below
- pair_count: int32 [32], replicated, may hold values from 1 to 3, as said below
- pair_range: int32 [32, 3], replicated, may hold values from 96 to 384, as said below
Outputs:
- lesser: float32 [8, 32, 2, 384, 384], P('energy', 'slab')
The draws below stay inside these ranges and needn't reach their ends.
Inputs may be any that keep to these rules, and one draw needn't show every extreme that they name: The partner slab k + pair_off[k, q] lies inside the grid. `pair_count`: some slab has 3 live slots. `pair_range`: a multiple of 96; some pair couples all 384 orbitals.
All inputs are finite; a program needn't handle non-finite values.
Results may differ from the reference program's by a relative error of at most 0.0035.
Values may be sent and summed in bfloat16 or wider, within the bound.
A program may use at most 64 MiB of HBM per device.

```python
import jax
import jax.numpy as jnp
from jax import lax

ORB = 384
MAXP = 3
NSLAB = 32
EN = 8


def draw_pair_off(key, part):
    shifts = jax.random.randint(key, (NSLAB, MAXP), -2, 3).astype(jnp.int32)
    slab_ids = jnp.arange(NSLAB, dtype=jnp.int32)[:, None]
    partner = slab_ids + shifts
    outside = (partner < 0) | (partner >= NSLAB)
    return jnp.where(outside, -shifts, shifts).astype(jnp.int32)


def draw_pair_count(key, part):
    counts = jax.random.randint(jax.random.fold_in(key, 11), (NSLAB,), 1, MAXP + 1).astype(jnp.int32)
    fullest = jax.random.randint(jax.random.fold_in(key, 12), (), 0, NSLAB)
    return counts.at[fullest].set(MAXP).astype(jnp.int32)


def draw_pair_range(key, part):
    quarters = jax.random.randint(jax.random.fold_in(key, 21), (NSLAB, MAXP), 1, 5).astype(jnp.int32)
    widest = jax.random.randint(jax.random.fold_in(key, 22), (), 0, NSLAB)
    quarters = quarters.at[widest, 0].set(4)
    return (quarters * (ORB // 4)).astype(jnp.int32)


def block_levels(own_key, dims, split, low, largest):
    loudness = 1.0
    for dim, parts in split:
        heights = jax.random.uniform(jax.random.fold_in(jax.random.fold_in(own_key, 6), dim), (parts,), jnp.float32, low / len(split), largest / len(split))
        loudness = loudness * jnp.repeat(jnp.exp(heights), dims[dim] // parts).reshape((-1,) + (1,) * (len(dims) - 1 - dim))
    return loudness


def bell_draw(own_key, shape, spread, most, pieces=(), kind=jnp.bfloat16):
    entries = jax.random.normal(own_key, shape, jnp.float32) * spread
    if len(pieces) > 0:
        entries = block_levels(own_key, shape, pieces, -0.22, 0.18) * entries
    return jnp.clip(entries, min=-most, max=most).astype(kind)


def setup_inputs(seed: int = 0) -> dict:
    keys = jax.random.split(jax.random.key(seed), 7)
    green = bell_draw(keys[0], (EN, NSLAB, 3, 2, ORB, ORB), ORB ** -0.5, 0.3125, ((0, 8), (1, 32)))
    sigma = bell_draw(keys[1], (EN, NSLAB, MAXP, 2, ORB, ORB), 0.3, 4.0, ((0, 8), (1, 32)))
    phonon = bell_draw(keys[2], (EN, NSLAB, 2, ORB, ORB), 0.3, 4.0, ((0, 8), (1, 32)))
    pair_off = draw_pair_off(jax.random.fold_in(keys[6], 71), 0)
    pair_count = draw_pair_count(jax.random.fold_in(keys[6], 71), 0)
    pair_range = draw_pair_range(jax.random.fold_in(keys[6], 71), 0)
    return {"green": green, "sigma": sigma, "phonon": phonon, "pair_off": pair_off, "pair_count": pair_count, "pair_range": pair_range}


def conj_sum(source, chosen):
    real = jnp.einsum('qmn,qpn->mp', source[:, 0], chosen[:, 0]) + jnp.einsum('qmn,qpn->mp', source[:, 1], chosen[:, 1])
    imag = jnp.einsum('qmn,qpn->mp', source[:, 1], chosen[:, 0]) - jnp.einsum('qmn,qpn->mp', source[:, 0], chosen[:, 1])
    return real, imag


def complex_times(left, real, imag):
    first = jnp.dot(left[0], real, preferred_element_type=jnp.float32) - jnp.dot(left[1], imag, preferred_element_type=jnp.float32)
    second = jnp.dot(left[0], imag, preferred_element_type=jnp.float32) + jnp.dot(left[1], real, preferred_element_type=jnp.float32)
    return jnp.stack([first, second])


def reference(green, sigma, phonon, pair_off, pair_count, pair_range):
    slab_total = green.shape[1]
    width = green.shape[-1]
    slots = pair_off.shape[1]
    positions = jnp.arange(width, dtype=jnp.int32)
    inside = positions[None, None, :] < pair_range[:, :, None]
    square = inside[:, :, :, None] & inside[:, :, None, :]
    masked = jnp.where(square[None, :, :, None], sigma, jnp.zeros((), jnp.bfloat16))
    padded = jnp.pad(phonon.astype(jnp.float32), ((1, 1), (0, 0), (0, 0), (0, 0), (0, 0)))
    phonon_mix = (0.5 * (padded[:-2] + padded[2:])).astype(jnp.bfloat16)
    sources = jnp.concatenate([masked, phonon_mix[:, :, None]], axis=2)
    slot_ids = jnp.arange(slots, dtype=jnp.int32)

    def one_row(flat):
        energy = flat // slab_total
        slab = flat % slab_total
        green_row = green[energy, slab]
        running = jnp.zeros((2, width, width), jnp.float32)
        for delta in (-1, 0, 1):
            other = (slab + delta).astype(jnp.int32)
            clipped = jnp.clip(other, 0, slab_total - 1).astype(jnp.int32)
            valid = (other >= 0) & (other < slab_total)
            source = sources[energy, clipped].astype(jnp.float32)
            offsets = pair_off[clipped]
            count = pair_count[clipped]
            place = (clipped + offsets - slab + 1).astype(jnp.int32)
            usable = (place >= 0) & (place <= 2) & (slot_ids < count)
            pick = jnp.concatenate([jnp.clip(place, 0, 2).astype(jnp.int32), jnp.array([delta + 1], jnp.int32)])
            keep = jnp.concatenate([usable, jnp.array([True])]).astype(jnp.float32)
            chosen = green_row[pick].astype(jnp.float32) * keep[:, None, None, None]
            real, imag = conj_sum(source, chosen)
            term = complex_times(green_row[delta + 1], real.astype(jnp.bfloat16), imag.astype(jnp.bfloat16))
            running = running + jnp.where(valid, term, jnp.zeros_like(term))
        return running

    flat_ids = jnp.arange(green.shape[0] * slab_total, dtype=jnp.int32)
    result = lax.map(one_row, flat_ids)
    return result.reshape(green.shape[0], slab_total, 2, width, width)
```

```python
import functools

import jax
import jax.numpy as jnp
from jax import lax
from jax.experimental import pallas as pl
from jax.experimental.pallas import tpu as pltpu
from jax.sharding import PartitionSpec as P

MESH = pl.DeviceIdType.MESH
F32 = jnp.float32
BF16 = jnp.bfloat16
TILE = 16
CHUNK = 128


def kernel(
    slabs,
    energies,
    off_ref,
    count_ref,
    range_ref,
    green_hbm,
    sigma_hbm,
    phonon_hbm,
    out_hbm,
    green_v,
    sigma_v,
    phonon_v,
    near_v,
    mine_v,
    left_v,
    right_v,
    b_v,
    a_v,
    y_v,
    part_v,
    acc_v,
    out_v,
    local_sem,
    near_send,
    near_recv,
    send_sem,
    recv_sem,
    out_sem,
):
    k = lax.axis_index("slab")
    e = lax.axis_index("energy")
    width = green_v.shape[-1]
    slots = sigma_v.shape[0]
    chunks = width // CHUNK
    has_left, has_right = k > 0, k < slabs - 1
    has_low, has_high = e > 0, e < energies - 1

    load_phonon = pltpu.make_async_copy(phonon_hbm.at[0, 0], phonon_v, local_sem.at[0])
    load_sigma = pltpu.make_async_copy(sigma_hbm.at[0, 0], sigma_v, local_sem.at[1])
    load_green = pltpu.make_async_copy(green_hbm.at[0, 0], green_v, local_sem.at[2])
    load_phonon.start()
    load_sigma.start()
    load_green.start()

    barrier = pltpu.get_barrier_semaphore()
    sides = (
        (has_left, {"slab": k - 1}),
        (has_right, {"slab": k + 1}),
        (has_low, {"energy": e - 1}),
        (has_high, {"energy": e + 1}),
    )
    for there, who in sides:

        @pl.when(there)
        def _():
            pl.semaphore_signal(barrier, inc=1, device_id=who, device_id_type=MESH)

    peers = 4 - sum((k == end).astype(jnp.int32) for end in (0, slabs - 1))
    peers = peers - sum((e == end).astype(jnp.int32) for end in (0, energies - 1))
    pl.semaphore_wait(barrier, peers)

    def near_copy(slot, target):
        return pltpu.make_async_remote_copy(
            src_ref=phonon_v,
            dst_ref=near_v.at[slot],
            send_sem=near_send.at[slot],
            recv_sem=near_recv.at[slot],
            device_id={"energy": target},
            device_id_type=MESH,
        )

    up, down = near_copy(0, e + 1), near_copy(1, e - 1)
    load_phonon.wait()

    @pl.when(has_high)
    def _():
        up.start()

    @pl.when(has_low)
    def _():
        down.start()

    def pieces(way):
        into = (left_v, right_v)[way]
        target = (k + 1, k - 1)[way]
        plan = [(2 * way, 0, 0, width), (2 * way + 1, 1, 0, width)]
        plan += [(4, 2, c * CHUNK, CHUNK) for c in range(chunks)]
        made = []
        for n, (source, slot, row, rows) in enumerate(plan):
            made.append(
                pltpu.make_async_remote_copy(
                    src_ref=mine_v.at[source, pl.ds(row, rows)],
                    dst_ref=into.at[slot, pl.ds(row, rows)],
                    send_sem=send_sem.at[way, n],
                    recv_sem=recv_sem.at[way, n],
                    device_id={"slab": target},
                    device_id_type=MESH,
                )
            )
        return made

    to_right, to_left = pieces(0), pieces(1)

    def combine(place, offset, with_phonon):
        reach = []
        for q in range(slots):
            live = (q < count_ref[k]) & (off_ref[k, q] == offset)
            reach.append(jnp.where(live, range_ref[k, q], 0))

        def step(t, carry):
            rows = pl.ds(pl.multiple_of(t * TILE, TILE), TILE)
            row_ids = t * TILE + lax.broadcasted_iota(jnp.int32, (TILE, width), 0)
            col_ids = lax.broadcasted_iota(jnp.int32, (TILE, width), 1)
            far = jnp.maximum(row_ids, col_ids)
            for part in range(2):
                if with_phonon:
                    low = near_v[0, part, rows, :].astype(F32)
                    high = near_v[1, part, rows, :].astype(F32)
                    total = (0.5 * (low + high)).astype(BF16).astype(F32)
                else:
                    total = jnp.zeros((TILE, width), F32)
                for q in range(slots):
                    term = sigma_v[q, part, rows, :].astype(F32)
                    total = total + jnp.where(far < reach[q], term, 0.0)
                mine_v[place, rows, part * width : (part + 1) * width] = total.astype(BF16)
            return carry

        lax.fori_loop(0, width // TILE, step, 0)

    def start(there, copies):
        @pl.when(there)
        def _():
            for copy in copies:
                copy.start()

    load_sigma.wait()
    combine(0, 1, False)
    start(has_right, to_right[:1])
    combine(2, -1, False)
    start(has_left, to_left[:1])
    combine(1, 2, False)
    start(has_right, to_right[1:2])
    combine(3, -2, False)
    start(has_left, to_left[1:2])

    for there, buffer in ((has_left, left_v), (has_right, right_v)):

        @pl.when(jnp.logical_not(there))
        def _():
            buffer[...] = jnp.zeros_like(buffer)

    for there, slot in ((has_low, 0), (has_high, 1)):

        @pl.when(jnp.logical_not(there))
        def _():
            near_v[slot] = jnp.zeros_like(near_v[slot])

    load_green.wait()
    for place in range(3):
        for part in range(2):
            turned = green_v[place, part].astype(F32).T
            for again in range(2):
                row = (part + again) % 2
                sign = -1.0 if (part == 1 and row == 0) else 1.0
                b_v[place, row * width : (row + 1) * width, again * width : (again + 1) * width] = (
                    sign * turned
                ).astype(BF16)
    for c in range(chunks):
        for n, place in enumerate((1, 0, 2)):
            for part in range(2):
                at = n * 2 * CHUNK + part * CHUNK
                a_v[c, :, at : at + CHUNK] = green_v[place, part, :, c * CHUNK : (c + 1) * CHUNK]

    @pl.when(has_low)
    def _():
        up.wait_recv()

    @pl.when(has_high)
    def _():
        down.wait_recv()

    combine(4, 0, True)
    start(has_right, to_right[2:])
    start(has_left, to_left[2:])

    def dot(a, b):
        return jnp.dot(a, b, preferred_element_type=F32)

    def put(at, x):
        real = x[:, :width].astype(BF16)
        imag = x[:, width:].astype(BF16)
        y_v[at : at + CHUNK, :width] = real
        y_v[at : at + CHUNK, width:] = imag
        y_v[at + CHUNK : at + 2 * CHUNK, :width] = -imag
        y_v[at + CHUNK : at + 2 * CHUNK, width:] = real

    for c in range(chunks):
        rows = slice(c * CHUNK, (c + 1) * CHUNK)
        x = dot(mine_v[2, rows], b_v[0]) + dot(mine_v[4, rows], b_v[1]) + dot(mine_v[0, rows], b_v[2])
        put(0, x)
        term = dot(a_v[c, :, : 2 * CHUNK], y_v[: 2 * CHUNK])
        acc_v[...] = term if c == 0 else acc_v[...] + term

    def arrived(there, copy):
        @pl.when(there)
        def _():
            copy.wait_recv()

    def blocks(way, slot, place):
        buffer = (left_v, right_v)[way]

        def step(c, carry):
            rows = pl.ds(pl.multiple_of(c * CHUNK, CHUNK), CHUNK)
            term = dot(buffer[slot, rows], b_v[place])
            part_v[way, rows] = term if slot == 0 else part_v[way, rows] + term
            return carry

        lax.fori_loop(0, chunks, step, 0)

    arrived(has_left, to_right[0])
    blocks(0, 0, 1)
    arrived(has_right, to_left[0])
    blocks(1, 0, 1)
    arrived(has_left, to_right[1])
    blocks(0, 1, 2)
    arrived(has_right, to_left[1])
    blocks(1, 1, 0)
    writes = []
    for c in range(chunks):
        rows = slice(c * CHUNK, (c + 1) * CHUNK)
        arrived(has_left, to_right[2 + c])
        put(0, part_v[0, rows] + dot(left_v[2, rows], b_v[0]))
        arrived(has_right, to_left[2 + c])
        put(2 * CHUNK, part_v[1, rows] + dot(right_v[2, rows], b_v[2]))
        if c < chunks - 1:
            acc_v[...] = acc_v[...] + dot(a_v[c, :, 2 * CHUNK :], y_v[...])
        else:
            for m in range(chunks):
                these = slice(m * CHUNK, (m + 1) * CHUNK)
                total = acc_v[these] + dot(a_v[c, these, 2 * CHUNK :], y_v[...])
                for part in range(2):
                    out_v[part, these] = total[:, part * width : (part + 1) * width]
                    write = pltpu.make_async_copy(
                        out_v.at[part, these], out_hbm.at[0, 0, part, these], out_sem.at[m, part]
                    )
                    write.start()
                    writes.append(write)

    @pl.when(has_high)
    def _():
        up.wait_send()

    @pl.when(has_low)
    def _():
        down.wait_send()

    for there, copies in ((has_right, to_right), (has_left, to_left)):

        @pl.when(there)
        def _():
            for copy in copies:
                copy.wait_send()

    for write in writes:
        write.wait()


def solution(mesh):
    slabs, energies = mesh.shape["slab"], mesh.shape["energy"]

    def body(green, sigma, phonon, pair_off, pair_count, pair_range):
        width = green.shape[-1]
        slots = sigma.shape[2]
        chunks = width // CHUNK
        smem = pl.BlockSpec(memory_space=pltpu.SMEM)
        hbm = pl.BlockSpec(memory_space=pl.ANY)
        block = (width, 2 * width)
        return pl.pallas_call(
            functools.partial(kernel, slabs, energies),
            out_shape=jax.ShapeDtypeStruct((1, 1, 2, width, width), F32),
            in_specs=[smem, smem, smem, hbm, hbm, hbm],
            out_specs=hbm,
            scratch_shapes=[
                pltpu.VMEM((3, 2, width, width), BF16),
                pltpu.VMEM((slots, 2, width, width), BF16),
                pltpu.VMEM((2, width, width), BF16),
                pltpu.VMEM((2, 2, width, width), BF16),
                pltpu.VMEM((5,) + block, BF16),
                pltpu.VMEM((3,) + block, BF16),
                pltpu.VMEM((3,) + block, BF16),
                pltpu.VMEM((3, 2 * width, 2 * width), BF16),
                pltpu.VMEM((chunks, width, 6 * CHUNK), BF16),
                pltpu.VMEM((4 * CHUNK, 2 * width), BF16),
                pltpu.VMEM((2,) + block, F32),
                pltpu.VMEM(block, F32),
                pltpu.VMEM((2, width, width), F32),
                pltpu.SemaphoreType.DMA((3,)),
                pltpu.SemaphoreType.DMA((2,)),
                pltpu.SemaphoreType.DMA((2,)),
                pltpu.SemaphoreType.DMA((2, 2 + chunks)),
                pltpu.SemaphoreType.DMA((2, 2 + chunks)),
                pltpu.SemaphoreType.DMA((chunks, 2)),
            ],
            compiler_params=pltpu.CompilerParams(
                collective_id=0, has_side_effects=True, vmem_limit_bytes=48 * 1024 * 1024
            ),
            name="lesser",
        )(pair_off, pair_count, pair_range, green, sigma, phonon)

    wide = P("energy", "slab", None, None, None, None)
    slim = P("energy", "slab", None, None, None)
    return jax.shard_map(
        body,
        mesh=mesh,
        in_specs=(wide, wide, slim, P(), P(), P()),
        out_specs=slim,
        check_vma=False,
    )
```

```python
import functools

import jax
import jax.numpy as jnp
from jax import lax
from jax.experimental import pallas as pl
from jax.experimental.pallas import tpu as pltpu
from jax.sharding import PartitionSpec as P

MESH = pl.DeviceIdType.MESH
F32 = jnp.float32
BF16 = jnp.bfloat16
TILE = 16
CHUNK = 128


def kernel(
    slabs,
    energies,
    off_hbm,
    count_hbm,
    range_hbm,
    green_hbm,
    sigma_hbm,
    phonon_hbm,
    out_ref,
    off_ref,
    count_ref,
    range_ref,
    green_v,
    sigma_v,
    phonon_v,
    near_v,
    mine_v,
    left_v,
    right_v,
    b_v,
    a_v,
    y_v,
    part_v,
    acc_v,
    local_sem,
    near_send,
    near_recv,
    send_sem,
    recv_sem,
):
    k = lax.axis_index("slab")
    e = lax.axis_index("energy")
    width = green_v.shape[-1]
    slots = sigma_v.shape[0]
    chunks = width // CHUNK
    has_left, has_right = k > 0, k < slabs - 1
    has_low, has_high = e > 0, e < energies - 1

    tables = [
        pltpu.make_async_copy(source, held, local_sem.at[3 + n])
        for n, (source, held) in enumerate(
            ((off_hbm, off_ref), (count_hbm, count_ref), (range_hbm, range_ref))
        )
    ]
    for table in tables:
        table.start()
    load_phonon = pltpu.make_async_copy(phonon_hbm.at[0, 0], phonon_v, local_sem.at[0])
    load_sigma = pltpu.make_async_copy(sigma_hbm.at[0, 0], sigma_v, local_sem.at[1])
    load_green = pltpu.make_async_copy(green_hbm.at[0, 0], green_v, local_sem.at[2])
    load_phonon.start()
    load_sigma.start()
    load_green.start()

    barrier = pltpu.get_barrier_semaphore()
    sides = (
        (has_left, {"slab": k - 1}),
        (has_right, {"slab": k + 1}),
        (has_low, {"energy": e - 1}),
        (has_high, {"energy": e + 1}),
    )
    for there, who in sides:

        @pl.when(there)
        def _():
            pl.semaphore_signal(barrier, inc=1, device_id=who, device_id_type=MESH)

    peers = 4 - sum((k == end).astype(jnp.int32) for end in (0, slabs - 1))
    peers = peers - sum((e == end).astype(jnp.int32) for end in (0, energies - 1))
    pl.semaphore_wait(barrier, peers)

    def near_copy(slot, target):
        return pltpu.make_async_remote_copy(
            src_ref=phonon_v,
            dst_ref=near_v.at[slot],
            send_sem=near_send.at[slot],
            recv_sem=near_recv.at[slot],
            device_id={"energy": target},
            device_id_type=MESH,
        )

    up, down = near_copy(0, e + 1), near_copy(1, e - 1)
    load_phonon.wait()

    @pl.when(has_high)
    def _():
        up.start()

    @pl.when(has_low)
    def _():
        down.start()

    def pieces(way):
        into = (left_v, right_v)[way]
        target = (k + 1, k - 1)[way]
        plan = [(2 * way, 0, 0, width), (2 * way + 1, 1, 0, width)]
        plan += [(4, 2, c * CHUNK, CHUNK) for c in range(chunks)]
        made = []
        for n, (source, slot, row, rows) in enumerate(plan):
            made.append(
                pltpu.make_async_remote_copy(
                    src_ref=mine_v.at[source, pl.ds(row, rows)],
                    dst_ref=into.at[slot, pl.ds(row, rows)],
                    send_sem=send_sem.at[way, n],
                    recv_sem=recv_sem.at[way, n],
                    device_id={"slab": target},
                    device_id_type=MESH,
                )
            )
        return made

    to_right, to_left = pieces(0), pieces(1)

    def combine(place, offset, with_phonon):
        reach = []
        for q in range(slots):
            live = (q < count_ref[k]) & (off_ref[q, k] == offset)
            reach.append(jnp.where(live, range_ref[q, k], 0))

        def step(t, carry):
            rows = pl.ds(pl.multiple_of(t * TILE, TILE), TILE)
            row_ids = t * TILE + lax.broadcasted_iota(jnp.int32, (TILE, width), 0)
            col_ids = lax.broadcasted_iota(jnp.int32, (TILE, width), 1)
            far = jnp.maximum(row_ids, col_ids)
            for part in range(2):
                if with_phonon:
                    low = near_v[0, part, rows, :].astype(F32)
                    high = near_v[1, part, rows, :].astype(F32)
                    total = (0.5 * (low + high)).astype(BF16).astype(F32)
                else:
                    total = jnp.zeros((TILE, width), F32)
                for q in range(slots):
                    term = sigma_v[q, part, rows, :].astype(F32)
                    total = total + jnp.where(far < reach[q], term, 0.0)
                mine_v[place, rows, part * width : (part + 1) * width] = total.astype(BF16)
            return carry

        lax.fori_loop(0, width // TILE, step, 0)

    def start(there, copies):
        @pl.when(there)
        def _():
            for copy in copies:
                copy.start()

    for table in tables:
        table.wait()
    load_sigma.wait()
    combine(0, 1, False)
    start(has_right, to_right[:1])
    combine(2, -1, False)
    start(has_left, to_left[:1])
    combine(1, 2, False)
    start(has_right, to_right[1:2])
    combine(3, -2, False)
    start(has_left, to_left[1:2])

    for there, buffer in ((has_left, left_v), (has_right, right_v)):

        @pl.when(jnp.logical_not(there))
        def _():
            buffer[...] = jnp.zeros_like(buffer)

    for there, slot in ((has_low, 0), (has_high, 1)):

        @pl.when(jnp.logical_not(there))
        def _():
            near_v[slot] = jnp.zeros_like(near_v[slot])

    load_green.wait()
    for place in range(3):
        for part in range(2):
            turned = green_v[place, part].astype(F32).T
            for again in range(2):
                row = (part + again) % 2
                sign = -1.0 if (part == 1 and row == 0) else 1.0
                b_v[place, row * width : (row + 1) * width, again * width : (again + 1) * width] = (
                    sign * turned
                ).astype(BF16)
    for c in range(chunks):
        for n, place in enumerate((1, 0, 2)):
            for part in range(2):
                at = n * 2 * CHUNK + part * CHUNK
                a_v[c, :, at : at + CHUNK] = green_v[place, part, :, c * CHUNK : (c + 1) * CHUNK]

    @pl.when(has_low)
    def _():
        up.wait_recv()

    @pl.when(has_high)
    def _():
        down.wait_recv()

    combine(4, 0, True)
    start(has_right, to_right[2:])
    start(has_left, to_left[2:])

    def dot(a, b):
        return jnp.dot(a, b, preferred_element_type=F32)

    def put(at, x):
        real = x[:, :width].astype(BF16)
        imag = x[:, width:].astype(BF16)
        y_v[at : at + CHUNK, :width] = real
        y_v[at : at + CHUNK, width:] = imag
        y_v[at + CHUNK : at + 2 * CHUNK, :width] = -imag
        y_v[at + CHUNK : at + 2 * CHUNK, width:] = real

    for c in range(chunks):
        rows = slice(c * CHUNK, (c + 1) * CHUNK)
        x = dot(mine_v[2, rows], b_v[0]) + dot(mine_v[4, rows], b_v[1]) + dot(mine_v[0, rows], b_v[2])
        put(0, x)
        term = dot(a_v[c, :, : 2 * CHUNK], y_v[: 2 * CHUNK])
        acc_v[...] = term if c == 0 else acc_v[...] + term

    def arrived(there, copy):
        @pl.when(there)
        def _():
            copy.wait_recv()

    def blocks(way, slot, place):
        buffer = (left_v, right_v)[way]

        def step(c, carry):
            rows = pl.ds(pl.multiple_of(c * CHUNK, CHUNK), CHUNK)
            term = dot(buffer[slot, rows], b_v[place])
            part_v[way, rows] = term if slot == 0 else part_v[way, rows] + term
            return carry

        lax.fori_loop(0, chunks, step, 0)

    arrived(has_left, to_right[0])
    blocks(0, 0, 1)
    arrived(has_right, to_left[0])
    blocks(1, 0, 1)
    arrived(has_left, to_right[1])
    blocks(0, 1, 2)
    arrived(has_right, to_left[1])
    blocks(1, 1, 0)
    for c in range(chunks):
        rows = slice(c * CHUNK, (c + 1) * CHUNK)
        arrived(has_left, to_right[2 + c])
        put(0, part_v[0, rows] + dot(left_v[2, rows], b_v[0]))
        arrived(has_right, to_left[2 + c])
        put(2 * CHUNK, part_v[1, rows] + dot(right_v[2, rows], b_v[2]))
        if c < chunks - 1:
            acc_v[...] = acc_v[...] + dot(a_v[c, :, 2 * CHUNK :], y_v[...])
        else:
            for m in range(chunks):
                these = slice(m * CHUNK, (m + 1) * CHUNK)
                total = acc_v[these] + dot(a_v[c, these, 2 * CHUNK :], y_v[...])
                for part in range(2):
                    out_ref[0, 0, part, these] = total[:, part * width : (part + 1) * width]

    @pl.when(has_high)
    def _():
        up.wait_send()

    @pl.when(has_low)
    def _():
        down.wait_send()

    for there, copies in ((has_right, to_right), (has_left, to_left)):

        @pl.when(there)
        def _():
            for copy in copies:
                copy.wait_send()


def solution(mesh):
    slabs, energies = mesh.shape["slab"], mesh.shape["energy"]

    def body(green, sigma, phonon, pair_off, pair_count, pair_range):
        width = green.shape[-1]
        slots = sigma.shape[2]
        chunks = width // CHUNK
        hbm = pl.BlockSpec(memory_space=pltpu.HBM)
        block = (width, 2 * width)
        operands = (pair_off.T, pair_count, pair_range.T, green, sigma, phonon)
        operands = [pltpu.with_memory_space_constraint(v, pltpu.HBM) for v in operands]
        return pl.pallas_call(
            functools.partial(kernel, slabs, energies),
            out_shape=jax.ShapeDtypeStruct((1, 1, 2, width, width), F32),
            in_specs=[hbm] * 6,
            out_specs=pl.BlockSpec(memory_space=pltpu.VMEM),
            scratch_shapes=[
                pltpu.SMEM((slots, slabs), jnp.int32),
                pltpu.SMEM((slabs,), jnp.int32),
                pltpu.SMEM((slots, slabs), jnp.int32),
                pltpu.VMEM((3, 2, width, width), BF16),
                pltpu.VMEM((slots, 2, width, width), BF16),
                pltpu.VMEM((2, width, width), BF16),
                pltpu.VMEM((2, 2, width, width), BF16),
                pltpu.VMEM((5,) + block, BF16),
                pltpu.VMEM((3,) + block, BF16),
                pltpu.VMEM((3,) + block, BF16),
                pltpu.VMEM((3, 2 * width, 2 * width), BF16),
                pltpu.VMEM((chunks, width, 6 * CHUNK), BF16),
                pltpu.VMEM((4 * CHUNK, 2 * width), BF16),
                pltpu.VMEM((2,) + block, F32),
                pltpu.VMEM(block, F32),
                pltpu.SemaphoreType.DMA((6,)),
                pltpu.SemaphoreType.DMA((2,)),
                pltpu.SemaphoreType.DMA((2,)),
                pltpu.SemaphoreType.DMA((2, 2 + chunks)),
                pltpu.SemaphoreType.DMA((2, 2 + chunks)),
            ],
            compiler_params=pltpu.CompilerParams(
                collective_id=0, has_side_effects=True, vmem_limit_bytes=48 * 1024 * 1024
            ),
            name="lesser",
        )(*operands)

    wide = P("energy", "slab", None, None, None, None)
    slim = P("energy", "slab", None, None, None)
    return jax.shard_map(
        body,
        mesh=mesh,
        in_specs=(wide, wide, slim, P(), P(), P()),
        out_specs=slim,
        check_vma=False,
    )
```

```python
import functools

import jax
import jax.numpy as jnp
from jax import lax
from jax.experimental import pallas as pl
from jax.experimental.pallas import tpu as pltpu
from jax.sharding import PartitionSpec as P

MESH = pl.DeviceIdType.MESH
F32 = jnp.float32
BF16 = jnp.bfloat16
TILE = 16
CHUNK = 128
UNIT = 96
GROUP = 6
LIST = 24
DIRECT = 18
HOP = 4
OFFSETS = (1, 2, -1, -2)


def extent(reach):
    steps = [(reach >= n * UNIT).astype(jnp.int32) for n in range(1, 5)]
    down = steps[0] + steps[1] + steps[2] + steps[3]
    across = steps[0] + steps[1] + steps[2]
    return down, across, down * across


def crowded_kernel(off_ref, count_ref, range_ref, out_ref):
    off, reach = off_ref[...], range_ref[...]
    slots, slabs = off.shape
    live = lax.broadcasted_iota(jnp.int32, off.shape, 0) < count_ref[...]
    place = lax.broadcasted_iota(jnp.int32, (1, slabs), 1) % HOP
    crowded = jnp.zeros((1, slabs), F32)
    for way in range(2):
        filled = jnp.zeros((1, slabs), jnp.int32)
        for offset in OFFSETS[2 * way : 2 * way + 2]:
            widest = jnp.max(jnp.where(live & (off == offset), reach, 0), axis=0, keepdims=True)
            filled = filled + extent(widest)[2]
        above = jnp.concatenate([filled[:, HOP:], filled[:, :HOP]], axis=1)
        below = jnp.concatenate([filled[:, -HOP:], filled[:, :-HOP]], axis=1)
        relay = jnp.where(place == HOP - 1, above, below) if way == 0 else jnp.where(place == 0, below, above)
        crowded = crowded + ((filled > DIRECT) & (relay > LIST - 2 * GROUP)).astype(F32)
    out_ref[0] = jnp.max(crowded).astype(jnp.int32)


def kernel(
    slabs,
    energies,
    around,
    off_hbm,
    count_hbm,
    range_hbm,
    green_hbm,
    sigma_hbm,
    phonon_hbm,
    out_ref,
    off_ref,
    count_ref,
    range_ref,
    green_v,
    sigma_v,
    near_v,
    mine_v,
    own_v,
    list_v,
    from_left_v,
    from_right_v,
    spill_v,
    cent_v,
    block_v,
    b_v,
    a_v,
    y_v,
    part_v,
    acc_v,
    local_sem,
    near_send,
    near_recv,
    unit_send,
    unit_recv,
    spill_send,
    spill_recv,
    back_send,
    back_recv,
    cent_send,
    cent_recv,
):
    k = lax.axis_index("slab")
    e = lax.axis_index("energy")
    width = green_v.shape[-1]
    slots = sigma_v.shape[0]
    chunks = width // CHUNK
    has_low, has_high = e > 0, e < energies - 1

    def ring(slab):
        return lax.rem(slab + slabs, slabs)

    next_k, last_k = ring(k + 1), ring(k - 1)

    tables = [
        pltpu.make_async_copy(source, held, local_sem.at[n])
        for n, (source, held) in enumerate(
            ((off_hbm, off_ref), (count_hbm, count_ref), (range_hbm, range_ref))
        )
    ]
    load_sigma = pltpu.make_async_copy(sigma_hbm.at[0, 0], sigma_v, local_sem.at[3])
    load_green = pltpu.make_async_copy(green_hbm.at[0, 0], green_v, local_sem.at[4])
    for table in tables:
        table.start()
    load_sigma.start()

    barrier = pltpu.get_barrier_semaphore()
    always = [next_k, last_k] + ([ring(k + HOP), ring(k - HOP)] if around else [])
    for slab in always:
        pl.semaphore_signal(barrier, inc=1, device_id={"slab": slab}, device_id_type=MESH)
    for there, energy in ((has_low, e - 1), (has_high, e + 1)):

        @pl.when(there)
        def _():
            pl.semaphore_signal(barrier, inc=1, device_id={"energy": energy}, device_id_type=MESH)

    peers = len(always) + 2 - sum((e == end).astype(jnp.int32) for end in (0, energies - 1))
    pl.semaphore_wait(barrier, peers)

    def near_copy(slot, target):
        return pltpu.make_async_remote_copy(
            src_ref=phonon_hbm.at[0, 0],
            dst_ref=near_v.at[slot],
            send_sem=near_send.at[slot],
            recv_sem=near_recv.at[slot],
            device_id={"energy": target},
            device_id_type=MESH,
        )

    up, down = near_copy(0, e + 1), near_copy(1, e - 1)

    @pl.when(has_high)
    def _():
        up.start()

    @pl.when(has_low)
    def _():
        down.start()

    def remote(source, target, sent, received, slab):
        return pltpu.make_async_remote_copy(
            src_ref=source,
            dst_ref=target,
            send_sem=sent,
            recv_sem=received,
            device_id={"slab": slab},
            device_id_type=MESH,
        )

    place = lax.rem(k, HOP)
    turn = (jnp.where(place == HOP - 1, HOP, -HOP), jnp.where(place == 0, -HOP, HOP))
    back = (jnp.where(place == 0, -HOP, HOP), jnp.where(place == HOP - 1, HOP, -HOP))
    beside = (next_k, last_k)
    got_v = (from_left_v, from_right_v)
    groups = (DIRECT if around else LIST) // GROUP
    direct, spill, returned, centre = [], [], [], []
    pieces = [(slice(None), c * CHUNK) for c in range(chunks - 1)]
    pieces += [(slice(c, c + 1), width - CHUNK) for c in range(chunks)]
    for way in range(2):
        direct.append([])
        for g in range(groups):
            units = slice(g * GROUP, (g + 1) * GROUP)
            direct[way].append(
                remote(
                    list_v.at[way, units],
                    got_v[way].at[units],
                    unit_send.at[way, g],
                    unit_recv.at[way, g],
                    beside[way],
                )
            )
        spill.append(
            remote(
                list_v.at[way, DIRECT:LIST],
                spill_v.at[way],
                spill_send.at[way],
                spill_recv.at[way],
                ring(k + turn[way]),
            )
        )
        returned.append(
            remote(
                got_v[way].at[DIRECT - GROUP : DIRECT],
                got_v[way].at[DIRECT:LIST],
                back_send.at[way],
                back_recv.at[way],
                ring(k + back[way]),
            )
        )
        centre.append([])
        for n, (these, row) in enumerate(pieces):
            centre[way].append(
                remote(
                    own_v.at[these, row : row + CHUNK],
                    cent_v.at[way, these, row : row + CHUNK],
                    cent_send.at[way, n],
                    cent_recv.at[way, n],
                    beside[way],
                )
            )

    def live_reach(slab, q, offset):
        live = (q < count_ref[slab]) & (off_ref[q, slab] == offset)
        return jnp.where(live, range_ref[q, slab], 0)

    def combine(wanted, with_phonon):
        reach = [[live_reach(k, q, offset) for q in range(slots)] for _, offset in wanted]

        def step(t, carry):
            rows = pl.ds(pl.multiple_of(t * TILE, TILE), TILE)
            row_ids = t * TILE + lax.broadcasted_iota(jnp.int32, (TILE, width), 0)
            col_ids = lax.broadcasted_iota(jnp.int32, (TILE, width), 1)
            far = jnp.maximum(row_ids, col_ids)
            m = lax.div(t, UNIT // TILE)
            unit_rows = pl.ds(pl.multiple_of(t * TILE - m * UNIT, TILE), TILE)
            for part in range(2):
                terms = [sigma_v[q, part, rows, :].astype(F32) for q in range(slots)]
                for n, (at, _) in enumerate(wanted):
                    kept = [jnp.where(far < reach[n][q], terms[q], 0.0) for q in range(slots)]
                    total = functools.reduce(jnp.add, kept)
                    if with_phonon:
                        low = near_v[0, part, rows, :].astype(F32)
                        high = near_v[1, part, rows, :].astype(F32)
                        total = total + (0.5 * (low + high)).astype(BF16).astype(F32)
                    total = total.astype(BF16)
                    lanes = slice(part * CHUNK, (part + 1) * CHUNK)
                    for c in range(chunks):
                        value = total[:, c * CHUNK : (c + 1) * CHUNK]
                        if with_phonon:
                            own_v[c, rows, lanes] = value
                        else:
                            mine_v[at, m, c, unit_rows, lanes] = value
            return carry

        lax.fori_loop(0, width // TILE, step, 0)

    def layout(slab, way):
        blocks = []
        for offset in OFFSETS[2 * way : 2 * way + 2]:
            reach = functools.reduce(jnp.maximum, [live_reach(slab, q, offset) for q in range(slots)])
            blocks.append(extent(reach))
        return blocks

    def pack(way, first, last):
        (_, across_a, size_a), (_, across_b, size_b) = layout(k, way)

        def step(p, carry):
            in_a = p < size_a
            unit = jnp.where(in_a, p, jnp.maximum(p - size_a, 0))
            across = jnp.where(in_a, across_a, across_b)
            row = jnp.where(across == 3, lax.div(unit, 3), jnp.where(across == 2, lax.div(unit, 2), unit))
            col = jnp.clip(unit - row * across, 0, chunks - 1)
            row = jnp.clip(row, 0, width // UNIT - 1)
            at = 2 * way + jnp.where(in_a, 0, 1)
            keep = jnp.where(p < size_a + size_b, 1.0, 0.0).astype(BF16)
            list_v[way, p] = mine_v[at, row, col] * keep
            return carry

        lax.fori_loop(first, last, step, 0)

    for table in tables:
        table.wait()
    load_sigma.wait()
    load_green.start()
    held_back = groups - 1 if around else groups
    for way in range(2):
        combine([(2 * way + n, OFFSETS[2 * way + n]) for n in range(2)], False)
        if around:
            pack(way, DIRECT, LIST)
            spill[way].start()
            pack(way, 0, DIRECT)
        else:
            pack(way, 0, LIST)
        for copy in direct[way][:held_back]:
            copy.start()

    for there, slot in ((has_low, 0), (has_high, 1)):

        @pl.when(jnp.logical_not(there))
        def _():
            near_v[slot] = jnp.zeros_like(near_v[slot])

    @pl.when(has_low)
    def _():
        up.wait_recv()

    @pl.when(has_high)
    def _():
        down.wait_recv()

    combine([(4, 0)], True)
    if around:
        for way in range(2):
            spill[way].wait_recv()
            for j in range(GROUP):
                p = DIRECT - GROUP + j
                list_v[way, p] = list_v[way, p] + spill_v[way, j]
        for way in range(2):
            direct[way][-1].start()
    for way in range(2):
        for copy in centre[way]:
            copy.start()

    load_green.wait()
    for at in range(3):
        for part in range(2):
            turned = green_v[at, part].astype(F32).T
            plain = turned.astype(BF16)
            minus = (-turned).astype(BF16)
            for c in range(chunks):
                source = slice(c * CHUNK, (c + 1) * CHUNK)
                real = slice(2 * c * CHUNK, (2 * c + 1) * CHUNK)
                imag = slice((2 * c + 1) * CHUNK, (2 * c + 2) * CHUNK)
                if part == 0:
                    b_v[at, real, :width] = plain[source]
                    b_v[at, imag, width:] = plain[source]
                else:
                    b_v[at, real, width:] = minus[source]
                    b_v[at, imag, :width] = plain[source]
    inside = (None, k > 0, k < slabs - 1)
    for c in range(chunks):
        for n, at in enumerate((1, 0, 2)):
            for part in range(2):
                to = n * 2 * CHUNK + part * CHUNK
                value = green_v[at, part, :, c * CHUNK : (c + 1) * CHUNK]
                if inside[n] is not None:
                    value = jnp.where(inside[n], value, jnp.zeros_like(value))
                a_v[c, :, to : to + CHUNK] = value

    def dot(a, b):
        return jnp.dot(a, b, preferred_element_type=F32)

    def b_chunk(at, c):
        return b_v[at, 2 * c * CHUNK : 2 * (c + 1) * CHUNK]

    def put(at, x):
        real = x[:, :width].astype(BF16)
        imag = x[:, width:].astype(BF16)
        y_v[at : at + CHUNK, :width] = real
        y_v[at : at + CHUNK, width:] = imag
        y_v[at + CHUNK : at + 2 * CHUNK, :width] = -imag
        y_v[at + CHUNK : at + 2 * CHUNK, width:] = real

    for n, (at, partner) in enumerate(((2, 0), (0, 2))):
        for r in range(2):
            rows = slice(r * width // 2, (r + 1) * width // 2)
            units = slice(rows.start // UNIT, rows.stop // UNIT)
            x = None
            for c in range(chunks):
                term = dot(mine_v[at, units, c].reshape(width // 2, 2 * CHUNK), b_chunk(partner, c))
                x = term if x is None else x + term
            part_v[0, rows] = x if n == 0 else part_v[0, rows] + x
    for r in range(chunks):
        rows = slice(r * CHUNK, (r + 1) * CHUNK)
        x = part_v[0, rows]
        for c in range(chunks):
            x = x + dot(own_v[c, rows], b_chunk(1, c))
        put(0, x)
        term = dot(a_v[r, :, : 2 * CHUNK], y_v[: 2 * CHUNK])
        acc_v[...] = term if r == 0 else acc_v[...] + term

    if around:
        for way in range(2):
            direct[way][-1].wait_recv()
            returned[way].start()

    for way in range(2):
        for copy in direct[way][:held_back]:
            copy.wait_recv()
        if around:
            returned[way].wait_recv()
        start = 0
        blocks = layout((last_k, next_k)[way], way)
        for n, (down_n, across_n, size_n) in enumerate(blocks):
            for m in range(width // UNIT):
                for c in range(chunks):
                    position = jnp.clip(start + m * across_n + c, 0, LIST - 1)
                    keep = jnp.where((m < down_n) & (c < across_n), 1.0, 0.0).astype(BF16)
                    block_v[c, m * UNIT : (m + 1) * UNIT] = got_v[way][position] * keep
            start = start + size_n
            partner = ((1, 2), (1, 0))[way][n]
            for r in range(chunks):
                rows = slice(r * CHUNK, (r + 1) * CHUNK)
                x = None
                for c in range(chunks):
                    term = dot(block_v[c, rows], b_chunk(partner, c))
                    x = term if x is None else x + term
                part_v[way, rows] = x if n == 0 else part_v[way, rows] + x

    for n, (these, row) in enumerate(pieces):
        rows = slice(row, row + CHUNK)
        final = n == len(pieces) - 1
        for way in range(2):
            centre[way][n].wait_recv()
            partner = (0, 2)[way]
            x = part_v[way, rows]
            for c in range(chunks)[these]:
                x = x + dot(cent_v[way, c, rows], b_chunk(partner, c))
            if n < chunks - 1 or final:
                put(2 * CHUNK * way, x)
            else:
                part_v[way, rows] = x
        if n < chunks - 1:
            acc_v[...] = acc_v[...] + dot(a_v[n, :, 2 * CHUNK :], y_v[...])
    for m in range(chunks):
        rows = slice(m * CHUNK, (m + 1) * CHUNK)
        total = acc_v[rows] + dot(a_v[chunks - 1, rows, 2 * CHUNK :], y_v[...])
        for part in range(2):
            out_ref[0, 0, part, rows] = total[:, part * width : (part + 1) * width]

    @pl.when(has_high)
    def _():
        up.wait_send()

    @pl.when(has_low)
    def _():
        down.wait_send()

    for way in range(2):
        for copy in direct[way] + centre[way] + ([spill[way], returned[way]] if around else []):
            copy.wait_send()


def solution(mesh):
    slabs, energies = mesh.shape["slab"], mesh.shape["energy"]

    def body(green, sigma, phonon, pair_off, pair_count, pair_range):
        width = green.shape[-1]
        slots = sigma.shape[2]
        chunks = width // CHUNK
        hbm = pl.BlockSpec(memory_space=pltpu.HBM)
        vmem = pl.BlockSpec(memory_space=pltpu.VMEM)
        split = (chunks, width, 2 * CHUNK)
        unit = (UNIT, 2 * CHUNK)
        operands = (pair_off.T, pair_count, pair_range.T, green, sigma, phonon)
        operands = [pltpu.with_memory_space_constraint(v, pltpu.HBM) for v in operands]

        def call(around, *operands):
            return pl.pallas_call(
                functools.partial(kernel, slabs, energies, around),
                out_shape=jax.ShapeDtypeStruct((1, 1, 2, width, width), F32),
                in_specs=[hbm] * 6,
                out_specs=vmem,
                scratch_shapes=[
                    pltpu.SMEM((slots, slabs), jnp.int32),
                    pltpu.SMEM((slabs,), jnp.int32),
                    pltpu.SMEM((slots, slabs), jnp.int32),
                    pltpu.VMEM((3, 2, width, width), BF16),
                    pltpu.VMEM((slots, 2, width, width), BF16),
                    pltpu.VMEM((2, 2, width, width), BF16),
                    pltpu.VMEM((4, width // UNIT, chunks) + unit, BF16),
                    pltpu.VMEM(split, BF16),
                    pltpu.VMEM((2, LIST) + unit, BF16),
                    pltpu.VMEM((LIST,) + unit, BF16),
                    pltpu.VMEM((LIST,) + unit, BF16),
                    pltpu.VMEM((2, GROUP) + unit, BF16),
                    pltpu.VMEM((2,) + split, BF16),
                    pltpu.VMEM(split, BF16),
                    pltpu.VMEM((3, 2 * width, 2 * width), BF16),
                    pltpu.VMEM((chunks, width, 6 * CHUNK), BF16),
                    pltpu.VMEM((4 * CHUNK, 2 * width), BF16),
                    pltpu.VMEM((2, width, 2 * width), F32),
                    pltpu.VMEM((width, 2 * width), F32),
                    pltpu.SemaphoreType.DMA((5,)),
                    pltpu.SemaphoreType.DMA((2,)),
                    pltpu.SemaphoreType.DMA((2,)),
                    pltpu.SemaphoreType.DMA((2, LIST // GROUP)),
                    pltpu.SemaphoreType.DMA((2, LIST // GROUP)),
                    pltpu.SemaphoreType.DMA((2,)),
                    pltpu.SemaphoreType.DMA((2,)),
                    pltpu.SemaphoreType.DMA((2,)),
                    pltpu.SemaphoreType.DMA((2,)),
                    pltpu.SemaphoreType.DMA((2, 2 * chunks - 1)),
                    pltpu.SemaphoreType.DMA((2, 2 * chunks - 1)),
                ],
                compiler_params=pltpu.CompilerParams(
                    collective_id=int(around), has_side_effects=True, vmem_limit_bytes=48 * 1024 * 1024
                ),
                name="around" if around else "straight",
            )(*operands)

        crowded = pl.pallas_call(
            crowded_kernel,
            out_shape=jax.ShapeDtypeStruct((1,), jnp.int32),
            in_specs=[vmem] * 3,
            out_specs=pl.BlockSpec(memory_space=pltpu.SMEM),
            name="crowded",
        )(pair_off.T, pair_count[None], pair_range.T)
        return lax.cond(
            crowded[0] > 0, functools.partial(call, False), functools.partial(call, True), *operands
        )

    wide = P("energy", "slab", None, None, None, None)
    slim = P("energy", "slab", None, None, None)
    return jax.shard_map(
        body,
        mesh=mesh,
        in_specs=(wide, wide, slim, P(), P(), P()),
        out_specs=slim,
        check_vma=False,
    )
```

```python
import functools

import jax
import jax.numpy as jnp
from jax import lax
from jax.experimental import pallas as pl
from jax.experimental.pallas import tpu as pltpu
from jax.sharding import PartitionSpec as P

MESH = pl.DeviceIdType.MESH
F32 = jnp.float32
BF16 = jnp.bfloat16
TILE = 16
CHUNK = 128
UNIT = 96
GROUP = 6
LIST = 24
DIRECT = 18
HOP = 4
OFFSETS = (1, 2, -1, -2)


def extent(reach):
    steps = [(reach >= n * UNIT).astype(jnp.int32) for n in range(1, 5)]
    down = steps[0] + steps[1] + steps[2] + steps[3]
    across = steps[0] + steps[1] + steps[2]
    return down, across, down * across


def crowded_kernel(off_ref, count_ref, range_ref, out_ref):
    off, reach = off_ref[...], range_ref[...]
    slots, slabs = off.shape
    live = lax.broadcasted_iota(jnp.int32, off.shape, 0) < count_ref[...]
    place = lax.broadcasted_iota(jnp.int32, (1, slabs), 1) % HOP
    crowded = jnp.zeros((1, slabs), F32)
    for way in range(2):
        filled = jnp.zeros((1, slabs), jnp.int32)
        for offset in OFFSETS[2 * way : 2 * way + 2]:
            widest = jnp.max(jnp.where(live & (off == offset), reach, 0), axis=0, keepdims=True)
            filled = filled + extent(widest)[2]
        above = jnp.concatenate([filled[:, HOP:], filled[:, :HOP]], axis=1)
        below = jnp.concatenate([filled[:, -HOP:], filled[:, :-HOP]], axis=1)
        relay = jnp.where(place == HOP - 1, below, above) if way == 0 else jnp.where(place == 0, above, below)
        crowded = crowded + ((filled > DIRECT) & (relay > LIST - 2 * GROUP)).astype(F32)
    out_ref[0] = jnp.max(crowded).astype(jnp.int32)


def kernel(
    slabs,
    energies,
    around,
    off_hbm,
    count_hbm,
    range_hbm,
    green_hbm,
    sigma_hbm,
    phonon_hbm,
    out_ref,
    off_ref,
    count_ref,
    range_ref,
    green_v,
    sigma_v,
    near_v,
    mine_v,
    own_v,
    list_v,
    from_left_v,
    from_right_v,
    spill_v,
    cent_v,
    block_v,
    b_v,
    a_v,
    y_v,
    part_v,
    acc_v,
    local_sem,
    near_send,
    near_recv,
    unit_send,
    unit_recv,
    spill_send,
    spill_recv,
    back_send,
    back_recv,
    cent_send,
    cent_recv,
):
    k = lax.axis_index("slab")
    e = lax.axis_index("energy")
    width = green_v.shape[-1]
    slots = sigma_v.shape[0]
    chunks = width // CHUNK
    has_low, has_high = e > 0, e < energies - 1

    def ring(slab):
        return lax.rem(slab + slabs, slabs)

    next_k, last_k = ring(k + 1), ring(k - 1)

    tables = [
        pltpu.make_async_copy(source, held, local_sem.at[n])
        for n, (source, held) in enumerate(
            ((off_hbm, off_ref), (count_hbm, count_ref), (range_hbm, range_ref))
        )
    ]
    load_sigma = pltpu.make_async_copy(sigma_hbm.at[0, 0], sigma_v, local_sem.at[3])
    load_green = pltpu.make_async_copy(green_hbm.at[0, 0], green_v, local_sem.at[4])
    for table in tables:
        table.start()
    load_sigma.start()

    barrier = pltpu.get_barrier_semaphore()
    always = [next_k, last_k] + ([ring(k + HOP), ring(k - HOP)] if around else [])
    for slab in always:
        pl.semaphore_signal(barrier, inc=1, device_id={"slab": slab}, device_id_type=MESH)
    for there, energy in ((has_low, e - 1), (has_high, e + 1)):

        @pl.when(there)
        def _():
            pl.semaphore_signal(barrier, inc=1, device_id={"energy": energy}, device_id_type=MESH)

    peers = len(always) + 2 - sum((e == end).astype(jnp.int32) for end in (0, energies - 1))
    pl.semaphore_wait(barrier, peers)

    def near_copy(slot, target):
        return pltpu.make_async_remote_copy(
            src_ref=phonon_hbm.at[0, 0],
            dst_ref=near_v.at[slot],
            send_sem=near_send.at[slot],
            recv_sem=near_recv.at[slot],
            device_id={"energy": target},
            device_id_type=MESH,
        )

    up, down = near_copy(0, e + 1), near_copy(1, e - 1)

    @pl.when(has_high)
    def _():
        up.start()

    @pl.when(has_low)
    def _():
        down.start()

    def remote(source, target, sent, received, slab):
        return pltpu.make_async_remote_copy(
            src_ref=source,
            dst_ref=target,
            send_sem=sent,
            recv_sem=received,
            device_id={"slab": slab},
            device_id_type=MESH,
        )

    place = lax.rem(k, HOP)
    turn = (jnp.where(place == HOP - 1, -HOP, HOP), jnp.where(place == 0, HOP, -HOP))
    back = (jnp.where(place == 0, HOP, -HOP), jnp.where(place == HOP - 1, -HOP, HOP))
    beside = (next_k, last_k)
    got_v = (from_left_v, from_right_v)
    groups = (DIRECT if around else LIST) // GROUP
    direct, spill, returned, centre = [], [], [], []
    pieces = [(slice(None), c * CHUNK) for c in range(chunks - 1)]
    pieces += [(slice(c, c + 1), width - CHUNK) for c in range(chunks)]
    for way in range(2):
        direct.append([])
        for g in range(groups):
            units = slice(g * GROUP, (g + 1) * GROUP)
            direct[way].append(
                remote(
                    list_v.at[way, units],
                    got_v[way].at[units],
                    unit_send.at[way, g],
                    unit_recv.at[way, g],
                    beside[way],
                )
            )
        spill.append(
            remote(
                list_v.at[way, DIRECT:LIST],
                spill_v.at[way],
                spill_send.at[way],
                spill_recv.at[way],
                ring(k + turn[way]),
            )
        )
        returned.append(
            remote(
                got_v[way].at[DIRECT - GROUP : DIRECT],
                got_v[way].at[DIRECT:LIST],
                back_send.at[way],
                back_recv.at[way],
                ring(k + back[way]),
            )
        )
        centre.append([])
        for n, (these, row) in enumerate(pieces):
            centre[way].append(
                remote(
                    own_v.at[these, row : row + CHUNK],
                    cent_v.at[way, these, row : row + CHUNK],
                    cent_send.at[way, n],
                    cent_recv.at[way, n],
                    beside[way],
                )
            )

    def live_reach(slab, q, offset):
        live = (q < count_ref[slab]) & (off_ref[q, slab] == offset)
        return jnp.where(live, range_ref[q, slab], 0)

    def combine(wanted, with_phonon):
        reach = [[live_reach(k, q, offset) for q in range(slots)] for _, offset in wanted]

        def step(t, carry):
            rows = pl.ds(pl.multiple_of(t * TILE, TILE), TILE)
            row_ids = t * TILE + lax.broadcasted_iota(jnp.int32, (TILE, width), 0)
            col_ids = lax.broadcasted_iota(jnp.int32, (TILE, width), 1)
            far = jnp.maximum(row_ids, col_ids)
            m = lax.div(t, UNIT // TILE)
            unit_rows = pl.ds(pl.multiple_of(t * TILE - m * UNIT, TILE), TILE)
            for part in range(2):
                terms = [sigma_v[q, part, rows, :].astype(F32) for q in range(slots)]
                for n, (at, _) in enumerate(wanted):
                    kept = [jnp.where(far < reach[n][q], terms[q], 0.0) for q in range(slots)]
                    total = functools.reduce(jnp.add, kept)
                    if with_phonon:
                        low = near_v[0, part, rows, :].astype(F32)
                        high = near_v[1, part, rows, :].astype(F32)
                        total = total + (0.5 * (low + high)).astype(BF16).astype(F32)
                    total = total.astype(BF16)
                    lanes = slice(part * CHUNK, (part + 1) * CHUNK)
                    for c in range(chunks):
                        value = total[:, c * CHUNK : (c + 1) * CHUNK]
                        if with_phonon:
                            own_v[c, rows, lanes] = value
                        else:
                            mine_v[at, m, c, unit_rows, lanes] = value
            return carry

        lax.fori_loop(0, width // TILE, step, 0)

    def layout(slab, way):
        blocks = []
        for offset in OFFSETS[2 * way : 2 * way + 2]:
            reach = functools.reduce(jnp.maximum, [live_reach(slab, q, offset) for q in range(slots)])
            blocks.append(extent(reach))
        return blocks

    def pack(way, first, last):
        (_, across_a, size_a), (_, across_b, size_b) = layout(k, way)

        def step(p, carry):
            in_a = p < size_a
            unit = jnp.where(in_a, p, jnp.maximum(p - size_a, 0))
            across = jnp.where(in_a, across_a, across_b)
            row = jnp.where(across == 3, lax.div(unit, 3), jnp.where(across == 2, lax.div(unit, 2), unit))
            col = jnp.clip(unit - row * across, 0, chunks - 1)
            row = jnp.clip(row, 0, width // UNIT - 1)
            at = 2 * way + jnp.where(in_a, 0, 1)
            keep = jnp.where(p < size_a + size_b, 1.0, 0.0).astype(BF16)
            list_v[way, p] = mine_v[at, row, col] * keep
            return carry

        lax.fori_loop(first, last, step, 0)

    for table in tables:
        table.wait()
    load_sigma.wait()
    load_green.start()
    held_back = groups - 1 if around else groups
    for way in range(2):
        combine([(2 * way + n, OFFSETS[2 * way + n]) for n in range(2)], False)
        if around:
            pack(way, DIRECT, LIST)
            spill[way].start()
            pack(way, 0, DIRECT)
        else:
            pack(way, 0, LIST)
        for copy in direct[way][:held_back]:
            copy.start()

    for there, slot in ((has_low, 0), (has_high, 1)):

        @pl.when(jnp.logical_not(there))
        def _():
            near_v[slot] = jnp.zeros_like(near_v[slot])

    @pl.when(has_low)
    def _():
        up.wait_recv()

    @pl.when(has_high)
    def _():
        down.wait_recv()

    combine([(4, 0)], True)
    if around:
        for way in range(2):
            spill[way].wait_recv()
            for j in range(GROUP):
                p = DIRECT - GROUP + j
                list_v[way, p] = list_v[way, p] + spill_v[way, j]
        for way in range(2):
            direct[way][-1].start()
    for way in range(2):
        for copy in centre[way]:
            copy.start()

    load_green.wait()
    for at in range(3):
        for part in range(2):
            turned = green_v[at, part].astype(F32).T
            plain = turned.astype(BF16)
            minus = (-turned).astype(BF16)
            for c in range(chunks):
                source = slice(c * CHUNK, (c + 1) * CHUNK)
                real = slice(2 * c * CHUNK, (2 * c + 1) * CHUNK)
                imag = slice((2 * c + 1) * CHUNK, (2 * c + 2) * CHUNK)
                if part == 0:
                    b_v[at, real, :width] = plain[source]
                    b_v[at, imag, width:] = plain[source]
                else:
                    b_v[at, real, width:] = minus[source]
                    b_v[at, imag, :width] = plain[source]
    inside = (None, k > 0, k < slabs - 1)
    for c in range(chunks):
        for n, at in enumerate((1, 0, 2)):
            for part in range(2):
                to = n * 2 * CHUNK + part * CHUNK
                value = green_v[at, part, :, c * CHUNK : (c + 1) * CHUNK]
                if inside[n] is not None:
                    value = jnp.where(inside[n], value, jnp.zeros_like(value))
                a_v[c, :, to : to + CHUNK] = value

    def dot(a, b):
        return jnp.dot(a, b, preferred_element_type=F32)

    def b_chunk(at, c):
        return b_v[at, 2 * c * CHUNK : 2 * (c + 1) * CHUNK]

    def put(at, x):
        real = x[:, :width].astype(BF16)
        imag = x[:, width:].astype(BF16)
        y_v[at : at + CHUNK, :width] = real
        y_v[at : at + CHUNK, width:] = imag
        y_v[at + CHUNK : at + 2 * CHUNK, :width] = -imag
        y_v[at + CHUNK : at + 2 * CHUNK, width:] = real

    for n, (at, partner) in enumerate(((2, 0), (0, 2))):
        for r in range(2):
            rows = slice(r * width // 2, (r + 1) * width // 2)
            units = slice(rows.start // UNIT, rows.stop // UNIT)
            x = None
            for c in range(chunks):
                term = dot(mine_v[at, units, c].reshape(width // 2, 2 * CHUNK), b_chunk(partner, c))
                x = term if x is None else x + term
            part_v[0, rows] = x if n == 0 else part_v[0, rows] + x
    for r in range(chunks):
        rows = slice(r * CHUNK, (r + 1) * CHUNK)
        x = part_v[0, rows]
        for c in range(chunks):
            x = x + dot(own_v[c, rows], b_chunk(1, c))
        put(0, x)
        term = dot(a_v[r, :, : 2 * CHUNK], y_v[: 2 * CHUNK])
        acc_v[...] = term if r == 0 else acc_v[...] + term

    if around:
        for way in range(2):
            direct[way][-1].wait_recv()
            returned[way].start()

    for way in range(2):
        for copy in direct[way][:held_back]:
            copy.wait_recv()
        if around:
            returned[way].wait_recv()
        start = 0
        blocks = layout((last_k, next_k)[way], way)
        for n, (down_n, across_n, size_n) in enumerate(blocks):
            for m in range(width // UNIT):
                for c in range(chunks):
                    position = jnp.clip(start + m * across_n + c, 0, LIST - 1)
                    keep = jnp.where((m < down_n) & (c < across_n), 1.0, 0.0).astype(BF16)
                    block_v[c, m * UNIT : (m + 1) * UNIT] = got_v[way][position] * keep
            start = start + size_n
            partner = ((1, 2), (1, 0))[way][n]
            for r in range(chunks):
                rows = slice(r * CHUNK, (r + 1) * CHUNK)
                x = None
                for c in range(chunks):
                    term = dot(block_v[c, rows], b_chunk(partner, c))
                    x = term if x is None else x + term
                part_v[way, rows] = x if n == 0 else part_v[way, rows] + x

    for n, (these, row) in enumerate(pieces):
        rows = slice(row, row + CHUNK)
        final = n == len(pieces) - 1
        for way in range(2):
            centre[way][n].wait_recv()
            partner = (0, 2)[way]
            x = part_v[way, rows]
            for c in range(chunks)[these]:
                x = x + dot(cent_v[way, c, rows], b_chunk(partner, c))
            if n < chunks - 1 or final:
                put(2 * CHUNK * way, x)
            else:
                part_v[way, rows] = x
        if n < chunks - 1:
            acc_v[...] = acc_v[...] + dot(a_v[n, :, 2 * CHUNK :], y_v[...])
    for m in range(chunks):
        rows = slice(m * CHUNK, (m + 1) * CHUNK)
        total = acc_v[rows] + dot(a_v[chunks - 1, rows, 2 * CHUNK :], y_v[...])
        for part in range(2):
            out_ref[0, 0, part, rows] = total[:, part * width : (part + 1) * width]

    @pl.when(has_high)
    def _():
        up.wait_send()

    @pl.when(has_low)
    def _():
        down.wait_send()

    for way in range(2):
        for copy in direct[way] + centre[way] + ([spill[way], returned[way]] if around else []):
            copy.wait_send()


def solution(mesh):
    slabs, energies = mesh.shape["slab"], mesh.shape["energy"]

    def body(green, sigma, phonon, pair_off, pair_count, pair_range):
        width = green.shape[-1]
        slots = sigma.shape[2]
        chunks = width // CHUNK
        hbm = pl.BlockSpec(memory_space=pltpu.HBM)
        vmem = pl.BlockSpec(memory_space=pltpu.VMEM)
        split = (chunks, width, 2 * CHUNK)
        unit = (UNIT, 2 * CHUNK)
        operands = (pair_off.T, pair_count, pair_range.T, green, sigma, phonon)
        operands = [pltpu.with_memory_space_constraint(v, pltpu.HBM) for v in operands]

        def call(around, *operands):
            return pl.pallas_call(
                functools.partial(kernel, slabs, energies, around),
                out_shape=jax.ShapeDtypeStruct((1, 1, 2, width, width), F32),
                in_specs=[hbm] * 6,
                out_specs=vmem,
                scratch_shapes=[
                    pltpu.SMEM((slots, slabs), jnp.int32),
                    pltpu.SMEM((slabs,), jnp.int32),
                    pltpu.SMEM((slots, slabs), jnp.int32),
                    pltpu.VMEM((3, 2, width, width), BF16),
                    pltpu.VMEM((slots, 2, width, width), BF16),
                    pltpu.VMEM((2, 2, width, width), BF16),
                    pltpu.VMEM((4, width // UNIT, chunks) + unit, BF16),
                    pltpu.VMEM(split, BF16),
                    pltpu.VMEM((2, LIST) + unit, BF16),
                    pltpu.VMEM((LIST,) + unit, BF16),
                    pltpu.VMEM((LIST,) + unit, BF16),
                    pltpu.VMEM((2, GROUP) + unit, BF16),
                    pltpu.VMEM((2,) + split, BF16),
                    pltpu.VMEM(split, BF16),
                    pltpu.VMEM((3, 2 * width, 2 * width), BF16),
                    pltpu.VMEM((chunks, width, 6 * CHUNK), BF16),
                    pltpu.VMEM((4 * CHUNK, 2 * width), BF16),
                    pltpu.VMEM((2, width, 2 * width), F32),
                    pltpu.VMEM((width, 2 * width), F32),
                    pltpu.SemaphoreType.DMA((5,)),
                    pltpu.SemaphoreType.DMA((2,)),
                    pltpu.SemaphoreType.DMA((2,)),
                    pltpu.SemaphoreType.DMA((2, LIST // GROUP)),
                    pltpu.SemaphoreType.DMA((2, LIST // GROUP)),
                    pltpu.SemaphoreType.DMA((2,)),
                    pltpu.SemaphoreType.DMA((2,)),
                    pltpu.SemaphoreType.DMA((2,)),
                    pltpu.SemaphoreType.DMA((2,)),
                    pltpu.SemaphoreType.DMA((2, 2 * chunks - 1)),
                    pltpu.SemaphoreType.DMA((2, 2 * chunks - 1)),
                ],
                compiler_params=pltpu.CompilerParams(
                    collective_id=int(around), has_side_effects=True, vmem_limit_bytes=48 * 1024 * 1024
                ),
                name="around" if around else "straight",
            )(*operands)

        crowded = pl.pallas_call(
            crowded_kernel,
            out_shape=jax.ShapeDtypeStruct((1,), jnp.int32),
            in_specs=[vmem] * 3,
            out_specs=pl.BlockSpec(memory_space=pltpu.SMEM),
            name="crowded",
        )(pair_off.T, pair_count[None], pair_range.T)
        return lax.cond(
            crowded[0] > 0, functools.partial(call, False), functools.partial(call, True), *operands
        )

    wide = P("energy", "slab", None, None, None, None)
    slim = P("energy", "slab", None, None, None)
    return jax.shard_map(
        body,
        mesh=mesh,
        in_specs=(wide, wide, slim, P(), P(), P()),
        out_specs=slim,
        check_vma=False,
    )
```

```python
import functools

import jax
import jax.numpy as jnp
from jax import lax
from jax.experimental import pallas as pl
from jax.experimental.pallas import tpu as pltpu
from jax.sharding import PartitionSpec as P

MESH = pl.DeviceIdType.MESH
F32 = jnp.float32
BF16 = jnp.bfloat16
TILE = 16
CHUNK = 128
UNIT = 96
GROUP = 6
LIST = 24
DIRECT = 18
HOP = 4
OFFSETS = (1, 2, -1, -2)


def extent(reach):
    steps = [(reach >= n * UNIT).astype(jnp.int32) for n in range(1, 5)]
    down = steps[0] + steps[1] + steps[2] + steps[3]
    across = steps[0] + steps[1] + steps[2]
    return down, across, down * across


def turned(slab, way):
    place = lax.rem(slab, HOP)
    paired = jnp.where(lax.rem(lax.div(slab, HOP), 2) == 0, HOP, -HOP)
    if way == 0:
        return jnp.where(place == HOP - 1, -HOP, jnp.where(place == 1, paired, HOP))
    return jnp.where(place == 0, HOP, jnp.where(place == 2, paired, -HOP))


def detours(slab, way, slabs):
    low, high = (0, slabs - 2) if way == 0 else (1, slabs - 1)
    relay = slab + turned(slab, way)
    return (slab >= low) & (slab <= high) & (relay >= low) & (relay <= high)


def relayed(relay, way):
    turn = turned(relay, way)
    return relay + jnp.where(lax.rem(relay, HOP) == 1 + way, turn, -turn)


def crowded_kernel(off_ref, count_ref, range_ref, out_ref):
    off, reach = off_ref[...], range_ref[...]
    slots, slabs = off.shape
    live = lax.broadcasted_iota(jnp.int32, off.shape, 0) < count_ref[...]
    slab = lax.broadcasted_iota(jnp.int32, (1, slabs), 1)
    crowded = jnp.zeros((1, slabs), F32)
    for way in range(2):
        filled = jnp.zeros((1, slabs), jnp.int32)
        for offset in OFFSETS[2 * way : 2 * way + 2]:
            widest = jnp.max(jnp.where(live & (off == offset), reach, 0), axis=0, keepdims=True)
            filled = filled + extent(widest)[2]
        above = jnp.concatenate([filled[:, HOP:], filled[:, :HOP]], axis=1)
        below = jnp.concatenate([filled[:, -HOP:], filled[:, :-HOP]], axis=1)
        relay = jnp.where(turned(slab, way) > 0, above, below)
        stuck = (relay > LIST - 2 * GROUP) | jnp.logical_not(detours(slab, way, slabs))
        crowded = crowded + ((filled > DIRECT) & stuck).astype(F32)
    out_ref[0] = jnp.max(crowded).astype(jnp.int32)


def kernel(
    slabs,
    energies,
    around,
    off_hbm,
    count_hbm,
    range_hbm,
    green_hbm,
    sigma_hbm,
    phonon_hbm,
    out_ref,
    off_ref,
    count_ref,
    range_ref,
    green_v,
    sigma_v,
    near_v,
    mine_v,
    own_v,
    list_v,
    from_left_v,
    from_right_v,
    spill_v,
    cent_v,
    block_v,
    b_v,
    a_v,
    y_v,
    part_v,
    acc_v,
    local_sem,
    near_send,
    near_recv,
    unit_send,
    unit_recv,
    spill_send,
    spill_recv,
    back_send,
    back_recv,
    cent_send,
    cent_recv,
):
    k = lax.axis_index("slab")
    e = lax.axis_index("energy")
    width = green_v.shape[-1]
    slots = sigma_v.shape[0]
    chunks = width // CHUNK
    has_low, has_high = e > 0, e < energies - 1

    has_left, has_right = k > 0, k < slabs - 1

    tables = [
        pltpu.make_async_copy(source, held, local_sem.at[n])
        for n, (source, held) in enumerate(
            ((off_hbm, off_ref), (count_hbm, count_ref), (range_hbm, range_ref))
        )
    ]
    load_sigma = []
    for c in range(chunks):
        rows = slice(c * CHUNK, (c + 1) * CHUNK)
        load_sigma.append(
            pltpu.make_async_copy(
                sigma_hbm.at[0, 0, :, :, rows], sigma_v.at[:, :, rows], local_sem.at[4 + c]
            )
        )
    load_green = pltpu.make_async_copy(green_hbm.at[0, 0], green_v, local_sem.at[3])
    for table in tables:
        table.start()
    for load in load_sigma:
        load.start()

    barrier = pltpu.get_barrier_semaphore()
    peers = [
        (has_left, {"slab": k - 1}),
        (has_right, {"slab": k + 1}),
        (has_low, {"energy": e - 1}),
        (has_high, {"energy": e + 1}),
    ]
    if around:
        peers += [(k >= HOP, {"slab": k - HOP}), (k < slabs - HOP, {"slab": k + HOP})]
    for there, who in peers:

        @pl.when(there)
        def _():
            pl.semaphore_signal(barrier, inc=1, device_id=who, device_id_type=MESH)

    pl.semaphore_wait(barrier, sum(there.astype(jnp.int32) for there, _ in peers))

    def near_copy(slot, target):
        return pltpu.make_async_remote_copy(
            src_ref=phonon_hbm.at[0, 0],
            dst_ref=near_v.at[slot],
            send_sem=near_send.at[slot],
            recv_sem=near_recv.at[slot],
            device_id={"energy": target},
            device_id_type=MESH,
        )

    up, down = near_copy(0, e + 1), near_copy(1, e - 1)

    @pl.when(has_high)
    def _():
        up.start()

    @pl.when(has_low)
    def _():
        down.start()

    def remote(source, target, sent, received, slab):
        return pltpu.make_async_remote_copy(
            src_ref=source,
            dst_ref=target,
            send_sem=sent,
            recv_sem=received,
            device_id={"slab": slab},
            device_id_type=MESH,
        )

    sends = [detours(k, way, slabs) for way in range(2)]
    rides = [relayed(k, way) for way in range(2)]
    relays = [detours(rides[way], way, slabs) for way in range(2)]
    handed = [relayed(k + step, way) for way, step in ((0, -1), (1, 1))]
    hands = [there & detours(handed[way], way, slabs) for way, there in enumerate((has_left, has_right))]
    gets = [there & detours(k + step, way, slabs) for way, (there, step) in enumerate(((has_left, -1), (has_right, 1)))]
    beside = (k + 1, k - 1)
    goes, comes = (has_right, has_left), (has_left, has_right)
    got_v = (from_left_v, from_right_v)
    groups = (DIRECT if around else LIST) // GROUP
    direct, spill, returned, centre = [], [], [], []
    pieces = [(slice(None), c * CHUNK) for c in range(chunks - 1)]
    pieces += [(slice(c, c + 1), width - CHUNK) for c in range(chunks)]
    for way in range(2):
        direct.append([])
        for g in range(groups):
            units = slice(g * GROUP, (g + 1) * GROUP)
            direct[way].append(
                remote(
                    list_v.at[way, units],
                    got_v[way].at[units],
                    unit_send.at[way, g],
                    unit_recv.at[way, g],
                    beside[way],
                )
            )
        spill.append(
            remote(
                list_v.at[way, DIRECT:LIST],
                spill_v.at[way],
                spill_send.at[way],
                spill_recv.at[way],
                k + turned(k, way),
            )
        )
        returned.append(
            remote(
                got_v[way].at[DIRECT - GROUP : DIRECT],
                got_v[way].at[DIRECT:LIST],
                back_send.at[way],
                back_recv.at[way],
                handed[way] + (1, -1)[way],
            )
        )
        centre.append([])
        for n, (these, row) in enumerate(pieces):
            centre[way].append(
                remote(
                    own_v.at[these, row : row + CHUNK],
                    cent_v.at[way, these, row : row + CHUNK],
                    cent_send.at[way, n],
                    cent_recv.at[way, n],
                    beside[way],
                )
            )

    def live_reach(slab, q, offset):
        live = (q < count_ref[slab]) & (off_ref[q, slab] == offset)
        return jnp.where(live, range_ref[q, slab], 0)

    def combine(wanted, with_phonon, first=0, last=width // TILE):
        reach = [[live_reach(k, q, offset) for q in range(slots)] for _, offset in wanted]

        def step(t, carry):
            rows = pl.ds(pl.multiple_of(t * TILE, TILE), TILE)
            col_ids = lax.broadcasted_iota(jnp.int32, (TILE, width), 1)
            m = lax.div(t, UNIT // TILE)
            unit_rows = pl.ds(pl.multiple_of(t * TILE - m * UNIT, TILE), TILE)
            inside = [
                [col_ids < jnp.where(t * TILE < reach[n][q], reach[n][q], 0) for q in range(slots)]
                for n in range(len(wanted))
            ]
            for part in range(2):
                terms = [sigma_v[q, part, rows, :].astype(F32) for q in range(slots)]
                for n, (at, _) in enumerate(wanted):
                    kept = [jnp.where(inside[n][q], terms[q], 0.0) for q in range(slots)]
                    total = functools.reduce(jnp.add, kept)
                    if with_phonon:
                        low = near_v[0, part, rows, :].astype(F32)
                        high = near_v[1, part, rows, :].astype(F32)
                        total = total + (0.5 * (low + high)).astype(BF16).astype(F32)
                    total = total.astype(BF16)
                    lanes = slice(part * CHUNK, (part + 1) * CHUNK)
                    for c in range(chunks):
                        value = total[:, c * CHUNK : (c + 1) * CHUNK]
                        if with_phonon:
                            own_v[c, rows, lanes] = value
                        else:
                            mine_v[at, m, c, unit_rows, lanes] = value
            return carry

        lax.fori_loop(first, last, step, 0)

    def layout(slab, way):
        blocks = []
        for offset in OFFSETS[2 * way : 2 * way + 2]:
            reach = functools.reduce(jnp.maximum, [live_reach(slab, q, offset) for q in range(slots)])
            blocks.append(extent(reach))
        return blocks

    def pack(way, first, last):
        (_, across_a, size_a), (_, across_b, size_b) = layout(k, way)

        def step(p, carry):
            in_a = p < size_a
            unit = jnp.where(in_a, p, jnp.maximum(p - size_a, 0))
            across = jnp.where(in_a, across_a, across_b)
            row = jnp.where(across == 3, lax.div(unit, 3), jnp.where(across == 2, lax.div(unit, 2), unit))
            col = jnp.clip(unit - row * across, 0, chunks - 1)
            row = jnp.clip(row, 0, width // UNIT - 1)
            at = 2 * way + jnp.where(in_a, 0, 1)
            keep = jnp.where(p < size_a + size_b, 1.0, 0.0).astype(BF16)
            list_v[way, p] = mine_v[at, row, col] * keep
            return carry

        lax.fori_loop(first, last, step, 0)

    for table in tables:
        table.wait()
    def start(there, *copies):
        @pl.when(there)
        def _():
            for copy in copies:
                copy.start()

    def arrived(there, *copies):
        @pl.when(there)
        def _():
            for copy in copies:
                copy.wait_recv()

    held_back = groups - 1 if around else groups
    tiles = width // TILE // chunks
    for way in range(2):
        wanted = [(2 * way + n, OFFSETS[2 * way + n]) for n in range(2)]
        if way == 0:
            for c in range(chunks):
                load_sigma[c].wait()
                combine(wanted, False, c * tiles, (c + 1) * tiles)
            load_green.start()
        else:
            combine(wanted, False)
        if around:
            pack(way, DIRECT, LIST)
            start(sends[way], spill[way])
            pack(way, 0, DIRECT)
        else:
            pack(way, 0, LIST)
        start(goes[way], *direct[way][:held_back])

    for way in range(2):

        @pl.when(jnp.logical_not(comes[way]))
        def _():
            got_v[way][...] = jnp.zeros_like(got_v[way])
            cent_v[way] = jnp.zeros_like(cent_v[way])

        if around:

            @pl.when(comes[way] & jnp.logical_not(gets[way]))
            def _():
                got_v[way][DIRECT:LIST] = jnp.zeros_like(got_v[way][DIRECT:LIST])

            @pl.when(jnp.logical_not(relays[way]))
            def _():
                spill_v[way] = jnp.zeros_like(spill_v[way])

    for there, slot in ((has_low, 0), (has_high, 1)):

        @pl.when(jnp.logical_not(there))
        def _():
            near_v[slot] = jnp.zeros_like(near_v[slot])

    @pl.when(has_low)
    def _():
        up.wait_recv()

    @pl.when(has_high)
    def _():
        down.wait_recv()

    combine([(4, 0)], True)
    if around:
        for way in range(2):
            arrived(relays[way], spill[way])
            for j in range(GROUP):
                p = DIRECT - GROUP + j
                list_v[way, p] = list_v[way, p] + spill_v[way, j]
        for way in range(2):
            start(goes[way], direct[way][-1])
    for way in range(2):
        start(goes[way], *centre[way])

    load_green.wait()
    for at in range(3):
        for part in range(2):
            flipped = green_v[at, part].astype(F32).T
            plain = flipped.astype(BF16)
            minus = (-flipped).astype(BF16)
            for c in range(chunks):
                source = slice(c * CHUNK, (c + 1) * CHUNK)
                real = slice(2 * c * CHUNK, (2 * c + 1) * CHUNK)
                imag = slice((2 * c + 1) * CHUNK, (2 * c + 2) * CHUNK)
                if part == 0:
                    b_v[at, real, :width] = plain[source]
                    b_v[at, imag, width:] = plain[source]
                else:
                    b_v[at, real, width:] = minus[source]
                    b_v[at, imag, :width] = plain[source]
    inside = (None, has_left, has_right)
    for c in range(chunks):
        for n, at in enumerate((1, 0, 2)):
            for part in range(2):
                to = n * 2 * CHUNK + part * CHUNK
                value = green_v[at, part, :, c * CHUNK : (c + 1) * CHUNK]
                if inside[n] is not None:
                    value = jnp.where(inside[n], value, jnp.zeros_like(value))
                a_v[c, :, to : to + CHUNK] = value

    def dot(a, b):
        return jnp.dot(a, b, preferred_element_type=F32)

    def b_chunk(at, c):
        return b_v[at, 2 * c * CHUNK : 2 * (c + 1) * CHUNK]

    def put(at, x):
        real = x[:, :width].astype(BF16)
        imag = x[:, width:].astype(BF16)
        y_v[at : at + CHUNK, :width] = real
        y_v[at : at + CHUNK, width:] = imag
        y_v[at + CHUNK : at + 2 * CHUNK, :width] = -imag
        y_v[at + CHUNK : at + 2 * CHUNK, width:] = real

    for n, (at, partner) in enumerate(((2, 0), (0, 2))):
        for r in range(2):
            rows = slice(r * width // 2, (r + 1) * width // 2)
            units = slice(rows.start // UNIT, rows.stop // UNIT)
            x = None
            for c in range(chunks):
                term = dot(mine_v[at, units, c].reshape(width // 2, 2 * CHUNK), b_chunk(partner, c))
                x = term if x is None else x + term
            part_v[0, rows] = x if n == 0 else part_v[0, rows] + x
    for r in range(chunks):
        rows = slice(r * CHUNK, (r + 1) * CHUNK)
        x = part_v[0, rows]
        for c in range(chunks):
            x = x + dot(own_v[c, rows], b_chunk(1, c))
        put(0, x)
        term = dot(a_v[r, :, : 2 * CHUNK], y_v[: 2 * CHUNK])
        acc_v[...] = term if r == 0 else acc_v[...] + term

    if around:
        for way in range(2):
            arrived(comes[way], direct[way][-1])
            start(hands[way], returned[way])

    for way in range(2):
        arrived(comes[way], *direct[way][:held_back])
        if around:
            arrived(gets[way], returned[way])
        before = 0
        blocks = layout((jnp.maximum(k - 1, 0), jnp.minimum(k + 1, slabs - 1))[way], way)
        for n, (down_n, across_n, size_n) in enumerate(blocks):
            for m in range(width // UNIT):
                for c in range(chunks):
                    position = jnp.clip(before + m * across_n + c, 0, LIST - 1)
                    keep = jnp.where((m < down_n) & (c < across_n), 1.0, 0.0).astype(BF16)
                    block_v[c, m * UNIT : (m + 1) * UNIT] = got_v[way][position] * keep
            before = before + size_n
            partner = ((1, 2), (1, 0))[way][n]
            for r in range(chunks):
                rows = slice(r * CHUNK, (r + 1) * CHUNK)
                x = None
                for c in range(chunks):
                    term = dot(block_v[c, rows], b_chunk(partner, c))
                    x = term if x is None else x + term
                part_v[way, rows] = x if n == 0 else part_v[way, rows] + x

    for n, (these, row) in enumerate(pieces):
        rows = slice(row, row + CHUNK)
        final = n == len(pieces) - 1
        for way in range(2):
            arrived(comes[way], centre[way][n])
            partner = (0, 2)[way]
            x = part_v[way, rows]
            for c in range(chunks)[these]:
                x = x + dot(cent_v[way, c, rows], b_chunk(partner, c))
            if n < chunks - 1 or final:
                put(2 * CHUNK * way, x)
            else:
                part_v[way, rows] = x
        if n < chunks - 1:
            acc_v[...] = acc_v[...] + dot(a_v[n, :, 2 * CHUNK :], y_v[...])
    for m in range(chunks):
        rows = slice(m * CHUNK, (m + 1) * CHUNK)
        total = acc_v[rows] + dot(a_v[chunks - 1, rows, 2 * CHUNK :], y_v[...])
        for part in range(2):
            out_ref[0, 0, part, rows] = total[:, part * width : (part + 1) * width]

    @pl.when(has_high)
    def _():
        up.wait_send()

    @pl.when(has_low)
    def _():
        down.wait_send()

    for way in range(2):
        for there, copies in (
            (goes[way], direct[way] + centre[way]),
            (sends[way], [spill[way]] if around else []),
            (hands[way], [returned[way]] if around else []),
        ):

            @pl.when(there)
            def _():
                for copy in copies:
                    copy.wait_send()


def solution(mesh):
    slabs, energies = mesh.shape["slab"], mesh.shape["energy"]

    def body(green, sigma, phonon, pair_off, pair_count, pair_range):
        width = green.shape[-1]
        slots = sigma.shape[2]
        chunks = width // CHUNK
        hbm = pl.BlockSpec(memory_space=pltpu.HBM)
        vmem = pl.BlockSpec(memory_space=pltpu.VMEM)
        split = (chunks, width, 2 * CHUNK)
        unit = (UNIT, 2 * CHUNK)
        operands = (pair_off.T, pair_count, pair_range.T, green, sigma, phonon)
        operands = [pltpu.with_memory_space_constraint(v, pltpu.HBM) for v in operands]

        def call(around, *operands):
            return pl.pallas_call(
                functools.partial(kernel, slabs, energies, around),
                out_shape=jax.ShapeDtypeStruct((1, 1, 2, width, width), F32),
                in_specs=[hbm] * 6,
                out_specs=vmem,
                scratch_shapes=[
                    pltpu.SMEM((slots, slabs), jnp.int32),
                    pltpu.SMEM((slabs,), jnp.int32),
                    pltpu.SMEM((slots, slabs), jnp.int32),
                    pltpu.VMEM((3, 2, width, width), BF16),
                    pltpu.VMEM((slots, 2, width, width), BF16),
                    pltpu.VMEM((2, 2, width, width), BF16),
                    pltpu.VMEM((4, width // UNIT, chunks) + unit, BF16),
                    pltpu.VMEM(split, BF16),
                    pltpu.VMEM((2, LIST) + unit, BF16),
                    pltpu.VMEM((LIST,) + unit, BF16),
                    pltpu.VMEM((LIST,) + unit, BF16),
                    pltpu.VMEM((2, GROUP) + unit, BF16),
                    pltpu.VMEM((2,) + split, BF16),
                    pltpu.VMEM(split, BF16),
                    pltpu.VMEM((3, 2 * width, 2 * width), BF16),
                    pltpu.VMEM((chunks, width, 6 * CHUNK), BF16),
                    pltpu.VMEM((4 * CHUNK, 2 * width), BF16),
                    pltpu.VMEM((2, width, 2 * width), F32),
                    pltpu.VMEM((width, 2 * width), F32),
                    pltpu.SemaphoreType.DMA((4 + chunks,)),
                    pltpu.SemaphoreType.DMA((2,)),
                    pltpu.SemaphoreType.DMA((2,)),
                    pltpu.SemaphoreType.DMA((2, LIST // GROUP)),
                    pltpu.SemaphoreType.DMA((2, LIST // GROUP)),
                    pltpu.SemaphoreType.DMA((2,)),
                    pltpu.SemaphoreType.DMA((2,)),
                    pltpu.SemaphoreType.DMA((2,)),
                    pltpu.SemaphoreType.DMA((2,)),
                    pltpu.SemaphoreType.DMA((2, 2 * chunks - 1)),
                    pltpu.SemaphoreType.DMA((2, 2 * chunks - 1)),
                ],
                compiler_params=pltpu.CompilerParams(
                    collective_id=int(around), has_side_effects=True, vmem_limit_bytes=48 * 1024 * 1024
                ),
                name="around" if around else "straight",
            )(*operands)

        crowded = pl.pallas_call(
            crowded_kernel,
            out_shape=jax.ShapeDtypeStruct((1,), jnp.int32),
            in_specs=[vmem] * 3,
            out_specs=pl.BlockSpec(memory_space=pltpu.SMEM),
            name="crowded",
        )(pair_off.T, pair_count[None], pair_range.T)
        return lax.cond(
            crowded[0] > 0, functools.partial(call, False), functools.partial(call, True), *operands
        )

    wide = P("energy", "slab", None, None, None, None)
    slim = P("energy", "slab", None, None, None)
    return jax.shard_map(
        body,
        mesh=mesh,
        in_specs=(wide, wide, slim, P(), P(), P()),
        out_specs=slim,
        check_vma=False,
    )
```

```python
import functools

import jax
import jax.numpy as jnp
from jax import lax
from jax.experimental import pallas as pl
from jax.experimental.pallas import tpu as pltpu
from jax.sharding import PartitionSpec as P

MESH = pl.DeviceIdType.MESH
F32 = jnp.float32
BF16 = jnp.bfloat16
TILE = 16
CHUNK = 128
LAST = 64


def kernel(
    slabs,
    energies,
    off_hbm,
    count_hbm,
    range_hbm,
    green_hbm,
    sigma_hbm,
    phonon_hbm,
    out_ref,
    off_ref,
    count_ref,
    range_ref,
    green_v,
    sigma_v,
    near_v,
    mine_v,
    got_v,
    b_v,
    a_v,
    side_v,
    y_v,
    part_v,
    acc_v,
    local_sem,
    near_send,
    near_recv,
    send_sem,
    recv_sem,
):
    k = lax.axis_index("slab")
    e = lax.axis_index("energy")
    width = green_v.shape[-1]
    slots = sigma_v.shape[0]
    chunks = width // CHUNK
    has_low, has_high = e > 0, e < energies - 1
    has_left, has_right = k > 0, k < slabs - 1
    goes, comes = (has_right, has_left), (has_left, has_right)

    tables = [
        pltpu.make_async_copy(source, held, local_sem.at[n])
        for n, (source, held) in enumerate(
            ((off_hbm, off_ref), (count_hbm, count_ref), (range_hbm, range_ref))
        )
    ]
    load_sigma = []
    for c in range(chunks):
        rows = slice(c * CHUNK, (c + 1) * CHUNK)
        load_sigma.append(
            pltpu.make_async_copy(
                sigma_hbm.at[0, 0, :, :, rows], sigma_v.at[:, :, rows], local_sem.at[4 + c]
            )
        )
    load_green = pltpu.make_async_copy(green_hbm.at[0, 0], green_v, local_sem.at[3])

    barrier = pltpu.get_barrier_semaphore()
    peers = (
        (has_left, {"slab": k - 1}),
        (has_right, {"slab": k + 1}),
        (has_low, {"energy": e - 1}),
        (has_high, {"energy": e + 1}),
    )
    for there, who in peers:

        @pl.when(there)
        def _():
            pl.semaphore_signal(barrier, inc=1, device_id=who, device_id_type=MESH)

    for table in tables:
        table.start()
    for load in load_sigma:
        load.start()

    def near_copy(slot, target):
        return pltpu.make_async_remote_copy(
            src_ref=phonon_hbm.at[0, 0],
            dst_ref=near_v.at[slot],
            send_sem=near_send.at[slot],
            recv_sem=near_recv.at[slot],
            device_id={"energy": target},
            device_id_type=MESH,
        )

    up, down = near_copy(0, e + 1), near_copy(1, e - 1)

    whole = slice(None)
    plan = [(0, whole, c * CHUNK, CHUNK) for c in range(chunks)]
    plan += [(1, whole, 0, width)]
    first_centre = len(plan)
    plan += [(2, whole, c * CHUNK, CHUNK) for c in range(chunks - 1)]
    plan += [(2, whole, width - CHUNK, CHUNK - LAST)]
    plan += [(2, slice(c, c + 1), width - LAST, LAST) for c in range(chunks)]
    sent = [[], []]
    for way in range(2):
        for n, (slot, these, row, count) in enumerate(plan):
            source = 4 if slot == 2 else 2 * way + slot
            sent[way].append(
                pltpu.make_async_remote_copy(
                    src_ref=mine_v.at[source, these, row : row + count],
                    dst_ref=got_v.at[way, slot, these, row : row + count],
                    send_sem=send_sem.at[way, n],
                    recv_sem=recv_sem.at[way, n],
                    device_id={"slab": (k + 1, k - 1)[way]},
                    device_id_type=MESH,
                )
            )

    def start(there, *copies):
        @pl.when(there)
        def _():
            for copy in copies:
                copy.start()

    def arrived(there, *copies):
        @pl.when(there)
        def _():
            for copy in copies:
                copy.wait_recv()

    def combine(at, offset, with_phonon, first=0, last=width // TILE):
        reach = []
        for q in range(slots):
            live = (q < count_ref[k]) & (off_ref[q, k] == offset)
            reach.append(jnp.where(live, range_ref[q, k], 0))

        def step(t, carry):
            rows = pl.ds(pl.multiple_of(t * TILE, TILE), TILE)
            col_ids = lax.broadcasted_iota(jnp.int32, (TILE, width), 1)
            inside = [col_ids < jnp.where(t * TILE < reach[q], reach[q], 0) for q in range(slots)]
            for part in range(2):
                kept = [
                    jnp.where(inside[q], sigma_v[q, part, rows, :].astype(F32), 0.0) for q in range(slots)
                ]
                total = functools.reduce(jnp.add, kept)
                if with_phonon:
                    low = near_v[0, part, rows, :].astype(F32)
                    high = near_v[1, part, rows, :].astype(F32)
                    total = total + (0.5 * (low + high)).astype(BF16).astype(F32)
                total = total.astype(BF16)
                for c in range(chunks):
                    mine_v[at, c, rows, part * CHUNK : (part + 1) * CHUNK] = total[
                        :, c * CHUNK : (c + 1) * CHUNK
                    ]
            return carry

        lax.fori_loop(first, last, step, 0)

    for table in tables:
        table.wait()
    tiles = CHUNK // TILE
    for c in range(chunks):
        load_sigma[c].wait()
        for way in range(2):
            combine(2 * way, (1, -1)[way], False, c * tiles, (c + 1) * tiles)
            if c == 0 and way == 0:
                pl.semaphore_wait(barrier, sum(there.astype(jnp.int32) for there, _ in peers))
            start(goes[way], sent[way][c])
        if c == 0:
            start(has_high, up)
            start(has_low, down)
    load_green.start()
    for way in range(2):
        combine(2 * way + 1, (2, -2)[way], False)
        start(goes[way], sent[way][chunks])

    for way in range(2):

        @pl.when(jnp.logical_not(comes[way]))
        def _():
            got_v[way] = jnp.zeros_like(got_v[way])

    for there, slot in ((has_low, 0), (has_high, 1)):

        @pl.when(jnp.logical_not(there))
        def _():
            near_v[slot] = jnp.zeros_like(near_v[slot])

    load_green.wait()
    for at in range(3):
        for part in range(2):
            flipped = green_v[at, part].astype(F32).T
            plain = flipped.astype(BF16)
            minus = (-flipped).astype(BF16)
            for c in range(chunks):
                source = slice(c * CHUNK, (c + 1) * CHUNK)
                real = slice(2 * c * CHUNK, (2 * c + 1) * CHUNK)
                imag = slice((2 * c + 1) * CHUNK, (2 * c + 2) * CHUNK)
                if part == 0:
                    b_v[at, real, :width] = plain[source]
                    b_v[at, imag, width:] = plain[source]
                else:
                    b_v[at, real, width:] = minus[source]
                    b_v[at, imag, :width] = plain[source]
    for c in range(chunks):
        for part in range(2):
            a_v[c, :, part * CHUNK : (part + 1) * CHUNK] = green_v[1, part, :, c * CHUNK : (c + 1) * CHUNK]
    for h in range(width // LAST):
        for n, at in enumerate((0, 2)):
            side_v[h, :, 2 * n * LAST : 2 * (n + 1) * LAST] = jnp.concatenate(
                [green_v[at, part, :, h * LAST : (h + 1) * LAST] for part in range(2)], axis=1
            )

    arrived(has_low, up)
    arrived(has_high, down)
    combine(4, 0, True)
    for way in range(2):
        start(goes[way], *sent[way][first_centre:])

    def dot(a, b):
        return jnp.dot(a, b, preferred_element_type=F32)

    def b_chunk(at, c):
        return b_v[at, 2 * c * CHUNK : 2 * (c + 1) * CHUNK]

    def put(at, x):
        rows = x.shape[0]
        real = x[:, :width].astype(BF16)
        imag = x[:, width:].astype(BF16)
        y_v[at : at + rows, :width] = real
        y_v[at : at + rows, width:] = imag
        y_v[at + rows : at + 2 * rows, :width] = -imag
        y_v[at + rows : at + 2 * rows, width:] = real

    for r in range(chunks):
        rows = slice(r * CHUNK, (r + 1) * CHUNK)
        x = None
        for at, partner in ((2, 0), (4, 1), (0, 2)):
            for c in range(chunks):
                term = dot(mine_v[at, c, rows], b_chunk(partner, c))
                x = term if x is None else x + term
        put(0, x)
        term = dot(a_v[r], y_v[: 2 * CHUNK])
        acc_v[...] = term if r == 0 else acc_v[...] + term

    for slot in range(2):
        for way in range(2):
            arrived(comes[way], *sent[way][chunks * slot : chunks + slot])
            partner = ((1, 2), (1, 0))[way][slot]
            for r in range(chunks):
                rows = slice(r * CHUNK, (r + 1) * CHUNK)
                x = None
                for c in range(chunks):
                    term = dot(got_v[way, slot, c, rows], b_chunk(partner, c))
                    x = term if x is None else x + term
                part_v[way, rows] = x if slot == 0 else part_v[way, rows] + x
    for n, (_, these, row, count) in enumerate(plan[first_centre:]):
        rows = slice(row, row + count)
        complete = these == whole or n == len(plan) - first_centre - 1
        for way in range(2):
            arrived(comes[way], sent[way][first_centre + n])
            x = part_v[way, rows]
            for c in range(chunks)[these]:
                x = x + dot(got_v[way, 2, c, rows], b_chunk((0, 2)[way], c))
            if complete:
                for h in range(count // LAST):
                    put(4 * h * LAST + 2 * way * LAST, x[h * LAST : (h + 1) * LAST])
            else:
                part_v[way, rows] = x
        if complete and n < len(plan) - first_centre - 1:
            total = acc_v[...]
            for h in range(count // LAST):
                total = total + dot(side_v[row // LAST + h], y_v[4 * h * LAST : 4 * (h + 1) * LAST])
            acc_v[...] = total
    for m in range(chunks):
        rows = slice(m * CHUNK, (m + 1) * CHUNK)
        total = acc_v[rows] + dot(side_v[width // LAST - 1, rows], y_v[: 4 * LAST])
        for part in range(2):
            out_ref[0, 0, part, rows] = total[:, part * width : (part + 1) * width]

    for there, copies in ((has_high, [up]), (has_low, [down]), (has_right, sent[0]), (has_left, sent[1])):

        @pl.when(there)
        def _():
            for copy in copies:
                copy.wait_send()


def solution(mesh):
    slabs, energies = mesh.shape["slab"], mesh.shape["energy"]

    def body(green, sigma, phonon, pair_off, pair_count, pair_range):
        width = green.shape[-1]
        slots = sigma.shape[2]
        chunks = width // CHUNK
        copies = 2 * chunks + 1 + chunks
        hbm = pl.BlockSpec(memory_space=pltpu.HBM)
        split = (chunks, width, 2 * CHUNK)
        operands = (pair_off.T, pair_count, pair_range.T, green, sigma, phonon)
        operands = [pltpu.with_memory_space_constraint(v, pltpu.HBM) for v in operands]
        return pl.pallas_call(
            functools.partial(kernel, slabs, energies),
            out_shape=jax.ShapeDtypeStruct((1, 1, 2, width, width), F32),
            in_specs=[hbm] * 6,
            out_specs=pl.BlockSpec(memory_space=pltpu.VMEM),
            scratch_shapes=[
                pltpu.SMEM((slots, slabs), jnp.int32),
                pltpu.SMEM((slabs,), jnp.int32),
                pltpu.SMEM((slots, slabs), jnp.int32),
                pltpu.VMEM((3, 2, width, width), BF16),
                pltpu.VMEM((slots, 2, width, width), BF16),
                pltpu.VMEM((2, 2, width, width), BF16),
                pltpu.VMEM((5,) + split, BF16),
                pltpu.VMEM((2, 3) + split, BF16),
                pltpu.VMEM((3, 2 * width, 2 * width), BF16),
                pltpu.VMEM(split, BF16),
                pltpu.VMEM((width // LAST, width, 4 * LAST), BF16),
                pltpu.VMEM((4 * CHUNK, 2 * width), BF16),
                pltpu.VMEM((2, width, 2 * width), F32),
                pltpu.VMEM((width, 2 * width), F32),
                pltpu.SemaphoreType.DMA((4 + chunks,)),
                pltpu.SemaphoreType.DMA((2,)),
                pltpu.SemaphoreType.DMA((2,)),
                pltpu.SemaphoreType.DMA((2, copies)),
                pltpu.SemaphoreType.DMA((2, copies)),
            ],
            compiler_params=pltpu.CompilerParams(
                collective_id=0, has_side_effects=True, vmem_limit_bytes=48 * 1024 * 1024
            ),
            name="lesser",
        )(*operands)

    wide = P("energy", "slab", None, None, None, None)
    slim = P("energy", "slab", None, None, None)
    return jax.shard_map(
        body,
        mesh=mesh,
        in_specs=(wide, wide, slim, P(), P(), P()),
        out_specs=slim,
        check_vma=False,
    )
```

```python
import functools

import jax
import jax.numpy as jnp
from jax import lax
from jax.experimental import pallas as pl
from jax.experimental.pallas import tpu as pltpu
from jax.sharding import PartitionSpec as P

MESH = pl.DeviceIdType.MESH
F32 = jnp.float32
BF16 = jnp.bfloat16
TILE = 16
CHUNK = 128
LAST = 64
UNIT = 96
GROUP = 3
LIST = 24
DIRECT = 18
SHARED = 12
HOP = 4
OFFSETS = (1, 2, -1, -2)


def extent(reach):
    steps = [(reach >= n * UNIT).astype(jnp.int32) for n in range(1, 5)]
    down = steps[0] + steps[1] + steps[2] + steps[3]
    across = steps[0] + steps[1] + steps[2]
    return down, across, down * across


def turned(slab, way):
    place = lax.rem(slab, HOP)
    paired = jnp.where(lax.rem(lax.div(slab, HOP), 2) == 0, HOP, -HOP)
    if way == 0:
        return jnp.where(place == HOP - 1, -HOP, jnp.where(place == 1, paired, HOP))
    return jnp.where(place == 0, HOP, jnp.where(place == 2, paired, -HOP))


def detours(slab, way, slabs):
    low, high = (0, slabs - 2) if way == 0 else (1, slabs - 1)
    relay = slab + turned(slab, way)
    return (slab >= low) & (slab <= high) & (relay >= low) & (relay <= high)


def relayed(relay, way):
    turn = turned(relay, way)
    return relay + jnp.where(lax.rem(relay, HOP) == 1 + way, turn, -turn)


def crowded_kernel(off_ref, count_ref, range_ref, out_ref):
    off, reach = off_ref[...], range_ref[...]
    slots, slabs = off.shape
    live = lax.broadcasted_iota(jnp.int32, off.shape, 0) < count_ref[...]
    slab = lax.broadcasted_iota(jnp.int32, (1, slabs), 1)
    crowded = jnp.zeros((1, slabs), F32)
    for way in range(2):
        filled = jnp.zeros((1, slabs), jnp.int32)
        for offset in OFFSETS[2 * way : 2 * way + 2]:
            widest = jnp.max(jnp.where(live & (off == offset), reach, 0), axis=0, keepdims=True)
            filled = filled + extent(widest)[2]
        above = jnp.concatenate([filled[:, HOP:], filled[:, :HOP]], axis=1)
        below = jnp.concatenate([filled[:, -HOP:], filled[:, :-HOP]], axis=1)
        relay = jnp.where(turned(slab, way) > 0, above, below)
        stuck = (relay > SHARED) | jnp.logical_not(detours(slab, way, slabs))
        crowded = crowded + ((filled > DIRECT) & stuck).astype(F32)
    out_ref[0] = jnp.max(crowded).astype(jnp.int32)


def dot(a, b):
    return jnp.dot(a, b, preferred_element_type=F32)


def start(there, *copies):
    @pl.when(there)
    def _():
        for copy in copies:
            copy.start()


def arrived(there, *copies):
    @pl.when(there)
    def _():
        for copy in copies:
            copy.wait_recv()


def gone(there, *copies):
    @pl.when(there)
    def _():
        for copy in copies:
            copy.wait_send()


def greet(peers):
    barrier = pltpu.get_barrier_semaphore()
    for there, who in peers:

        @pl.when(there)
        def _():
            pl.semaphore_signal(barrier, inc=1, device_id=who, device_id_type=MESH)


def greeted(peers):
    barrier = pltpu.get_barrier_semaphore()
    pl.semaphore_wait(barrier, sum(there.astype(jnp.int32) for there, _ in peers))


def prepare(green_v, b_v, a_v, side_v):
    width = green_v.shape[-1]
    for at in range(3):
        for part in range(2):
            flipped = green_v[at, part].astype(F32).T
            plain = flipped.astype(BF16)
            minus = (-flipped).astype(BF16)
            for c in range(width // CHUNK):
                source = slice(c * CHUNK, (c + 1) * CHUNK)
                real = slice(2 * c * CHUNK, (2 * c + 1) * CHUNK)
                imag = slice((2 * c + 1) * CHUNK, (2 * c + 2) * CHUNK)
                if part == 0:
                    b_v[at, real, :width] = plain[source]
                    b_v[at, imag, width:] = plain[source]
                else:
                    b_v[at, real, width:] = minus[source]
                    b_v[at, imag, :width] = plain[source]
    for c in range(width // CHUNK):
        for part in range(2):
            a_v[c, :, part * CHUNK : (part + 1) * CHUNK] = green_v[1, part, :, c * CHUNK : (c + 1) * CHUNK]
    for h in range(width // LAST):
        for n, at in enumerate((0, 2)):
            side_v[h, :, 2 * n * LAST : 2 * (n + 1) * LAST] = jnp.concatenate(
                [green_v[at, part, :, h * LAST : (h + 1) * LAST] for part in range(2)], axis=1
            )


def b_chunk(b_v, at, c):
    return b_v[at, 2 * c * CHUNK : 2 * (c + 1) * CHUNK]


def put(y_v, at, x):
    rows, width = x.shape[0], x.shape[1] // 2
    real = x[:, :width].astype(BF16)
    imag = x[:, width:].astype(BF16)
    y_v[at : at + rows, :width] = real
    y_v[at : at + rows, width:] = imag
    y_v[at + rows : at + 2 * rows, :width] = -imag
    y_v[at + rows : at + 2 * rows, width:] = real


def centre_plan(width):
    chunks, whole = width // CHUNK, slice(None)
    plan = [(whole, c * CHUNK, CHUNK) for c in range(chunks - 1)]
    plan += [(whole, width - CHUNK, CHUNK - LAST)]
    return plan + [(slice(c, c + 1), width - LAST, LAST) for c in range(chunks)]


def finish(centre, comes, cent, b_v, side_v, y_v, part_v, acc_v, out_ref):
    width = acc_v.shape[0]
    chunks = width // CHUNK
    plan = centre_plan(width)
    for n, (these, row, count) in enumerate(plan):
        rows = slice(row, row + count)
        final = n == len(plan) - 1
        complete = these == slice(None) or final
        for way in range(2):
            arrived(comes[way], centre[way][n])
            x = part_v[way, rows]
            for c in range(chunks)[these]:
                x = x + dot(cent(way, c, rows), b_chunk(b_v, (0, 2)[way], c))
            if complete:
                for h in range(count // LAST):
                    put(y_v, 4 * h * LAST + 2 * way * LAST, x[h * LAST : (h + 1) * LAST])
            else:
                part_v[way, rows] = x
        if complete and not final:
            total = acc_v[...]
            for h in range(count // LAST):
                total = total + dot(side_v[row // LAST + h], y_v[4 * h * LAST : 4 * (h + 1) * LAST])
            acc_v[...] = total
    for m in range(chunks):
        rows = slice(m * CHUNK, (m + 1) * CHUNK)
        total = acc_v[rows] + dot(side_v[width // LAST - 1, rows], y_v[: 4 * LAST])
        for part in range(2):
            out_ref[0, 0, part, rows] = total[:, part * width : (part + 1) * width]


def straight_kernel(
    slabs,
    energies,
    off_hbm,
    count_hbm,
    range_hbm,
    green_hbm,
    sigma_hbm,
    phonon_hbm,
    out_ref,
    off_ref,
    count_ref,
    range_ref,
    green_v,
    sigma_v,
    near_v,
    mine_v,
    got_v,
    b_v,
    a_v,
    side_v,
    y_v,
    part_v,
    acc_v,
    local_sem,
    near_send,
    near_recv,
    send_sem,
    recv_sem,
):
    k = lax.axis_index("slab")
    e = lax.axis_index("energy")
    width = green_v.shape[-1]
    slots = sigma_v.shape[0]
    chunks = width // CHUNK
    has_low, has_high = e > 0, e < energies - 1
    has_left, has_right = k > 0, k < slabs - 1
    goes, comes = (has_right, has_left), (has_left, has_right)

    tables = [
        pltpu.make_async_copy(source, held, local_sem.at[n])
        for n, (source, held) in enumerate(
            ((off_hbm, off_ref), (count_hbm, count_ref), (range_hbm, range_ref))
        )
    ]
    load_sigma = []
    for c in range(chunks):
        rows = slice(c * CHUNK, (c + 1) * CHUNK)
        load_sigma.append(
            pltpu.make_async_copy(
                sigma_hbm.at[0, 0, :, :, rows], sigma_v.at[:, :, rows], local_sem.at[4 + c]
            )
        )
    load_green = pltpu.make_async_copy(green_hbm.at[0, 0], green_v, local_sem.at[3])

    peers = (
        (has_left, {"slab": k - 1}),
        (has_right, {"slab": k + 1}),
        (has_low, {"energy": e - 1}),
        (has_high, {"energy": e + 1}),
    )
    greet(peers)
    for table in tables:
        table.start()
    for load in load_sigma:
        load.start()

    def near_copy(slot, target):
        return pltpu.make_async_remote_copy(
            src_ref=phonon_hbm.at[0, 0],
            dst_ref=near_v.at[slot],
            send_sem=near_send.at[slot],
            recv_sem=near_recv.at[slot],
            device_id={"energy": target},
            device_id_type=MESH,
        )

    up, down = near_copy(0, e + 1), near_copy(1, e - 1)

    whole = slice(None)
    plan = [(0, whole, c * CHUNK, CHUNK) for c in range(chunks)]
    plan += [(1, whole, 0, width)]
    first_centre = len(plan)
    plan += [(2,) + piece for piece in centre_plan(width)]
    sent = [[], []]
    for way in range(2):
        for n, (slot, these, row, count) in enumerate(plan):
            source = 4 if slot == 2 else 2 * way + slot
            sent[way].append(
                pltpu.make_async_remote_copy(
                    src_ref=mine_v.at[source, these, row : row + count],
                    dst_ref=got_v.at[way, slot, these, row : row + count],
                    send_sem=send_sem.at[way, n],
                    recv_sem=recv_sem.at[way, n],
                    device_id={"slab": (k + 1, k - 1)[way]},
                    device_id_type=MESH,
                )
            )

    def combine(at, offset, with_phonon, first=0, last=width // TILE):
        reach = []
        for q in range(slots):
            live = (q < count_ref[k]) & (off_ref[q, k] == offset)
            reach.append(jnp.where(live, range_ref[q, k], 0))

        def step(t, carry):
            rows = pl.ds(pl.multiple_of(t * TILE, TILE), TILE)
            col_ids = lax.broadcasted_iota(jnp.int32, (TILE, width), 1)
            inside = [col_ids < jnp.where(t * TILE < reach[q], reach[q], 0) for q in range(slots)]
            for part in range(2):
                kept = [
                    jnp.where(inside[q], sigma_v[q, part, rows, :].astype(F32), 0.0) for q in range(slots)
                ]
                total = functools.reduce(jnp.add, kept)
                if with_phonon:
                    low = near_v[0, part, rows, :].astype(F32)
                    high = near_v[1, part, rows, :].astype(F32)
                    total = total + (0.5 * (low + high)).astype(BF16).astype(F32)
                total = total.astype(BF16)
                for c in range(chunks):
                    mine_v[at, c, rows, part * CHUNK : (part + 1) * CHUNK] = total[
                        :, c * CHUNK : (c + 1) * CHUNK
                    ]
            return carry

        lax.fori_loop(first, last, step, 0)

    for table in tables:
        table.wait()
    tiles = CHUNK // TILE
    for c in range(chunks):
        load_sigma[c].wait()
        for way in range(2):
            combine(2 * way, (1, -1)[way], False, c * tiles, (c + 1) * tiles)
            if c == 0 and way == 0:
                greeted(peers)
            start(goes[way], sent[way][c])
        if c == 0:
            start(has_high, up)
            start(has_low, down)
    load_green.start()
    for way in range(2):
        combine(2 * way + 1, (2, -2)[way], False)
        start(goes[way], sent[way][chunks])

    for way in range(2):

        @pl.when(jnp.logical_not(comes[way]))
        def _():
            got_v[way] = jnp.zeros_like(got_v[way])

    for there, slot in ((has_low, 0), (has_high, 1)):

        @pl.when(jnp.logical_not(there))
        def _():
            near_v[slot] = jnp.zeros_like(near_v[slot])

    load_green.wait()
    prepare(green_v, b_v, a_v, side_v)

    arrived(has_low, up)
    arrived(has_high, down)
    combine(4, 0, True)
    for way in range(2):
        start(goes[way], *sent[way][first_centre:])

    for r in range(chunks):
        rows = slice(r * CHUNK, (r + 1) * CHUNK)
        x = None
        for at, partner in ((2, 0), (4, 1), (0, 2)):
            for c in range(chunks):
                term = dot(mine_v[at, c, rows], b_chunk(b_v, partner, c))
                x = term if x is None else x + term
        put(y_v, 0, x)
        term = dot(a_v[r], y_v[: 2 * CHUNK])
        acc_v[...] = term if r == 0 else acc_v[...] + term

    for slot in range(2):
        for way in range(2):
            arrived(comes[way], *sent[way][chunks * slot : chunks + slot])
            partner = ((1, 2), (1, 0))[way][slot]
            for r in range(chunks):
                rows = slice(r * CHUNK, (r + 1) * CHUNK)
                x = None
                for c in range(chunks):
                    term = dot(got_v[way, slot, c, rows], b_chunk(b_v, partner, c))
                    x = term if x is None else x + term
                part_v[way, rows] = x if slot == 0 else part_v[way, rows] + x
    centre = [copies[first_centre:] for copies in sent]
    finish(
        centre, comes, lambda way, c, rows: got_v[way, 2, c, rows], b_v, side_v, y_v, part_v, acc_v, out_ref
    )

    gone(has_high, up)
    gone(has_low, down)
    gone(has_right, *sent[0])
    gone(has_left, *sent[1])


def around_kernel(
    slabs,
    energies,
    off_hbm,
    count_hbm,
    range_hbm,
    green_hbm,
    sigma_hbm,
    phonon_hbm,
    out_ref,
    off_ref,
    count_ref,
    range_ref,
    green_v,
    sigma_v,
    near_v,
    mine_v,
    own_v,
    list_v,
    from_left_v,
    from_right_v,
    back_left_v,
    back_right_v,
    spill_v,
    cent_v,
    block_v,
    b_v,
    a_v,
    side_v,
    y_v,
    part_v,
    acc_v,
    local_sem,
    near_send,
    near_recv,
    unit_send,
    unit_recv,
    spill_send,
    spill_recv,
    back_send,
    back_recv,
    cent_send,
    cent_recv,
):
    k = lax.axis_index("slab")
    e = lax.axis_index("energy")
    width = green_v.shape[-1]
    slots = sigma_v.shape[0]
    chunks = width // CHUNK
    has_low, has_high = e > 0, e < energies - 1

    has_left, has_right = k > 0, k < slabs - 1

    tables = [
        pltpu.make_async_copy(source, held, local_sem.at[n])
        for n, (source, held) in enumerate(
            ((off_hbm, off_ref), (count_hbm, count_ref), (range_hbm, range_ref))
        )
    ]
    load_sigma = []
    for c in range(chunks):
        rows = slice(c * CHUNK, (c + 1) * CHUNK)
        load_sigma.append(
            pltpu.make_async_copy(
                sigma_hbm.at[0, 0, :, :, rows], sigma_v.at[:, :, rows], local_sem.at[4 + c]
            )
        )
    load_green = pltpu.make_async_copy(green_hbm.at[0, 0], green_v, local_sem.at[3])
    peers = (
        (has_left, {"slab": k - 1}),
        (has_right, {"slab": k + 1}),
        (has_low, {"energy": e - 1}),
        (has_high, {"energy": e + 1}),
        (k >= HOP, {"slab": k - HOP}),
        (k < slabs - HOP, {"slab": k + HOP}),
    )
    greet(peers)
    for table in tables:
        table.start()
    for load in load_sigma:
        load.start()

    def near_copy(slot, target):
        return pltpu.make_async_remote_copy(
            src_ref=phonon_hbm.at[0, 0],
            dst_ref=near_v.at[slot],
            send_sem=near_send.at[slot],
            recv_sem=near_recv.at[slot],
            device_id={"energy": target},
            device_id_type=MESH,
        )

    up, down = near_copy(0, e + 1), near_copy(1, e - 1)

    def remote(source, target, sent, received, slab):
        return pltpu.make_async_remote_copy(
            src_ref=source,
            dst_ref=target,
            send_sem=sent,
            recv_sem=received,
            device_id={"slab": slab},
            device_id_type=MESH,
        )

    sends = [detours(k, way, slabs) for way in range(2)]
    rides = [relayed(k, way) for way in range(2)]
    relays = [detours(rides[way], way, slabs) for way in range(2)]
    handed = [relayed(k + step, way) for way, step in ((0, -1), (1, 1))]
    hands = [there & detours(handed[way], way, slabs) for way, there in enumerate((has_left, has_right))]
    gets = [there & detours(k + step, way, slabs) for way, (there, step) in enumerate(((has_left, -1), (has_right, 1)))]
    beside = (k + 1, k - 1)
    goes, comes = (has_right, has_left), (has_left, has_right)
    got_v, back_v = (from_left_v, from_right_v), (back_left_v, back_right_v)
    units = (slice(0, 9), slice(12, 15), slice(9, 12), slice(15, 18))
    halves = (slice(0, GROUP), slice(GROUP, 2 * GROUP))
    direct, spill, returned, centre = [[], []], [[], []], [[], []], [[], []]
    for way in range(2):
        for n, these in enumerate(units):
            direct[way].append(
                remote(
                    list_v.at[way, these],
                    got_v[way].at[these],
                    unit_send.at[way, n],
                    unit_recv.at[way, n],
                    beside[way],
                )
            )
        for h, these in enumerate(halves):
            spill[way].append(
                remote(
                    list_v.at[way, DIRECT + h * GROUP : DIRECT + (h + 1) * GROUP],
                    spill_v.at[way, these],
                    spill_send.at[way, h],
                    spill_recv.at[way, h],
                    k + turned(k, way),
                )
            )
            returned[way].append(
                remote(
                    got_v[way].at[SHARED + h * GROUP : SHARED + (h + 1) * GROUP],
                    back_v[way].at[these],
                    back_send.at[way, h],
                    back_recv.at[way, h],
                    handed[way] + (1, -1)[way],
                )
            )
        for n, (these, row, count) in enumerate(centre_plan(width)):
            centre[way].append(
                remote(
                    own_v.at[these, row : row + count],
                    cent_v.at[way, these, row : row + count],
                    cent_send.at[way, n],
                    cent_recv.at[way, n],
                    beside[way],
                )
            )

    def live_reach(slab, q, offset):
        live = (q < count_ref[slab]) & (off_ref[q, slab] == offset)
        return jnp.where(live, range_ref[q, slab], 0)

    def combine(wanted, with_phonon, first=0, last=width // TILE):
        reach = [[live_reach(k, q, offset) for q in range(slots)] for _, offset in wanted]

        def step(t, carry):
            rows = pl.ds(pl.multiple_of(t * TILE, TILE), TILE)
            col_ids = lax.broadcasted_iota(jnp.int32, (TILE, width), 1)
            m = lax.div(t, UNIT // TILE)
            unit_rows = pl.ds(pl.multiple_of(t * TILE - m * UNIT, TILE), TILE)
            inside = [
                [col_ids < jnp.where(t * TILE < reach[n][q], reach[n][q], 0) for q in range(slots)]
                for n in range(len(wanted))
            ]
            for part in range(2):
                terms = [sigma_v[q, part, rows, :].astype(F32) for q in range(slots)]
                for n, (at, _) in enumerate(wanted):
                    kept = [jnp.where(inside[n][q], terms[q], 0.0) for q in range(slots)]
                    total = functools.reduce(jnp.add, kept)
                    if with_phonon:
                        low = near_v[0, part, rows, :].astype(F32)
                        high = near_v[1, part, rows, :].astype(F32)
                        total = total + (0.5 * (low + high)).astype(BF16).astype(F32)
                    total = total.astype(BF16)
                    lanes = slice(part * CHUNK, (part + 1) * CHUNK)
                    for c in range(chunks):
                        value = total[:, c * CHUNK : (c + 1) * CHUNK]
                        if with_phonon:
                            own_v[c, rows, lanes] = value
                        else:
                            mine_v[at, m, c, unit_rows, lanes] = value
            return carry

        lax.fori_loop(first, last, step, 0)

    def layout(slab, way):
        blocks = []
        for offset in OFFSETS[2 * way : 2 * way + 2]:
            reach = functools.reduce(jnp.maximum, [live_reach(slab, q, offset) for q in range(slots)])
            blocks.append(extent(reach))
        return blocks

    def pack(way, first, last):
        (_, across_a, size_a), (_, across_b, size_b) = layout(k, way)

        def step(p, carry):
            in_a = p < size_a
            unit = jnp.where(in_a, p, jnp.maximum(p - size_a, 0))
            across = jnp.where(in_a, across_a, across_b)
            row = jnp.where(across == 3, lax.div(unit, 3), jnp.where(across == 2, lax.div(unit, 2), unit))
            col = jnp.clip(unit - row * across, 0, chunks - 1)
            row = jnp.clip(row, 0, width // UNIT - 1)
            at = 2 * way + jnp.where(in_a, 0, 1)
            keep = jnp.where(p < size_a + size_b, 1.0, 0.0).astype(BF16)
            list_v[way, p] = mine_v[at, row, col] * keep
            return carry

        lax.fori_loop(first, last, step, 0)

    for table in tables:
        table.wait()
    tiles = width // TILE // chunks
    for way in range(2):
        wanted = [(2 * way + n, OFFSETS[2 * way + n]) for n in range(2)]
        if way == 0:
            for c in range(chunks):
                load_sigma[c].wait()
                combine(wanted, False, c * tiles, (c + 1) * tiles)
            load_green.start()
        else:
            combine(wanted, False)
        pack(way, 0, LIST)
        if way == 0:
            greeted(peers)
        start(sends[way], spill[way][0])
        start(goes[way], direct[way][0])
        if way == 0:
            start(has_high, up)
            start(has_low, down)
    for way in range(2):
        start(sends[way], spill[way][1])

    for way in range(2):

        @pl.when(jnp.logical_not(comes[way]))
        def _():
            got_v[way][...] = jnp.zeros_like(got_v[way])
            cent_v[way] = jnp.zeros_like(cent_v[way])

        @pl.when(jnp.logical_not(gets[way]))
        def _():
            back_v[way][...] = jnp.zeros_like(back_v[way])

        @pl.when(jnp.logical_not(relays[way]))
        def _():
            spill_v[way] = jnp.zeros_like(spill_v[way])

    for there, slot in ((has_low, 0), (has_high, 1)):

        @pl.when(jnp.logical_not(there))
        def _():
            near_v[slot] = jnp.zeros_like(near_v[slot])

    load_green.wait()
    prepare(green_v, b_v, a_v, side_v)

    arrived(has_low, up)
    arrived(has_high, down)
    combine([(4, 0)], True)

    def merge(h):
        for way in range(2):
            arrived(relays[way], spill[way][h])
            for j in range(h * GROUP, (h + 1) * GROUP):
                list_v[way, SHARED + j] = list_v[way, SHARED + j] + spill_v[way, j]

    merge(0)
    for way in range(2):
        start(goes[way], direct[way][1], direct[way][2])

    for n, (at, partner) in enumerate(((2, 0), (0, 2))):
        for r in range(2):
            rows = slice(r * width // 2, (r + 1) * width // 2)
            these = slice(rows.start // UNIT, rows.stop // UNIT)
            x = None
            for c in range(chunks):
                term = dot(mine_v[at, these, c].reshape(width // 2, 2 * CHUNK), b_chunk(b_v, partner, c))
                x = term if x is None else x + term
            part_v[0, rows] = x if n == 0 else part_v[0, rows] + x
    for r in range(chunks):
        rows = slice(r * CHUNK, (r + 1) * CHUNK)
        x = part_v[0, rows]
        for c in range(chunks):
            x = x + dot(own_v[c, rows], b_chunk(b_v, 1, c))
        put(y_v, 0, x)
        term = dot(a_v[r], y_v[: 2 * CHUNK])
        acc_v[...] = term if r == 0 else acc_v[...] + term

    merge(1)
    for way in range(2):
        start(goes[way], direct[way][3], *centre[way])
    for n, h in ((1, 0), (3, 1)):
        for way in range(2):
            arrived(comes[way], direct[way][n])
            start(hands[way], returned[way][h])

    def multiply(way, source, first, last, down_n, across_n, before, partner, fresh):
        for m in range(width // UNIT):
            for c in range(chunks):
                position = before + m * across_n + c
                there = (m < down_n) & (c < across_n) & (position >= first) & (position < last)
                keep = jnp.where(there, 1.0, 0.0).astype(BF16)
                position = jnp.clip(position - first, 0, last - first - 1)
                block_v[c, m * UNIT : (m + 1) * UNIT] = source[position] * keep
        for r in range(chunks):
            rows = slice(r * CHUNK, (r + 1) * CHUNK)
            x = None
            for c in range(chunks):
                term = dot(block_v[c, rows], b_chunk(b_v, partner, c))
                x = term if x is None else x + term
            part_v[way, rows] = x if fresh else part_v[way, rows] + x

    blocks = [
        layout(jnp.maximum(k - 1, 0), 0),
        layout(jnp.minimum(k + 1, slabs - 1), 1),
    ]
    for way in range(2):
        (down_a, across_a, size_a), (down_b, across_b, _) = blocks[way]
        partner_a, partner_b = ((1, 2), (1, 0))[way]
        arrived(comes[way], direct[way][0], direct[way][2])
        multiply(way, got_v[way], 0, DIRECT, down_a, across_a, 0, partner_a, True)
        multiply(way, got_v[way], 0, DIRECT, down_b, across_b, size_a, partner_b, False)
    for way in range(2):
        (_, _, size_a), (down_b, across_b, _) = blocks[way]
        partner_b = (2, 0)[way]
        arrived(gets[way], *returned[way])
        multiply(way, back_v[way], DIRECT, LIST, down_b, across_b, size_a, partner_b, False)

    finish(
        centre, comes, lambda way, c, rows: cent_v[way, c, rows], b_v, side_v, y_v, part_v, acc_v, out_ref
    )

    gone(has_high, up)
    gone(has_low, down)
    for way in range(2):
        gone(goes[way], *direct[way], *centre[way])
        gone(sends[way], *spill[way])
        gone(hands[way], *returned[way])


def solution(mesh):
    slabs, energies = mesh.shape["slab"], mesh.shape["energy"]

    def body(green, sigma, phonon, pair_off, pair_count, pair_range):
        width = green.shape[-1]
        slots = sigma.shape[2]
        chunks = width // CHUNK
        pieces = len(centre_plan(width))
        hbm = pl.BlockSpec(memory_space=pltpu.HBM)
        vmem = pl.BlockSpec(memory_space=pltpu.VMEM)
        split = (chunks, width, 2 * CHUNK)
        unit = (UNIT, 2 * CHUNK)
        operands = (pair_off.T, pair_count, pair_range.T, green, sigma, phonon)
        operands = [pltpu.with_memory_space_constraint(v, pltpu.HBM) for v in operands]
        taken = [
            pltpu.SMEM((slots, slabs), jnp.int32),
            pltpu.SMEM((slabs,), jnp.int32),
            pltpu.SMEM((slots, slabs), jnp.int32),
            pltpu.VMEM((3, 2, width, width), BF16),
            pltpu.VMEM((slots, 2, width, width), BF16),
            pltpu.VMEM((2, 2, width, width), BF16),
        ]
        factors = [
            pltpu.VMEM((3, 2 * width, 2 * width), BF16),
            pltpu.VMEM(split, BF16),
            pltpu.VMEM((width // LAST, width, 4 * LAST), BF16),
            pltpu.VMEM((4 * CHUNK, 2 * width), BF16),
            pltpu.VMEM((2, width, 2 * width), F32),
            pltpu.VMEM((width, 2 * width), F32),
            pltpu.SemaphoreType.DMA((4 + chunks,)),
            pltpu.SemaphoreType.DMA((2,)),
            pltpu.SemaphoreType.DMA((2,)),
        ]

        def flags(count):
            return [pltpu.SemaphoreType.DMA((2, count))] * 2

        def call(what, number, name, blocks, semaphores, *operands):
            return pl.pallas_call(
                functools.partial(what, slabs, energies),
                out_shape=jax.ShapeDtypeStruct((1, 1, 2, width, width), F32),
                in_specs=[hbm] * 6,
                out_specs=vmem,
                scratch_shapes=taken + blocks + factors + semaphores,
                compiler_params=pltpu.CompilerParams(
                    collective_id=number, has_side_effects=True, vmem_limit_bytes=48 * 1024 * 1024
                ),
                name=name,
            )(*operands)

        straight = functools.partial(
            call,
            straight_kernel,
            0,
            "straight",
            [pltpu.VMEM((5,) + split, BF16), pltpu.VMEM((2, 3) + split, BF16)],
            flags(chunks + 1 + pieces),
        )
        around = functools.partial(
            call,
            around_kernel,
            1,
            "around",
            [
                pltpu.VMEM((4, width // UNIT, chunks) + unit, BF16),
                pltpu.VMEM(split, BF16),
                pltpu.VMEM((2, LIST) + unit, BF16),
                pltpu.VMEM((DIRECT,) + unit, BF16),
                pltpu.VMEM((DIRECT,) + unit, BF16),
                pltpu.VMEM((LIST - DIRECT,) + unit, BF16),
                pltpu.VMEM((LIST - DIRECT,) + unit, BF16),
                pltpu.VMEM((2, LIST - DIRECT) + unit, BF16),
                pltpu.VMEM((2,) + split, BF16),
                pltpu.VMEM(split, BF16),
            ],
            flags(4) + flags(2) + flags(2) + flags(pieces),
        )
        crowded = pl.pallas_call(
            crowded_kernel,
            out_shape=jax.ShapeDtypeStruct((1,), jnp.int32),
            in_specs=[vmem] * 3,
            out_specs=pl.BlockSpec(memory_space=pltpu.SMEM),
            name="crowded",
        )(pair_off.T, pair_count[None], pair_range.T)
        return lax.cond(crowded[0] > 0, straight, around, *operands)

    wide = P("energy", "slab", None, None, None, None)
    slim = P("energy", "slab", None, None, None)
    return jax.shard_map(
        body,
        mesh=mesh,
        in_specs=(wide, wide, slim, P(), P(), P()),
        out_specs=slim,
        check_vma=False,
    )
```

```python
import functools

import jax
import jax.numpy as jnp
from jax import lax
from jax.experimental import pallas as pl
from jax.experimental.pallas import tpu as pltpu
from jax.sharding import PartitionSpec as P

MESH = pl.DeviceIdType.MESH
F32 = jnp.float32
BF16 = jnp.bfloat16
TILE = 16
CHUNK = 128
LAST = 64
UNIT = 96
GROUP = 3
LIST = 24
DIRECT = 18
SHARED = 12
HOP = 4
OFFSETS = (1, 2, -1, -2)


def extent(reach):
    steps = [(reach >= n * UNIT).astype(jnp.int32) for n in range(1, 5)]
    down = steps[0] + steps[1] + steps[2] + steps[3]
    across = steps[0] + steps[1] + steps[2]
    return down, across, down * across


def turned(slab, way):
    place = lax.rem(slab, HOP)
    paired = jnp.where(lax.rem(lax.div(slab, HOP), 2) == 0, HOP, -HOP)
    if way == 0:
        return jnp.where(place == HOP - 1, -HOP, jnp.where(place == 1, paired, HOP))
    return jnp.where(place == 0, HOP, jnp.where(place == 2, paired, -HOP))


def detours(slab, way, slabs):
    low, high = (0, slabs - 2) if way == 0 else (1, slabs - 1)
    relay = slab + turned(slab, way)
    return (slab >= low) & (slab <= high) & (relay >= low) & (relay <= high)


def relayed(relay, way):
    turn = turned(relay, way)
    return relay + jnp.where(lax.rem(relay, HOP) == 1 + way, turn, -turn)


def crowded_kernel(off_ref, count_ref, range_ref, out_ref):
    off, reach = off_ref[...], range_ref[...]
    slots, slabs = off.shape
    live = lax.broadcasted_iota(jnp.int32, off.shape, 0) < count_ref[...]
    slab = lax.broadcasted_iota(jnp.int32, (1, slabs), 1)
    crowded = jnp.zeros((1, slabs), F32)
    for way in range(2):
        filled = jnp.zeros((1, slabs), jnp.int32)
        for offset in OFFSETS[2 * way : 2 * way + 2]:
            widest = jnp.max(jnp.where(live & (off == offset), reach, 0), axis=0, keepdims=True)
            filled = filled + extent(widest)[2]
        above = jnp.concatenate([filled[:, HOP:], filled[:, :HOP]], axis=1)
        below = jnp.concatenate([filled[:, -HOP:], filled[:, :-HOP]], axis=1)
        relay = jnp.where(turned(slab, way) > 0, above, below)
        room = jnp.where(filled > DIRECT + GROUP, SHARED, SHARED + GROUP)
        stuck = (relay > room) | jnp.logical_not(detours(slab, way, slabs))
        crowded = crowded + ((filled > DIRECT) & stuck).astype(F32)
    out_ref[0] = jnp.max(crowded).astype(jnp.int32)


def dot(a, b):
    return jnp.dot(a, b, preferred_element_type=F32)


def start(there, *copies):
    @pl.when(there)
    def _():
        for copy in copies:
            copy.start()


def arrived(there, *copies):
    @pl.when(there)
    def _():
        for copy in copies:
            copy.wait_recv()


def gone(there, *copies):
    @pl.when(there)
    def _():
        for copy in copies:
            copy.wait_send()


def greet(peers):
    barrier = pltpu.get_barrier_semaphore()
    for there, who in peers:

        @pl.when(there)
        def _():
            pl.semaphore_signal(barrier, inc=1, device_id=who, device_id_type=MESH)


def greeted(peers):
    barrier = pltpu.get_barrier_semaphore()
    pl.semaphore_wait(barrier, sum(there.astype(jnp.int32) for there, _ in peers))


def prepare(green_v, b_v, a_v, side_v):
    width = green_v.shape[-1]
    for at in range(3):
        for part in range(2):
            flipped = green_v[at, part].astype(F32).T
            plain = flipped.astype(BF16)
            minus = (-flipped).astype(BF16)
            for c in range(width // CHUNK):
                source = slice(c * CHUNK, (c + 1) * CHUNK)
                real = slice(2 * c * CHUNK, (2 * c + 1) * CHUNK)
                imag = slice((2 * c + 1) * CHUNK, (2 * c + 2) * CHUNK)
                if part == 0:
                    b_v[at, real, :width] = plain[source]
                    b_v[at, imag, width:] = plain[source]
                else:
                    b_v[at, real, width:] = minus[source]
                    b_v[at, imag, :width] = plain[source]
    for c in range(width // CHUNK):
        for part in range(2):
            a_v[c, :, part * CHUNK : (part + 1) * CHUNK] = green_v[1, part, :, c * CHUNK : (c + 1) * CHUNK]
    for h in range(width // LAST):
        for n, at in enumerate((0, 2)):
            side_v[h, :, 2 * n * LAST : 2 * (n + 1) * LAST] = jnp.concatenate(
                [green_v[at, part, :, h * LAST : (h + 1) * LAST] for part in range(2)], axis=1
            )


def b_chunk(b_v, at, c):
    return b_v[at, 2 * c * CHUNK : 2 * (c + 1) * CHUNK]


def put(y_v, at, x):
    rows, width = x.shape[0], x.shape[1] // 2
    real = x[:, :width].astype(BF16)
    imag = x[:, width:].astype(BF16)
    y_v[at : at + rows, :width] = real
    y_v[at : at + rows, width:] = imag
    y_v[at + rows : at + 2 * rows, :width] = -imag
    y_v[at + rows : at + 2 * rows, width:] = real


def centre_plan(width):
    whole, half, most = slice(None), width // 2, width - LAST
    plan = [(whole, 0, CHUNK), (whole, CHUNK, half - CHUNK), (whole, half, most - half)]
    return plan + [(slice(c, c + 1), most, LAST) for c in range(width // CHUNK)]


def finish(centre, comes, cent, late, b_v, side_v, y_v, part_v, acc_v, out_ref):
    width = acc_v.shape[0]
    chunks = width // CHUNK
    plan = centre_plan(width)
    for n, (these, row, count) in enumerate(plan):
        rows = slice(row, row + count)
        final = n == len(plan) - 1
        complete = these == slice(None) or final
        if row == width // 2:
            late()
        for way in range(2):
            arrived(comes[way], centre[way][n])
            x = part_v[way, rows]
            for c in range(chunks)[these]:
                x = x + dot(cent(way, c, rows), b_chunk(b_v, (0, 2)[way], c))
            if complete:
                for h in range(count // LAST):
                    put(y_v, 4 * h * LAST + 2 * way * LAST, x[h * LAST : (h + 1) * LAST])
            else:
                part_v[way, rows] = x
        if complete and not final:
            total = acc_v[...]
            for h in range(count // LAST):
                total = total + dot(side_v[row // LAST + h], y_v[4 * h * LAST : 4 * (h + 1) * LAST])
            acc_v[...] = total
    for m in range(chunks):
        rows = slice(m * CHUNK, (m + 1) * CHUNK)
        total = acc_v[rows] + dot(side_v[width // LAST - 1, rows], y_v[: 4 * LAST])
        for part in range(2):
            out_ref[0, 0, part, rows] = total[:, part * width : (part + 1) * width]


def straight_kernel(
    slabs,
    energies,
    off_hbm,
    count_hbm,
    range_hbm,
    green_hbm,
    sigma_hbm,
    phonon_hbm,
    out_ref,
    off_ref,
    count_ref,
    range_ref,
    green_v,
    sigma_v,
    near_v,
    mine_v,
    got_v,
    b_v,
    a_v,
    side_v,
    y_v,
    part_v,
    acc_v,
    local_sem,
    near_send,
    near_recv,
    send_sem,
    recv_sem,
):
    k = lax.axis_index("slab")
    e = lax.axis_index("energy")
    width = green_v.shape[-1]
    slots = sigma_v.shape[0]
    chunks = width // CHUNK
    has_low, has_high = e > 0, e < energies - 1
    has_left, has_right = k > 0, k < slabs - 1
    goes, comes = (has_right, has_left), (has_left, has_right)

    tables = [
        pltpu.make_async_copy(source, held, local_sem.at[n])
        for n, (source, held) in enumerate(
            ((off_hbm, off_ref), (count_hbm, count_ref), (range_hbm, range_ref))
        )
    ]
    load_sigma = []
    for c in range(chunks):
        rows = slice(c * CHUNK, (c + 1) * CHUNK)
        load_sigma.append(
            pltpu.make_async_copy(
                sigma_hbm.at[0, 0, :, :, rows], sigma_v.at[:, :, rows], local_sem.at[4 + c]
            )
        )
    load_green = pltpu.make_async_copy(green_hbm.at[0, 0], green_v, local_sem.at[3])

    peers = (
        (has_left, {"slab": k - 1}),
        (has_right, {"slab": k + 1}),
        (has_low, {"energy": e - 1}),
        (has_high, {"energy": e + 1}),
    )
    greet(peers)
    for table in tables:
        table.start()
    for load in load_sigma:
        load.start()

    def near_copy(slot, target):
        return pltpu.make_async_remote_copy(
            src_ref=phonon_hbm.at[0, 0],
            dst_ref=near_v.at[slot],
            send_sem=near_send.at[slot],
            recv_sem=near_recv.at[slot],
            device_id={"energy": target},
            device_id_type=MESH,
        )

    up, down = near_copy(0, e + 1), near_copy(1, e - 1)

    whole = slice(None)
    plan = [(0, whole, c * CHUNK, CHUNK) for c in range(chunks)]
    plan += [(1, whole, 0, width)]
    first_centre = len(plan)
    plan += [(2,) + piece for piece in centre_plan(width)]
    sent = [[], []]
    for way in range(2):
        for n, (slot, these, row, count) in enumerate(plan):
            source = 4 if slot == 2 else 2 * way + slot
            sent[way].append(
                pltpu.make_async_remote_copy(
                    src_ref=mine_v.at[source, these, row : row + count],
                    dst_ref=got_v.at[way, slot, these, row : row + count],
                    send_sem=send_sem.at[way, n],
                    recv_sem=recv_sem.at[way, n],
                    device_id={"slab": (k + 1, k - 1)[way]},
                    device_id_type=MESH,
                )
            )

    def combine(at, offset, with_phonon, first=0, last=width // TILE):
        reach = []
        for q in range(slots):
            live = (q < count_ref[k]) & (off_ref[q, k] == offset)
            reach.append(jnp.where(live, range_ref[q, k], 0))

        def step(t, carry):
            rows = pl.ds(pl.multiple_of(t * TILE, TILE), TILE)
            col_ids = lax.broadcasted_iota(jnp.int32, (TILE, width), 1)
            inside = [col_ids < jnp.where(t * TILE < reach[q], reach[q], 0) for q in range(slots)]
            for part in range(2):
                kept = [
                    jnp.where(inside[q], sigma_v[q, part, rows, :].astype(F32), 0.0) for q in range(slots)
                ]
                total = functools.reduce(jnp.add, kept)
                if with_phonon:
                    low = near_v[0, part, rows, :].astype(F32)
                    high = near_v[1, part, rows, :].astype(F32)
                    total = total + (0.5 * (low + high)).astype(BF16).astype(F32)
                total = total.astype(BF16)
                for c in range(chunks):
                    mine_v[at, c, rows, part * CHUNK : (part + 1) * CHUNK] = total[
                        :, c * CHUNK : (c + 1) * CHUNK
                    ]
            return carry

        lax.fori_loop(first, last, step, 0, unroll=4)

    for table in tables:
        table.wait()
    tiles = CHUNK // TILE
    for c in range(chunks):
        load_sigma[c].wait()
        for way in range(2):
            combine(2 * way, (1, -1)[way], False, c * tiles, (c + 1) * tiles)
            if c == 0 and way == 0:
                greeted(peers)
            start(goes[way], sent[way][c])
        if c == 0:
            start(has_high, up)
            start(has_low, down)
    load_green.start()
    for way in range(2):
        combine(2 * way + 1, (2, -2)[way], False)
        start(goes[way], sent[way][chunks])

    for way in range(2):

        @pl.when(jnp.logical_not(comes[way]))
        def _():
            got_v[way] = jnp.zeros_like(got_v[way])

    for there, slot in ((has_low, 0), (has_high, 1)):

        @pl.when(jnp.logical_not(there))
        def _():
            near_v[slot] = jnp.zeros_like(near_v[slot])

    load_green.wait()
    prepare(green_v, b_v, a_v, side_v)

    arrived(has_low, up)
    arrived(has_high, down)
    combine(4, 0, True)
    for way in range(2):
        start(goes[way], *sent[way][first_centre:])

    for r in range(chunks):
        rows = slice(r * CHUNK, (r + 1) * CHUNK)
        x = None
        for at, partner in ((2, 0), (4, 1), (0, 2)):
            for c in range(chunks):
                term = dot(mine_v[at, c, rows], b_chunk(b_v, partner, c))
                x = term if x is None else x + term
        put(y_v, 0, x)
        term = dot(a_v[r], y_v[: 2 * CHUNK])
        acc_v[...] = term if r == 0 else acc_v[...] + term

    for slot in range(2):
        for way in range(2):
            arrived(comes[way], *sent[way][chunks * slot : chunks + slot])
            partner = ((1, 2), (1, 0))[way][slot]
            for r in range(chunks):
                rows = slice(r * CHUNK, (r + 1) * CHUNK)
                x = None
                for c in range(chunks):
                    term = dot(got_v[way, slot, c, rows], b_chunk(b_v, partner, c))
                    x = term if x is None else x + term
                part_v[way, rows] = x if slot == 0 else part_v[way, rows] + x
    centre = [copies[first_centre:] for copies in sent]
    finish(
        centre,
        comes,
        lambda way, c, rows: got_v[way, 2, c, rows],
        lambda: None,
        b_v,
        side_v,
        y_v,
        part_v,
        acc_v,
        out_ref,
    )

    gone(has_high, up)
    gone(has_low, down)
    gone(has_right, *sent[0])
    gone(has_left, *sent[1])


def around_kernel(
    slabs,
    energies,
    off_hbm,
    count_hbm,
    range_hbm,
    green_hbm,
    sigma_hbm,
    phonon_hbm,
    out_ref,
    off_ref,
    count_ref,
    range_ref,
    green_v,
    sigma_v,
    near_v,
    mine_v,
    own_v,
    list_v,
    from_left_v,
    from_right_v,
    back_left_v,
    back_right_v,
    spill_v,
    cent_v,
    block_v,
    b_v,
    a_v,
    side_v,
    y_v,
    part_v,
    acc_v,
    local_sem,
    near_send,
    near_recv,
    unit_send,
    unit_recv,
    spill_send,
    spill_recv,
    back_send,
    back_recv,
    cent_send,
    cent_recv,
):
    k = lax.axis_index("slab")
    e = lax.axis_index("energy")
    width = green_v.shape[-1]
    slots = sigma_v.shape[0]
    chunks = width // CHUNK
    has_low, has_high = e > 0, e < energies - 1

    has_left, has_right = k > 0, k < slabs - 1

    tables = [
        pltpu.make_async_copy(source, held, local_sem.at[n])
        for n, (source, held) in enumerate(
            ((off_hbm, off_ref), (count_hbm, count_ref), (range_hbm, range_ref))
        )
    ]
    load_sigma = []
    for c in range(chunks):
        rows = slice(c * CHUNK, (c + 1) * CHUNK)
        load_sigma.append(
            pltpu.make_async_copy(
                sigma_hbm.at[0, 0, :, :, rows], sigma_v.at[:, :, rows], local_sem.at[4 + c]
            )
        )
    load_green = pltpu.make_async_copy(green_hbm.at[0, 0], green_v, local_sem.at[3])
    peers = (
        (has_left, {"slab": k - 1}),
        (has_right, {"slab": k + 1}),
        (has_low, {"energy": e - 1}),
        (has_high, {"energy": e + 1}),
        (k >= HOP, {"slab": k - HOP}),
        (k < slabs - HOP, {"slab": k + HOP}),
    )
    greet(peers)
    for table in tables:
        table.start()
    for load in load_sigma:
        load.start()

    def near_copy(slot, target):
        return pltpu.make_async_remote_copy(
            src_ref=phonon_hbm.at[0, 0],
            dst_ref=near_v.at[slot],
            send_sem=near_send.at[slot],
            recv_sem=near_recv.at[slot],
            device_id={"energy": target},
            device_id_type=MESH,
        )

    up, down = near_copy(0, e + 1), near_copy(1, e - 1)

    def remote(source, target, sent, received, slab):
        return pltpu.make_async_remote_copy(
            src_ref=source,
            dst_ref=target,
            send_sem=sent,
            recv_sem=received,
            device_id={"slab": slab},
            device_id_type=MESH,
        )

    sends = [detours(k, way, slabs) for way in range(2)]
    rides = [relayed(k, way) for way in range(2)]
    relays = [detours(rides[way], way, slabs) for way in range(2)]
    handed = [relayed(k + step, way) for way, step in ((0, -1), (1, 1))]
    hands = [there & detours(handed[way], way, slabs) for way, there in enumerate((has_left, has_right))]
    gets = [there & detours(k + step, way, slabs) for way, (there, step) in enumerate(((has_left, -1), (has_right, 1)))]
    beside = (k + 1, k - 1)
    goes, comes = (has_right, has_left), (has_left, has_right)
    got_v, back_v = (from_left_v, from_right_v), (back_left_v, back_right_v)
    units = (slice(0, 9), slice(12, 15), slice(9, 12), slice(15, 18))
    halves = (slice(0, GROUP), slice(GROUP, 2 * GROUP))
    direct, spill, returned, centre = [[], []], [[], []], [[], []], [[], []]
    for way in range(2):
        for n, these in enumerate(units):
            direct[way].append(
                remote(
                    list_v.at[way, these],
                    got_v[way].at[these],
                    unit_send.at[way, n],
                    unit_recv.at[way, n],
                    beside[way],
                )
            )
        for h, these in enumerate(halves):
            spill[way].append(
                remote(
                    list_v.at[way, LIST - (h + 1) * GROUP : LIST - h * GROUP],
                    spill_v.at[way, these],
                    spill_send.at[way, h],
                    spill_recv.at[way, h],
                    k + turned(k, way),
                )
            )
            returned[way].append(
                remote(
                    got_v[way].at[SHARED + h * GROUP : SHARED + (h + 1) * GROUP],
                    back_v[way].at[halves[1 - h]],
                    back_send.at[way, h],
                    back_recv.at[way, h],
                    handed[way] + (1, -1)[way],
                )
            )
        for n, (these, row, count) in enumerate(centre_plan(width)):
            centre[way].append(
                remote(
                    own_v.at[these, row : row + count],
                    cent_v.at[way, these, row : row + count],
                    cent_send.at[way, n],
                    cent_recv.at[way, n],
                    beside[way],
                )
            )

    def live_reach(slab, q, offset):
        live = (q < count_ref[slab]) & (off_ref[q, slab] == offset)
        return jnp.where(live, range_ref[q, slab], 0)

    def combine(wanted, with_phonon, first=0, last=width // TILE):
        reach = [[live_reach(k, q, offset) for q in range(slots)] for _, offset in wanted]

        def step(t, carry):
            rows = pl.ds(pl.multiple_of(t * TILE, TILE), TILE)
            col_ids = lax.broadcasted_iota(jnp.int32, (TILE, width), 1)
            m = lax.div(t, UNIT // TILE)
            unit_rows = pl.ds(pl.multiple_of(t * TILE - m * UNIT, TILE), TILE)
            inside = [
                [col_ids < jnp.where(t * TILE < reach[n][q], reach[n][q], 0) for q in range(slots)]
                for n in range(len(wanted))
            ]
            for part in range(2):
                terms = [sigma_v[q, part, rows, :].astype(F32) for q in range(slots)]
                for n, (at, _) in enumerate(wanted):
                    kept = [jnp.where(inside[n][q], terms[q], 0.0) for q in range(slots)]
                    total = functools.reduce(jnp.add, kept)
                    if with_phonon:
                        low = near_v[0, part, rows, :].astype(F32)
                        high = near_v[1, part, rows, :].astype(F32)
                        total = total + (0.5 * (low + high)).astype(BF16).astype(F32)
                    total = total.astype(BF16)
                    lanes = slice(part * CHUNK, (part + 1) * CHUNK)
                    for c in range(chunks):
                        value = total[:, c * CHUNK : (c + 1) * CHUNK]
                        if with_phonon:
                            own_v[c, rows, lanes] = value
                        else:
                            mine_v[at, m, c, unit_rows, lanes] = value
            return carry

        lax.fori_loop(first, last, step, 0, unroll=4)

    def layout(slab, way):
        blocks = []
        for offset in OFFSETS[2 * way : 2 * way + 2]:
            reach = functools.reduce(jnp.maximum, [live_reach(slab, q, offset) for q in range(slots)])
            blocks.append(extent(reach))
        return blocks

    def pack(way, first, last):
        (_, across_a, size_a), (_, across_b, size_b) = layout(k, way)

        def step(p, carry):
            in_a = p < size_a
            unit = jnp.where(in_a, p, jnp.maximum(p - size_a, 0))
            across = jnp.where(in_a, across_a, across_b)
            row = jnp.where(across == 3, lax.div(unit, 3), jnp.where(across == 2, lax.div(unit, 2), unit))
            col = jnp.clip(unit - row * across, 0, chunks - 1)
            row = jnp.clip(row, 0, width // UNIT - 1)
            at = 2 * way + jnp.where(in_a, 0, 1)
            keep = jnp.where(p < size_a + size_b, 1.0, 0.0).astype(BF16)
            list_v[way, p] = mine_v[at, row, col] * keep
            return carry

        lax.fori_loop(first, last, step, 0, unroll=4)

    for table in tables:
        table.wait()
    tiles = width // TILE // chunks
    for way in range(2):
        wanted = [(2 * way + n, OFFSETS[2 * way + n]) for n in range(2)]
        if way == 0:
            for c in range(chunks):
                load_sigma[c].wait()
                combine(wanted, False, c * tiles, (c + 1) * tiles)
            load_green.start()
        else:
            combine(wanted, False)
        pack(way, 0, LIST)
        if way == 0:
            greeted(peers)
        start(sends[way], spill[way][0])
        start(goes[way], direct[way][0])
        if way == 0:
            start(has_high, up)
            start(has_low, down)
    for way in range(2):
        start(sends[way], spill[way][1])

    for way in range(2):

        @pl.when(jnp.logical_not(comes[way]))
        def _():
            got_v[way][...] = jnp.zeros_like(got_v[way])
            cent_v[way] = jnp.zeros_like(cent_v[way])

        @pl.when(jnp.logical_not(gets[way]))
        def _():
            back_v[way][...] = jnp.zeros_like(back_v[way])

        @pl.when(jnp.logical_not(relays[way]))
        def _():
            spill_v[way] = jnp.zeros_like(spill_v[way])

    for there, slot in ((has_low, 0), (has_high, 1)):

        @pl.when(jnp.logical_not(there))
        def _():
            near_v[slot] = jnp.zeros_like(near_v[slot])

    load_green.wait()
    prepare(green_v, b_v, a_v, side_v)

    arrived(has_low, up)
    arrived(has_high, down)
    combine([(4, 0)], True)

    def merge(h):
        for way in range(2):
            arrived(relays[way], spill[way][h])
            for j in range(h * GROUP, (h + 1) * GROUP):
                list_v[way, SHARED + j] = list_v[way, SHARED + j] + spill_v[way, j]

    merge(0)
    for way in range(2):
        start(goes[way], direct[way][1], direct[way][2])

    for n, (at, partner) in enumerate(((2, 0), (0, 2))):
        for r in range(2):
            rows = slice(r * width // 2, (r + 1) * width // 2)
            these = slice(rows.start // UNIT, rows.stop // UNIT)
            x = None
            for c in range(chunks):
                term = dot(mine_v[at, these, c].reshape(width // 2, 2 * CHUNK), b_chunk(b_v, partner, c))
                x = term if x is None else x + term
            part_v[0, rows] = x if n == 0 else part_v[0, rows] + x
    for r in range(chunks):
        rows = slice(r * CHUNK, (r + 1) * CHUNK)
        x = part_v[0, rows]
        for c in range(chunks):
            x = x + dot(own_v[c, rows], b_chunk(b_v, 1, c))
        put(y_v, 0, x)
        term = dot(a_v[r], y_v[: 2 * CHUNK])
        acc_v[...] = term if r == 0 else acc_v[...] + term

    merge(1)
    for way in range(2):
        start(goes[way], direct[way][3], *centre[way])
    for n, h in ((1, 0), (3, 1)):
        for way in range(2):
            arrived(comes[way], direct[way][n])
            start(hands[way], returned[way][h])

    def multiply(way, source, first, last, down_n, across_n, before, partner, fresh, top=0):
        for m in range(top // UNIT, width // UNIT):
            for c in range(chunks):
                position = before + m * across_n + c
                there = (m < down_n) & (c < across_n) & (position >= first) & (position < last)
                keep = jnp.where(there, 1.0, 0.0).astype(BF16)
                position = jnp.clip(position - first, 0, last - first - 1)
                block_v[c, m * UNIT : (m + 1) * UNIT] = source[position] * keep
        for row in range(top, width, width // 2):
            rows = slice(row, row + width // 2)
            x = None
            for c in range(chunks):
                term = dot(block_v[c, rows], b_chunk(b_v, partner, c))
                x = term if x is None else x + term
            part_v[way, rows] = x if fresh else part_v[way, rows] + x

    blocks = [
        layout(jnp.maximum(k - 1, 0), 0),
        layout(jnp.minimum(k + 1, slabs - 1), 1),
    ]
    for way in range(2):
        (down_a, across_a, size_a), (down_b, across_b, _) = blocks[way]
        partner_a, partner_b = ((1, 2), (1, 0))[way]
        arrived(comes[way], direct[way][0], direct[way][2])
        multiply(way, got_v[way], 0, DIRECT, down_a, across_a, 0, partner_a, True)
        multiply(way, got_v[way], 0, DIRECT, down_b, across_b, size_a, partner_b, False)

    def late():
        for way in range(2):
            (_, _, size_a), (down_b, across_b, _) = blocks[way]
            arrived(gets[way], *returned[way])
            multiply(
                way, back_v[way], DIRECT, LIST, down_b, across_b, size_a, (2, 0)[way], False, width // 2
            )

    finish(
        centre,
        comes,
        lambda way, c, rows: cent_v[way, c, rows],
        late,
        b_v,
        side_v,
        y_v,
        part_v,
        acc_v,
        out_ref,
    )

    gone(has_high, up)
    gone(has_low, down)
    for way in range(2):
        gone(goes[way], *direct[way], *centre[way])
        gone(sends[way], *spill[way])
        gone(hands[way], *returned[way])


def solution(mesh):
    slabs, energies = mesh.shape["slab"], mesh.shape["energy"]

    def body(green, sigma, phonon, pair_off, pair_count, pair_range):
        width = green.shape[-1]
        slots = sigma.shape[2]
        chunks = width // CHUNK
        pieces = len(centre_plan(width))
        hbm = pl.BlockSpec(memory_space=pltpu.HBM)
        vmem = pl.BlockSpec(memory_space=pltpu.VMEM)
        split = (chunks, width, 2 * CHUNK)
        unit = (UNIT, 2 * CHUNK)
        operands = (pair_off.T, pair_count, pair_range.T, green, sigma, phonon)
        operands = [pltpu.with_memory_space_constraint(v, pltpu.HBM) for v in operands]
        taken = [
            pltpu.SMEM((slots, slabs), jnp.int32),
            pltpu.SMEM((slabs,), jnp.int32),
            pltpu.SMEM((slots, slabs), jnp.int32),
            pltpu.VMEM((3, 2, width, width), BF16),
            pltpu.VMEM((slots, 2, width, width), BF16),
            pltpu.VMEM((2, 2, width, width), BF16),
        ]
        factors = [
            pltpu.VMEM((3, 2 * width, 2 * width), BF16),
            pltpu.VMEM(split, BF16),
            pltpu.VMEM((width // LAST, width, 4 * LAST), BF16),
            pltpu.VMEM((4 * CHUNK, 2 * width), BF16),
            pltpu.VMEM((2, width, 2 * width), F32),
            pltpu.VMEM((width, 2 * width), F32),
            pltpu.SemaphoreType.DMA((4 + chunks,)),
            pltpu.SemaphoreType.DMA((2,)),
            pltpu.SemaphoreType.DMA((2,)),
        ]

        def flags(count):
            return [pltpu.SemaphoreType.DMA((2, count))] * 2

        def call(what, number, name, blocks, semaphores, *operands):
            return pl.pallas_call(
                functools.partial(what, slabs, energies),
                out_shape=jax.ShapeDtypeStruct((1, 1, 2, width, width), F32),
                in_specs=[hbm] * 6,
                out_specs=vmem,
                scratch_shapes=taken + blocks + factors + semaphores,
                compiler_params=pltpu.CompilerParams(
                    collective_id=number, has_side_effects=True, vmem_limit_bytes=48 * 1024 * 1024
                ),
                name=name,
            )(*operands)

        straight = functools.partial(
            call,
            straight_kernel,
            0,
            "straight",
            [pltpu.VMEM((5,) + split, BF16), pltpu.VMEM((2, 3) + split, BF16)],
            flags(chunks + 1 + pieces),
        )
        around = functools.partial(
            call,
            around_kernel,
            1,
            "around",
            [
                pltpu.VMEM((4, width // UNIT, chunks) + unit, BF16),
                pltpu.VMEM(split, BF16),
                pltpu.VMEM((2, LIST) + unit, BF16),
                pltpu.VMEM((DIRECT,) + unit, BF16),
                pltpu.VMEM((DIRECT,) + unit, BF16),
                pltpu.VMEM((LIST - DIRECT,) + unit, BF16),
                pltpu.VMEM((LIST - DIRECT,) + unit, BF16),
                pltpu.VMEM((2, LIST - DIRECT) + unit, BF16),
                pltpu.VMEM((2,) + split, BF16),
                pltpu.VMEM(split, BF16),
            ],
            flags(4) + flags(2) + flags(2) + flags(pieces),
        )
        crowded = pl.pallas_call(
            crowded_kernel,
            out_shape=jax.ShapeDtypeStruct((1,), jnp.int32),
            in_specs=[vmem] * 3,
            out_specs=pl.BlockSpec(memory_space=pltpu.SMEM),
            name="crowded",
        )(pair_off.T, pair_count[None], pair_range.T)
        return lax.cond(crowded[0] > 0, straight, around, *operands)

    wide = P("energy", "slab", None, None, None, None)
    slim = P("energy", "slab", None, None, None)
    return jax.shard_map(
        body,
        mesh=mesh,
        in_specs=(wide, wide, slim, P(), P(), P()),
        out_specs=slim,
        check_vma=False,
    )
```

```python
import functools

import jax
import jax.numpy as jnp
from jax import lax
from jax.experimental import pallas as pl
from jax.experimental.pallas import tpu as pltpu
from jax.sharding import PartitionSpec as P

MESH = pl.DeviceIdType.MESH
F32 = jnp.float32
BF16 = jnp.bfloat16
TILE = 16
CHUNK = 128
LAST = 64
UNIT = 96
GROUP = 3
LIST = 24
DIRECT = 18
SHARED = 12
HOP = 4
OFFSETS = (1, 2, -1, -2)


def extent(reach):
    steps = [(reach >= n * UNIT).astype(jnp.int32) for n in range(1, 5)]
    down = steps[0] + steps[1] + steps[2] + steps[3]
    across = steps[0] + steps[1] + steps[2]
    return down, across, down * across


def turned(slab, way):
    place = lax.rem(slab, HOP)
    paired = jnp.where(lax.rem(lax.div(slab, HOP), 2) == 0, HOP, -HOP)
    if way == 0:
        return jnp.where(place == HOP - 1, -HOP, jnp.where(place == 1, paired, HOP))
    return jnp.where(place == 0, HOP, jnp.where(place == 2, paired, -HOP))


def detours(slab, way, slabs):
    low, high = (0, slabs - 2) if way == 0 else (1, slabs - 1)
    relay = slab + turned(slab, way)
    return (slab >= low) & (slab <= high) & (relay >= low) & (relay <= high)


def relayed(relay, way):
    turn = turned(relay, way)
    return relay + jnp.where(lax.rem(relay, HOP) == 1 + way, turn, -turn)


def crowded_kernel(off_hbm, count_hbm, range_hbm, out_ref, off_ref, count_ref, range_ref, sem):
    tables = [
        pltpu.make_async_copy(source, held, sem.at[n])
        for n, (source, held) in enumerate(
            ((off_hbm, off_ref), (count_hbm, count_ref), (range_hbm, range_ref))
        )
    ]
    for table in tables:
        table.start()
    for table in tables:
        table.wait()
    off, reach = off_ref[...], range_ref[...]
    slots, slabs = off.shape
    live = lax.broadcasted_iota(jnp.int32, off.shape, 0) < count_ref[...]
    slab = lax.broadcasted_iota(jnp.int32, (1, slabs), 1)
    crowded = jnp.zeros((1, slabs), F32)
    for way in range(2):
        filled = jnp.zeros((1, slabs), jnp.int32)
        for offset in OFFSETS[2 * way : 2 * way + 2]:
            widest = jnp.max(jnp.where(live & (off == offset), reach, 0), axis=0, keepdims=True)
            filled = filled + extent(widest)[2]
        above = jnp.concatenate([filled[:, HOP:], filled[:, :HOP]], axis=1)
        below = jnp.concatenate([filled[:, -HOP:], filled[:, :-HOP]], axis=1)
        relay = jnp.where(turned(slab, way) > 0, above, below)
        room = jnp.where(filled > DIRECT + GROUP, SHARED, SHARED + GROUP)
        stuck = (relay > room) | jnp.logical_not(detours(slab, way, slabs))
        crowded = crowded + ((filled > DIRECT) & stuck).astype(F32)
    out_ref[0] = jnp.max(crowded).astype(jnp.int32)


def dot(a, b):
    return jnp.dot(a, b, preferred_element_type=F32)


def start(there, *copies):
    @pl.when(there)
    def _():
        for copy in copies:
            copy.start()


def arrived(there, *copies):
    @pl.when(there)
    def _():
        for copy in copies:
            copy.wait_recv()


def gone(there, *copies):
    @pl.when(there)
    def _():
        for copy in copies:
            copy.wait_send()


def greet(peers):
    barrier = pltpu.get_barrier_semaphore()
    for there, who in peers:

        @pl.when(there)
        def _():
            pl.semaphore_signal(barrier, inc=1, device_id=who, device_id_type=MESH)


def greeted(peers):
    barrier = pltpu.get_barrier_semaphore()
    pl.semaphore_wait(barrier, sum(there.astype(jnp.int32) for there, _ in peers))


def prepare(green_v, b_v, a_v, side_v):
    width = green_v.shape[-1]
    for at in range(3):
        for part in range(2):
            flipped = green_v[at, part].astype(F32).T
            plain = flipped.astype(BF16)
            minus = (-flipped).astype(BF16)
            for c in range(width // CHUNK):
                source = slice(c * CHUNK, (c + 1) * CHUNK)
                real = slice(2 * c * CHUNK, (2 * c + 1) * CHUNK)
                imag = slice((2 * c + 1) * CHUNK, (2 * c + 2) * CHUNK)
                if part == 0:
                    b_v[at, real, :width] = plain[source]
                    b_v[at, imag, width:] = plain[source]
                else:
                    b_v[at, real, width:] = minus[source]
                    b_v[at, imag, :width] = plain[source]
    for c in range(width // CHUNK):
        for part in range(2):
            a_v[c, :, part * CHUNK : (part + 1) * CHUNK] = green_v[1, part, :, c * CHUNK : (c + 1) * CHUNK]
    for h in range(width // LAST):
        for n, at in enumerate((0, 2)):
            side_v[h, :, 2 * n * LAST : 2 * (n + 1) * LAST] = jnp.concatenate(
                [green_v[at, part, :, h * LAST : (h + 1) * LAST] for part in range(2)], axis=1
            )


def b_chunk(b_v, at, c):
    return b_v[at, 2 * c * CHUNK : 2 * (c + 1) * CHUNK]


def put(y_v, at, x):
    rows, width = x.shape[0], x.shape[1] // 2
    real = x[:, :width].astype(BF16)
    imag = x[:, width:].astype(BF16)
    y_v[at : at + rows, :width] = real
    y_v[at : at + rows, width:] = imag
    y_v[at + rows : at + 2 * rows, :width] = -imag
    y_v[at + rows : at + 2 * rows, width:] = real


def centre_plan(width):
    whole, half, most = slice(None), width // 2, width - LAST
    plan = [(whole, 0, CHUNK), (whole, CHUNK, half - CHUNK), (whole, half, most - half)]
    return plan + [(slice(c, c + 1), most, LAST) for c in range(width // CHUNK)]


def finish(centre, comes, cent, late, b_v, side_v, y_v, part_v, acc_v, out_ref):
    width = acc_v.shape[0]
    chunks = width // CHUNK
    plan = centre_plan(width)
    for n, (these, row, count) in enumerate(plan):
        rows = slice(row, row + count)
        final = n == len(plan) - 1
        complete = these == slice(None) or final
        if row == width // 2:
            late()
        for way in range(2):
            arrived(comes[way], centre[way][n])
            x = part_v[way, rows]
            for c in range(chunks)[these]:
                x = x + dot(cent(way, c, rows), b_chunk(b_v, (0, 2)[way], c))
            if complete:
                for h in range(count // LAST):
                    put(y_v, 4 * h * LAST + 2 * way * LAST, x[h * LAST : (h + 1) * LAST])
            else:
                part_v[way, rows] = x
        if complete and not final:
            total = acc_v[...]
            for h in range(count // LAST):
                total = total + dot(side_v[row // LAST + h], y_v[4 * h * LAST : 4 * (h + 1) * LAST])
            acc_v[...] = total
    for m in range(chunks):
        rows = slice(m * CHUNK, (m + 1) * CHUNK)
        total = acc_v[rows] + dot(side_v[width // LAST - 1, rows], y_v[: 4 * LAST])
        for part in range(2):
            out_ref[0, 0, part, rows] = total[:, part * width : (part + 1) * width]


def straight_kernel(
    slabs,
    energies,
    off_hbm,
    count_hbm,
    range_hbm,
    green_hbm,
    sigma_hbm,
    phonon_hbm,
    out_ref,
    off_ref,
    count_ref,
    range_ref,
    green_v,
    sigma_v,
    near_v,
    mine_v,
    got_v,
    b_v,
    a_v,
    side_v,
    y_v,
    part_v,
    acc_v,
    local_sem,
    near_send,
    near_recv,
    send_sem,
    recv_sem,
):
    k = lax.axis_index("slab")
    e = lax.axis_index("energy")
    width = green_v.shape[-1]
    slots = sigma_v.shape[0]
    chunks = width // CHUNK
    has_low, has_high = e > 0, e < energies - 1
    has_left, has_right = k > 0, k < slabs - 1
    goes, comes = (has_right, has_left), (has_left, has_right)

    tables = [
        pltpu.make_async_copy(source, held, local_sem.at[n])
        for n, (source, held) in enumerate(
            ((off_hbm, off_ref), (count_hbm, count_ref), (range_hbm, range_ref))
        )
    ]
    load_sigma = []
    for c in range(chunks):
        rows = slice(c * CHUNK, (c + 1) * CHUNK)
        load_sigma.append(
            pltpu.make_async_copy(
                sigma_hbm.at[0, 0, :, :, rows], sigma_v.at[:, :, rows], local_sem.at[4 + c]
            )
        )
    load_green = pltpu.make_async_copy(green_hbm.at[0, 0], green_v, local_sem.at[3])

    peers = (
        (has_left, {"slab": k - 1}),
        (has_right, {"slab": k + 1}),
        (has_low, {"energy": e - 1}),
        (has_high, {"energy": e + 1}),
    )
    greet(peers)
    for table in tables:
        table.start()
    for load in load_sigma:
        load.start()

    def near_copy(slot, target):
        return pltpu.make_async_remote_copy(
            src_ref=phonon_hbm.at[0, 0],
            dst_ref=near_v.at[slot],
            send_sem=near_send.at[slot],
            recv_sem=near_recv.at[slot],
            device_id={"energy": target},
            device_id_type=MESH,
        )

    up, down = near_copy(0, e + 1), near_copy(1, e - 1)

    whole = slice(None)
    plan = [(0, whole, c * CHUNK, CHUNK) for c in range(chunks)]
    plan += [(1, whole, 0, width)]
    first_centre = len(plan)
    plan += [(2,) + piece for piece in centre_plan(width)]
    sent = [[], []]
    for way in range(2):
        for n, (slot, these, row, count) in enumerate(plan):
            source = 4 if slot == 2 else 2 * way + slot
            sent[way].append(
                pltpu.make_async_remote_copy(
                    src_ref=mine_v.at[source, these, row : row + count],
                    dst_ref=got_v.at[way, slot, these, row : row + count],
                    send_sem=send_sem.at[way, n],
                    recv_sem=recv_sem.at[way, n],
                    device_id={"slab": (k + 1, k - 1)[way]},
                    device_id_type=MESH,
                )
            )

    def combine(at, offset, with_phonon, first=0, last=width // TILE):
        reach = []
        for q in range(slots):
            live = (q < count_ref[k]) & (off_ref[q, k] == offset)
            reach.append(jnp.where(live, range_ref[q, k], 0))

        def step(t, carry):
            rows = pl.ds(pl.multiple_of(t * TILE, TILE), TILE)
            col_ids = lax.broadcasted_iota(jnp.int32, (TILE, width), 1)
            inside = [col_ids < jnp.where(t * TILE < reach[q], reach[q], 0) for q in range(slots)]
            for part in range(2):
                kept = [
                    jnp.where(inside[q], sigma_v[q, part, rows, :].astype(F32), 0.0) for q in range(slots)
                ]
                total = functools.reduce(jnp.add, kept)
                if with_phonon:
                    low = near_v[0, part, rows, :].astype(F32)
                    high = near_v[1, part, rows, :].astype(F32)
                    total = total + (0.5 * (low + high)).astype(BF16).astype(F32)
                total = total.astype(BF16)
                for c in range(chunks):
                    mine_v[at, c, rows, part * CHUNK : (part + 1) * CHUNK] = total[
                        :, c * CHUNK : (c + 1) * CHUNK
                    ]
            return carry

        lax.fori_loop(first, last, step, 0, unroll=4)

    for table in tables:
        table.wait()
    tiles = CHUNK // TILE
    for c in range(chunks):
        load_sigma[c].wait()
        for way in range(2):
            combine(2 * way, (1, -1)[way], False, c * tiles, (c + 1) * tiles)
            if c == 0 and way == 0:
                greeted(peers)
            start(goes[way], sent[way][c])
        if c == 0:
            start(has_high, up)
            start(has_low, down)
    load_green.start()
    for way in range(2):
        combine(2 * way + 1, (2, -2)[way], False)
        start(goes[way], sent[way][chunks])

    for way in range(2):

        @pl.when(jnp.logical_not(comes[way]))
        def _():
            got_v[way] = jnp.zeros_like(got_v[way])

    for there, slot in ((has_low, 0), (has_high, 1)):

        @pl.when(jnp.logical_not(there))
        def _():
            near_v[slot] = jnp.zeros_like(near_v[slot])

    load_green.wait()
    prepare(green_v, b_v, a_v, side_v)

    arrived(has_low, up)
    arrived(has_high, down)
    combine(4, 0, True)
    for way in range(2):
        start(goes[way], *sent[way][first_centre:])

    for r in range(chunks):
        rows = slice(r * CHUNK, (r + 1) * CHUNK)
        x = None
        for at, partner in ((2, 0), (4, 1), (0, 2)):
            for c in range(chunks):
                term = dot(mine_v[at, c, rows], b_chunk(b_v, partner, c))
                x = term if x is None else x + term
        put(y_v, 0, x)
        term = dot(a_v[r], y_v[: 2 * CHUNK])
        acc_v[...] = term if r == 0 else acc_v[...] + term

    for slot in range(2):
        for way in range(2):
            arrived(comes[way], *sent[way][chunks * slot : chunks + slot])
            partner = ((1, 2), (1, 0))[way][slot]
            for r in range(chunks):
                rows = slice(r * CHUNK, (r + 1) * CHUNK)
                x = None
                for c in range(chunks):
                    term = dot(got_v[way, slot, c, rows], b_chunk(b_v, partner, c))
                    x = term if x is None else x + term
                part_v[way, rows] = x if slot == 0 else part_v[way, rows] + x
    centre = [copies[first_centre:] for copies in sent]
    finish(
        centre,
        comes,
        lambda way, c, rows: got_v[way, 2, c, rows],
        lambda: None,
        b_v,
        side_v,
        y_v,
        part_v,
        acc_v,
        out_ref,
    )

    gone(has_high, up)
    gone(has_low, down)
    gone(has_right, *sent[0])
    gone(has_left, *sent[1])


def around_kernel(
    slabs,
    energies,
    off_hbm,
    count_hbm,
    range_hbm,
    green_hbm,
    sigma_hbm,
    phonon_hbm,
    out_ref,
    off_ref,
    count_ref,
    range_ref,
    green_v,
    sigma_v,
    near_v,
    mine_v,
    own_v,
    list_v,
    from_left_v,
    from_right_v,
    back_left_v,
    back_right_v,
    spill_v,
    cent_v,
    block_v,
    b_v,
    a_v,
    side_v,
    y_v,
    part_v,
    acc_v,
    local_sem,
    near_send,
    near_recv,
    unit_send,
    unit_recv,
    spill_send,
    spill_recv,
    back_send,
    back_recv,
    cent_send,
    cent_recv,
):
    k = lax.axis_index("slab")
    e = lax.axis_index("energy")
    width = green_v.shape[-1]
    slots = sigma_v.shape[0]
    chunks = width // CHUNK
    has_low, has_high = e > 0, e < energies - 1

    has_left, has_right = k > 0, k < slabs - 1

    tables = [
        pltpu.make_async_copy(source, held, local_sem.at[n])
        for n, (source, held) in enumerate(
            ((off_hbm, off_ref), (count_hbm, count_ref), (range_hbm, range_ref))
        )
    ]
    load_sigma = []
    for c in range(chunks):
        rows = slice(c * CHUNK, (c + 1) * CHUNK)
        load_sigma.append(
            pltpu.make_async_copy(
                sigma_hbm.at[0, 0, :, :, rows], sigma_v.at[:, :, rows], local_sem.at[4 + c]
            )
        )
    load_green = pltpu.make_async_copy(green_hbm.at[0, 0], green_v, local_sem.at[3])
    peers = (
        (has_left, {"slab": k - 1}),
        (has_right, {"slab": k + 1}),
        (has_low, {"energy": e - 1}),
        (has_high, {"energy": e + 1}),
        (k >= HOP, {"slab": k - HOP}),
        (k < slabs - HOP, {"slab": k + HOP}),
    )
    greet(peers)
    for table in tables:
        table.start()
    for load in load_sigma:
        load.start()

    def near_copy(slot, target):
        return pltpu.make_async_remote_copy(
            src_ref=phonon_hbm.at[0, 0],
            dst_ref=near_v.at[slot],
            send_sem=near_send.at[slot],
            recv_sem=near_recv.at[slot],
            device_id={"energy": target},
            device_id_type=MESH,
        )

    up, down = near_copy(0, e + 1), near_copy(1, e - 1)

    def remote(source, target, sent, received, slab):
        return pltpu.make_async_remote_copy(
            src_ref=source,
            dst_ref=target,
            send_sem=sent,
            recv_sem=received,
            device_id={"slab": slab},
            device_id_type=MESH,
        )

    sends = [detours(k, way, slabs) for way in range(2)]
    rides = [relayed(k, way) for way in range(2)]
    relays = [detours(rides[way], way, slabs) for way in range(2)]
    handed = [relayed(k + step, way) for way, step in ((0, -1), (1, 1))]
    hands = [there & detours(handed[way], way, slabs) for way, there in enumerate((has_left, has_right))]
    gets = [there & detours(k + step, way, slabs) for way, (there, step) in enumerate(((has_left, -1), (has_right, 1)))]
    beside = (k + 1, k - 1)
    goes, comes = (has_right, has_left), (has_left, has_right)
    got_v, back_v = (from_left_v, from_right_v), (back_left_v, back_right_v)
    units = (slice(0, 9), slice(12, 15), slice(9, 12), slice(15, 18))
    halves = (slice(0, GROUP), slice(GROUP, 2 * GROUP))
    direct, spill, returned, centre = [[], []], [[], []], [[], []], [[], []]
    for way in range(2):
        for n, these in enumerate(units):
            direct[way].append(
                remote(
                    list_v.at[way, these],
                    got_v[way].at[these],
                    unit_send.at[way, n],
                    unit_recv.at[way, n],
                    beside[way],
                )
            )
        for h, these in enumerate(halves):
            spill[way].append(
                remote(
                    list_v.at[way, LIST - (h + 1) * GROUP : LIST - h * GROUP],
                    spill_v.at[way, these],
                    spill_send.at[way, h],
                    spill_recv.at[way, h],
                    k + turned(k, way),
                )
            )
            returned[way].append(
                remote(
                    got_v[way].at[SHARED + h * GROUP : SHARED + (h + 1) * GROUP],
                    back_v[way].at[halves[1 - h]],
                    back_send.at[way, h],
                    back_recv.at[way, h],
                    handed[way] + (1, -1)[way],
                )
            )
        for n, (these, row, count) in enumerate(centre_plan(width)):
            centre[way].append(
                remote(
                    own_v.at[these, row : row + count],
                    cent_v.at[way, these, row : row + count],
                    cent_send.at[way, n],
                    cent_recv.at[way, n],
                    beside[way],
                )
            )

    def live_reach(slab, q, offset):
        live = (q < count_ref[slab]) & (off_ref[q, slab] == offset)
        return jnp.where(live, range_ref[q, slab], 0)

    def combine(wanted, with_phonon, first=0, last=width // TILE):
        reach = [[live_reach(k, q, offset) for q in range(slots)] for _, offset in wanted]

        def step(t, carry):
            rows = pl.ds(pl.multiple_of(t * TILE, TILE), TILE)
            col_ids = lax.broadcasted_iota(jnp.int32, (TILE, width), 1)
            m = lax.div(t, UNIT // TILE)
            unit_rows = pl.ds(pl.multiple_of(t * TILE - m * UNIT, TILE), TILE)
            inside = [
                [col_ids < jnp.where(t * TILE < reach[n][q], reach[n][q], 0) for q in range(slots)]
                for n in range(len(wanted))
            ]
            for part in range(2):
                terms = [sigma_v[q, part, rows, :].astype(F32) for q in range(slots)]
                for n, (at, _) in enumerate(wanted):
                    kept = [jnp.where(inside[n][q], terms[q], 0.0) for q in range(slots)]
                    total = functools.reduce(jnp.add, kept)
                    if with_phonon:
                        low = near_v[0, part, rows, :].astype(F32)
                        high = near_v[1, part, rows, :].astype(F32)
                        total = total + (0.5 * (low + high)).astype(BF16).astype(F32)
                    total = total.astype(BF16)
                    lanes = slice(part * CHUNK, (part + 1) * CHUNK)
                    for c in range(chunks):
                        value = total[:, c * CHUNK : (c + 1) * CHUNK]
                        if with_phonon:
                            own_v[c, rows, lanes] = value
                        else:
                            mine_v[at, m, c, unit_rows, lanes] = value
            return carry

        lax.fori_loop(first, last, step, 0, unroll=4)

    def layout(slab, way):
        blocks = []
        for offset in OFFSETS[2 * way : 2 * way + 2]:
            reach = functools.reduce(jnp.maximum, [live_reach(slab, q, offset) for q in range(slots)])
            blocks.append(extent(reach))
        return blocks

    def pack(way, first, last):
        (_, across_a, size_a), (_, across_b, size_b) = layout(k, way)

        def step(p, carry):
            in_a = p < size_a
            unit = jnp.where(in_a, p, jnp.maximum(p - size_a, 0))
            across = jnp.where(in_a, across_a, across_b)
            row = jnp.where(across == 3, lax.div(unit, 3), jnp.where(across == 2, lax.div(unit, 2), unit))
            col = jnp.clip(unit - row * across, 0, chunks - 1)
            row = jnp.clip(row, 0, width // UNIT - 1)
            at = 2 * way + jnp.where(in_a, 0, 1)
            keep = jnp.where(p < size_a + size_b, 1.0, 0.0).astype(BF16)
            list_v[way, p] = mine_v[at, row, col] * keep
            return carry

        lax.fori_loop(first, last, step, 0, unroll=3)

    for table in tables:
        table.wait()
    tiles = width // TILE // chunks
    for c in range(chunks):
        load_sigma[c].wait()
        for way in range(2):
            wanted = [(2 * way + n, OFFSETS[2 * way + n]) for n in range(2)]
            combine(wanted, False, c * tiles, (c + 1) * tiles)
    load_green.start()
    for way in range(2):
        pack(way, DIRECT, LIST)
        pack(way, 0, 9)
        if way == 0:
            greeted(peers)
        start(sends[way], spill[way][0])
        start(goes[way], direct[way][0])
    start(has_high, up)
    start(has_low, down)
    for way in range(2):
        start(sends[way], spill[way][1])
        pack(way, 9, DIRECT)

    for way in range(2):

        @pl.when(jnp.logical_not(comes[way]))
        def _():
            got_v[way][...] = jnp.zeros_like(got_v[way])
            cent_v[way] = jnp.zeros_like(cent_v[way])

        @pl.when(jnp.logical_not(gets[way]))
        def _():
            back_v[way][...] = jnp.zeros_like(back_v[way])

        @pl.when(jnp.logical_not(relays[way]))
        def _():
            spill_v[way] = jnp.zeros_like(spill_v[way])

    for there, slot in ((has_low, 0), (has_high, 1)):

        @pl.when(jnp.logical_not(there))
        def _():
            near_v[slot] = jnp.zeros_like(near_v[slot])

    load_green.wait()
    prepare(green_v, b_v, a_v, side_v)

    arrived(has_low, up)
    arrived(has_high, down)
    combine([(4, 0)], True)

    def merge(h):
        for way in range(2):
            arrived(relays[way], spill[way][h])
            for j in range(h * GROUP, (h + 1) * GROUP):
                list_v[way, SHARED + j] = list_v[way, SHARED + j] + spill_v[way, j]

    merge(0)
    for way in range(2):
        start(goes[way], direct[way][1], direct[way][2])

    for n, (at, partner) in enumerate(((2, 0), (0, 2))):
        for r in range(2):
            rows = slice(r * width // 2, (r + 1) * width // 2)
            these = slice(rows.start // UNIT, rows.stop // UNIT)
            x = None
            for c in range(chunks):
                term = dot(mine_v[at, these, c].reshape(width // 2, 2 * CHUNK), b_chunk(b_v, partner, c))
                x = term if x is None else x + term
            part_v[0, rows] = x if n == 0 else part_v[0, rows] + x
    for r in range(chunks):
        rows = slice(r * CHUNK, (r + 1) * CHUNK)
        x = part_v[0, rows]
        for c in range(chunks):
            x = x + dot(own_v[c, rows], b_chunk(b_v, 1, c))
        put(y_v, 0, x)
        term = dot(a_v[r], y_v[: 2 * CHUNK])
        acc_v[...] = term if r == 0 else acc_v[...] + term

    merge(1)
    for way in range(2):
        start(goes[way], direct[way][3], *centre[way])
    first_row = lax.rem(k, HOP) == 0
    for order, here in (((1, 0), first_row), ((0, 1), jnp.logical_not(first_row))):

        @pl.when(here)
        def _():
            for n, h in ((1, 0), (3, 1)):
                for way in order:
                    arrived(comes[way], direct[way][n])
                    start(hands[way], returned[way][h])


    def multiply(way, source, first, last, down_n, across_n, before, partner, fresh, top=0):
        for m in range(top // UNIT, width // UNIT):
            for c in range(chunks):
                position = before + m * across_n + c
                there = (m < down_n) & (c < across_n) & (position >= first) & (position < last)
                keep = jnp.where(there, 1.0, 0.0).astype(BF16)
                position = jnp.clip(position - first, 0, last - first - 1)
                block_v[c, m * UNIT : (m + 1) * UNIT] = source[position] * keep
        for row in range(top, width, width // 2):
            rows = slice(row, row + width // 2)
            x = None
            for c in range(chunks):
                term = dot(block_v[c, rows], b_chunk(b_v, partner, c))
                x = term if x is None else x + term
            part_v[way, rows] = x if fresh else part_v[way, rows] + x

    blocks = [
        layout(jnp.maximum(k - 1, 0), 0),
        layout(jnp.minimum(k + 1, slabs - 1), 1),
    ]
    for way in range(2):
        (down_a, across_a, size_a), (down_b, across_b, _) = blocks[way]
        partner_a, partner_b = ((1, 2), (1, 0))[way]
        arrived(comes[way], direct[way][0], direct[way][2])
        multiply(way, got_v[way], 0, DIRECT, down_a, across_a, 0, partner_a, True)
        multiply(way, got_v[way], 0, DIRECT, down_b, across_b, size_a, partner_b, False)

    def late():
        for way in range(2):
            (_, _, size_a), (down_b, across_b, _) = blocks[way]
            arrived(gets[way], *returned[way])
            multiply(
                way, back_v[way], DIRECT, LIST, down_b, across_b, size_a, (2, 0)[way], False, width // 2
            )

    finish(
        centre,
        comes,
        lambda way, c, rows: cent_v[way, c, rows],
        late,
        b_v,
        side_v,
        y_v,
        part_v,
        acc_v,
        out_ref,
    )

    gone(has_high, up)
    gone(has_low, down)
    for way in range(2):
        gone(goes[way], *direct[way], *centre[way])
        gone(sends[way], *spill[way])
        gone(hands[way], *returned[way])


def solution(mesh):
    slabs, energies = mesh.shape["slab"], mesh.shape["energy"]

    def body(green, sigma, phonon, pair_off, pair_count, pair_range):
        width = green.shape[-1]
        slots = sigma.shape[2]
        chunks = width // CHUNK
        pieces = len(centre_plan(width))
        hbm = pl.BlockSpec(memory_space=pltpu.HBM)
        vmem = pl.BlockSpec(memory_space=pltpu.VMEM)
        split = (chunks, width, 2 * CHUNK)
        unit = (UNIT, 2 * CHUNK)
        operands = (pair_off.T, pair_count, pair_range.T, green, sigma, phonon)
        operands = [pltpu.with_memory_space_constraint(v, pltpu.HBM) for v in operands]
        taken = [
            pltpu.SMEM((slots, slabs), jnp.int32),
            pltpu.SMEM((slabs,), jnp.int32),
            pltpu.SMEM((slots, slabs), jnp.int32),
            pltpu.VMEM((3, 2, width, width), BF16),
            pltpu.VMEM((slots, 2, width, width), BF16),
            pltpu.VMEM((2, 2, width, width), BF16),
        ]
        factors = [
            pltpu.VMEM((3, 2 * width, 2 * width), BF16),
            pltpu.VMEM(split, BF16),
            pltpu.VMEM((width // LAST, width, 4 * LAST), BF16),
            pltpu.VMEM((4 * CHUNK, 2 * width), BF16),
            pltpu.VMEM((2, width, 2 * width), F32),
            pltpu.VMEM((width, 2 * width), F32),
            pltpu.SemaphoreType.DMA((4 + chunks,)),
            pltpu.SemaphoreType.DMA((2,)),
            pltpu.SemaphoreType.DMA((2,)),
        ]

        def flags(count):
            return [pltpu.SemaphoreType.DMA((2, count))] * 2

        def call(what, number, name, blocks, semaphores, *operands):
            return pl.pallas_call(
                functools.partial(what, slabs, energies),
                out_shape=jax.ShapeDtypeStruct((1, 1, 2, width, width), F32),
                in_specs=[hbm] * 6,
                out_specs=vmem,
                scratch_shapes=taken + blocks + factors + semaphores,
                compiler_params=pltpu.CompilerParams(
                    collective_id=number, has_side_effects=True, vmem_limit_bytes=48 * 1024 * 1024
                ),
                name=name,
            )(*operands)

        straight = functools.partial(
            call,
            straight_kernel,
            0,
            "straight",
            [pltpu.VMEM((5,) + split, BF16), pltpu.VMEM((2, 3) + split, BF16)],
            flags(chunks + 1 + pieces),
        )
        around = functools.partial(
            call,
            around_kernel,
            1,
            "around",
            [
                pltpu.VMEM((4, width // UNIT, chunks) + unit, BF16),
                pltpu.VMEM(split, BF16),
                pltpu.VMEM((2, LIST) + unit, BF16),
                pltpu.VMEM((DIRECT,) + unit, BF16),
                pltpu.VMEM((DIRECT,) + unit, BF16),
                pltpu.VMEM((LIST - DIRECT,) + unit, BF16),
                pltpu.VMEM((LIST - DIRECT,) + unit, BF16),
                pltpu.VMEM((2, LIST - DIRECT) + unit, BF16),
                pltpu.VMEM((2,) + split, BF16),
                pltpu.VMEM(split, BF16),
            ],
            flags(4) + flags(2) + flags(2) + flags(pieces),
        )
        crowded = pl.pallas_call(
            crowded_kernel,
            out_shape=jax.ShapeDtypeStruct((1,), jnp.int32),
            in_specs=[hbm] * 3,
            out_specs=pl.BlockSpec(memory_space=pltpu.SMEM),
            scratch_shapes=[
                pltpu.VMEM((slots, slabs), jnp.int32),
                pltpu.VMEM((1, slabs), jnp.int32),
                pltpu.VMEM((slots, slabs), jnp.int32),
                pltpu.SemaphoreType.DMA((3,)),
            ],
            name="crowded",
        )(operands[0], pltpu.with_memory_space_constraint(pair_count[None], pltpu.HBM), operands[2])
        return lax.cond(crowded[0] > 0, straight, around, *operands)

    wide = P("energy", "slab", None, None, None, None)
    slim = P("energy", "slab", None, None, None)
    return jax.shard_map(
        body,
        mesh=mesh,
        in_specs=(wide, wide, slim, P(), P(), P()),
        out_specs=slim,
        check_vma=False,
    )
```

```python
import functools

import jax
import jax.numpy as jnp
from jax import lax
from jax.experimental import pallas as pl
from jax.experimental.pallas import tpu as pltpu
from jax.sharding import PartitionSpec as P

MESH = pl.DeviceIdType.MESH
F32 = jnp.float32
BF16 = jnp.bfloat16
TILE = 16
CHUNK = 128
LAST = 64
UNIT = 96
GROUP = 3
LIST = 24
DIRECT = 18
SHARED = 12
HOP = 4
OFFSETS = (1, 2, -1, -2)


def extent(reach):
    steps = [(reach >= n * UNIT).astype(jnp.int32) for n in range(1, 5)]
    down = steps[0] + steps[1] + steps[2] + steps[3]
    across = steps[0] + steps[1] + steps[2]
    return down, across, down * across


def turned(slab, way):
    place = lax.rem(slab, HOP)
    paired = jnp.where(lax.rem(lax.div(slab, HOP), 2) == 0, HOP, -HOP)
    if way == 0:
        return jnp.where(place == HOP - 1, -HOP, jnp.where(place == 1, paired, HOP))
    return jnp.where(place == 0, HOP, jnp.where(place == 2, paired, -HOP))


def detours(slab, way, slabs):
    low, high = (0, slabs - 2) if way == 0 else (1, slabs - 1)
    relay = slab + turned(slab, way)
    return (slab >= low) & (slab <= high) & (relay >= low) & (relay <= high)


def relayed(relay, way):
    turn = turned(relay, way)
    return relay + jnp.where(lax.rem(relay, HOP) == 1 + way, turn, -turn)


def crowded_kernel(off_ref, count_ref, range_ref, out_ref):
    off, reach = off_ref[...], range_ref[...]
    slots, slabs = off.shape
    live = lax.broadcasted_iota(jnp.int32, off.shape, 0) < count_ref[...]
    slab = lax.broadcasted_iota(jnp.int32, (1, slabs), 1)
    crowded = jnp.zeros((1, slabs), F32)
    for way in range(2):
        filled = jnp.zeros((1, slabs), jnp.int32)
        for offset in OFFSETS[2 * way : 2 * way + 2]:
            widest = jnp.max(jnp.where(live & (off == offset), reach, 0), axis=0, keepdims=True)
            filled = filled + extent(widest)[2]
        above = jnp.concatenate([filled[:, HOP:], filled[:, :HOP]], axis=1)
        below = jnp.concatenate([filled[:, -HOP:], filled[:, :-HOP]], axis=1)
        relay = jnp.where(turned(slab, way) > 0, above, below)
        room = jnp.where(filled > DIRECT + GROUP, SHARED, SHARED + GROUP)
        stuck = (relay > room) | jnp.logical_not(detours(slab, way, slabs))
        crowded = crowded + ((filled > DIRECT) & stuck).astype(F32)
    out_ref[0] = jnp.max(crowded).astype(jnp.int32)


def dot(a, b):
    return jnp.dot(a, b, preferred_element_type=F32)


def start(there, *copies):
    @pl.when(there)
    def _():
        for copy in copies:
            copy.start()


def arrived(there, *copies):
    @pl.when(there)
    def _():
        for copy in copies:
            copy.wait_recv()


def gone(there, *copies):
    @pl.when(there)
    def _():
        for copy in copies:
            copy.wait_send()


def greet(peers):
    barrier = pltpu.get_barrier_semaphore()
    for there, who in peers:

        @pl.when(there)
        def _():
            pl.semaphore_signal(barrier, inc=1, device_id=who, device_id_type=MESH)


def greeted(peers):
    barrier = pltpu.get_barrier_semaphore()
    pl.semaphore_wait(barrier, sum(there.astype(jnp.int32) for there, _ in peers))


def prepare(green_v, b_v, a_v, side_v):
    width = green_v.shape[-1]
    for at in range(3):
        for part in range(2):
            flipped = green_v[at, part].astype(F32).T
            plain = flipped.astype(BF16)
            minus = (-flipped).astype(BF16)
            for c in range(width // CHUNK):
                source = slice(c * CHUNK, (c + 1) * CHUNK)
                real = slice(2 * c * CHUNK, (2 * c + 1) * CHUNK)
                imag = slice((2 * c + 1) * CHUNK, (2 * c + 2) * CHUNK)
                if part == 0:
                    b_v[at, real, :width] = plain[source]
                    b_v[at, imag, width:] = plain[source]
                else:
                    b_v[at, real, width:] = minus[source]
                    b_v[at, imag, :width] = plain[source]
    for c in range(width // CHUNK):
        for part in range(2):
            a_v[c, :, part * CHUNK : (part + 1) * CHUNK] = green_v[1, part, :, c * CHUNK : (c + 1) * CHUNK]
    for h in range(width // LAST):
        for n, at in enumerate((0, 2)):
            side_v[h, :, 2 * n * LAST : 2 * (n + 1) * LAST] = jnp.concatenate(
                [green_v[at, part, :, h * LAST : (h + 1) * LAST] for part in range(2)], axis=1
            )


def b_chunk(b_v, at, c):
    return b_v[at, 2 * c * CHUNK : 2 * (c + 1) * CHUNK]


def put(y_v, at, x):
    rows, width = x.shape[0], x.shape[1] // 2
    real = x[:, :width].astype(BF16)
    imag = x[:, width:].astype(BF16)
    y_v[at : at + rows, :width] = real
    y_v[at : at + rows, width:] = imag
    y_v[at + rows : at + 2 * rows, :width] = -imag
    y_v[at + rows : at + 2 * rows, width:] = real


def centre_plan(width):
    whole, half, most = slice(None), width // 2, width - LAST
    plan = [(whole, 0, CHUNK), (whole, CHUNK, half - CHUNK), (whole, half, most - half)]
    return plan + [(slice(c, c + 1), most, LAST) for c in range(width // CHUNK)]


def finish(centre, comes, cent, late, b_v, side_v, y_v, part_v, acc_v, out_ref):
    width = acc_v.shape[0]
    chunks = width // CHUNK
    plan = centre_plan(width)
    for n, (these, row, count) in enumerate(plan):
        rows = slice(row, row + count)
        final = n == len(plan) - 1
        complete = these == slice(None) or final
        if row == width // 2:
            late()
        for way in range(2):
            arrived(comes[way], centre[way][n])
            x = part_v[way, rows]
            for c in range(chunks)[these]:
                x = x + dot(cent(way, c, rows), b_chunk(b_v, (0, 2)[way], c))
            if complete:
                for h in range(count // LAST):
                    put(y_v, 4 * h * LAST + 2 * way * LAST, x[h * LAST : (h + 1) * LAST])
            else:
                part_v[way, rows] = x
        if complete and not final:
            total = acc_v[...]
            for h in range(count // LAST):
                total = total + dot(side_v[row // LAST + h], y_v[4 * h * LAST : 4 * (h + 1) * LAST])
            acc_v[...] = total
    for m in range(chunks):
        rows = slice(m * CHUNK, (m + 1) * CHUNK)
        total = acc_v[rows] + dot(side_v[width // LAST - 1, rows], y_v[: 4 * LAST])
        for part in range(2):
            out_ref[0, 0, part, rows] = total[:, part * width : (part + 1) * width]


def straight_kernel(
    slabs,
    energies,
    off_hbm,
    count_hbm,
    range_hbm,
    green_hbm,
    sigma_hbm,
    phonon_hbm,
    out_ref,
    off_ref,
    count_ref,
    range_ref,
    green_v,
    sigma_v,
    near_v,
    mine_v,
    got_v,
    b_v,
    a_v,
    side_v,
    y_v,
    part_v,
    acc_v,
    local_sem,
    near_send,
    near_recv,
    send_sem,
    recv_sem,
):
    k = lax.axis_index("slab")
    e = lax.axis_index("energy")
    width = green_v.shape[-1]
    slots = sigma_v.shape[0]
    chunks = width // CHUNK
    has_low, has_high = e > 0, e < energies - 1
    has_left, has_right = k > 0, k < slabs - 1
    goes, comes = (has_right, has_left), (has_left, has_right)

    tables = [
        pltpu.make_async_copy(source, held, local_sem.at[n])
        for n, (source, held) in enumerate(
            ((off_hbm, off_ref), (count_hbm, count_ref), (range_hbm, range_ref))
        )
    ]
    load_sigma = []
    for c in range(chunks):
        rows = slice(c * CHUNK, (c + 1) * CHUNK)
        load_sigma.append(
            pltpu.make_async_copy(
                sigma_hbm.at[0, 0, :, :, rows], sigma_v.at[:, :, rows], local_sem.at[4 + c]
            )
        )
    load_green = pltpu.make_async_copy(green_hbm.at[0, 0], green_v, local_sem.at[3])

    peers = (
        (has_left, {"slab": k - 1}),
        (has_right, {"slab": k + 1}),
        (has_low, {"energy": e - 1}),
        (has_high, {"energy": e + 1}),
    )
    greet(peers)
    for table in tables:
        table.start()
    for load in load_sigma:
        load.start()

    def near_copy(slot, target):
        return pltpu.make_async_remote_copy(
            src_ref=phonon_hbm.at[0, 0],
            dst_ref=near_v.at[slot],
            send_sem=near_send.at[slot],
            recv_sem=near_recv.at[slot],
            device_id={"energy": target},
            device_id_type=MESH,
        )

    up, down = near_copy(0, e + 1), near_copy(1, e - 1)

    whole = slice(None)
    plan = [(0, whole, c * CHUNK, CHUNK) for c in range(chunks)]
    plan += [(1, whole, 0, width)]
    first_centre = len(plan)
    plan += [(2,) + piece for piece in centre_plan(width)]
    sent = [[], []]
    for way in range(2):
        for n, (slot, these, row, count) in enumerate(plan):
            source = 4 if slot == 2 else 2 * way + slot
            sent[way].append(
                pltpu.make_async_remote_copy(
                    src_ref=mine_v.at[source, these, row : row + count],
                    dst_ref=got_v.at[way, slot, these, row : row + count],
                    send_sem=send_sem.at[way, n],
                    recv_sem=recv_sem.at[way, n],
                    device_id={"slab": (k + 1, k - 1)[way]},
                    device_id_type=MESH,
                )
            )

    def combine(at, offset, with_phonon, first=0, last=width // TILE):
        reach = []
        for q in range(slots):
            live = (q < count_ref[k]) & (off_ref[q, k] == offset)
            reach.append(jnp.where(live, range_ref[q, k], 0))

        def step(t, carry):
            rows = pl.ds(pl.multiple_of(t * TILE, TILE), TILE)
            col_ids = lax.broadcasted_iota(jnp.int32, (TILE, width), 1)
            inside = [col_ids < jnp.where(t * TILE < reach[q], reach[q], 0) for q in range(slots)]
            for part in range(2):
                kept = [
                    jnp.where(inside[q], sigma_v[q, part, rows, :].astype(F32), 0.0) for q in range(slots)
                ]
                total = functools.reduce(jnp.add, kept)
                if with_phonon:
                    low = near_v[0, part, rows, :].astype(F32)
                    high = near_v[1, part, rows, :].astype(F32)
                    total = total + (0.5 * (low + high)).astype(BF16).astype(F32)
                total = total.astype(BF16)
                for c in range(chunks):
                    mine_v[at, c, rows, part * CHUNK : (part + 1) * CHUNK] = total[
                        :, c * CHUNK : (c + 1) * CHUNK
                    ]
            return carry

        lax.fori_loop(first, last, step, 0, unroll=4)

    for table in tables:
        table.wait()
    tiles = CHUNK // TILE
    for c in range(chunks):
        load_sigma[c].wait()
        for way in range(2):
            combine(2 * way, (1, -1)[way], False, c * tiles, (c + 1) * tiles)
            if c == 0 and way == 0:
                greeted(peers)
            start(goes[way], sent[way][c])
        if c == 0:
            start(has_high, up)
            start(has_low, down)
    load_green.start()
    for way in range(2):
        combine(2 * way + 1, (2, -2)[way], False)
        start(goes[way], sent[way][chunks])

    for way in range(2):

        @pl.when(jnp.logical_not(comes[way]))
        def _():
            got_v[way] = jnp.zeros_like(got_v[way])

    for there, slot in ((has_low, 0), (has_high, 1)):

        @pl.when(jnp.logical_not(there))
        def _():
            near_v[slot] = jnp.zeros_like(near_v[slot])

    load_green.wait()
    prepare(green_v, b_v, a_v, side_v)

    arrived(has_low, up)
    arrived(has_high, down)
    combine(4, 0, True)
    for way in range(2):
        start(goes[way], *sent[way][first_centre:])

    for r in range(chunks):
        rows = slice(r * CHUNK, (r + 1) * CHUNK)
        x = None
        for at, partner in ((2, 0), (4, 1), (0, 2)):
            for c in range(chunks):
                term = dot(mine_v[at, c, rows], b_chunk(b_v, partner, c))
                x = term if x is None else x + term
        put(y_v, 0, x)
        term = dot(a_v[r], y_v[: 2 * CHUNK])
        acc_v[...] = term if r == 0 else acc_v[...] + term

    for slot in range(2):
        for way in range(2):
            arrived(comes[way], *sent[way][chunks * slot : chunks + slot])
            partner = ((1, 2), (1, 0))[way][slot]
            for r in range(chunks):
                rows = slice(r * CHUNK, (r + 1) * CHUNK)
                x = None
                for c in range(chunks):
                    term = dot(got_v[way, slot, c, rows], b_chunk(b_v, partner, c))
                    x = term if x is None else x + term
                part_v[way, rows] = x if slot == 0 else part_v[way, rows] + x
    centre = [copies[first_centre:] for copies in sent]
    finish(
        centre,
        comes,
        lambda way, c, rows: got_v[way, 2, c, rows],
        lambda: None,
        b_v,
        side_v,
        y_v,
        part_v,
        acc_v,
        out_ref,
    )

    gone(has_high, up)
    gone(has_low, down)
    gone(has_right, *sent[0])
    gone(has_left, *sent[1])


def around_kernel(
    slabs,
    energies,
    off_hbm,
    count_hbm,
    range_hbm,
    green_hbm,
    sigma_hbm,
    phonon_hbm,
    out_ref,
    off_ref,
    count_ref,
    range_ref,
    green_v,
    sigma_v,
    near_v,
    mine_v,
    own_v,
    list_v,
    from_left_v,
    from_right_v,
    back_left_v,
    back_right_v,
    spill_v,
    cent_v,
    block_v,
    b_v,
    a_v,
    side_v,
    y_v,
    part_v,
    acc_v,
    local_sem,
    near_send,
    near_recv,
    unit_send,
    unit_recv,
    spill_send,
    spill_recv,
    back_send,
    back_recv,
    cent_send,
    cent_recv,
):
    k = lax.axis_index("slab")
    e = lax.axis_index("energy")
    width = green_v.shape[-1]
    slots = sigma_v.shape[0]
    chunks = width // CHUNK
    has_low, has_high = e > 0, e < energies - 1

    has_left, has_right = k > 0, k < slabs - 1

    tables = [
        pltpu.make_async_copy(source, held, local_sem.at[n])
        for n, (source, held) in enumerate(
            ((off_hbm, off_ref), (count_hbm, count_ref), (range_hbm, range_ref))
        )
    ]
    load_sigma = []
    for c in range(chunks):
        rows = slice(c * CHUNK, (c + 1) * CHUNK)
        load_sigma.append(
            pltpu.make_async_copy(
                sigma_hbm.at[0, 0, :, :, rows], sigma_v.at[:, :, rows], local_sem.at[4 + c]
            )
        )
    load_green = pltpu.make_async_copy(green_hbm.at[0, 0], green_v, local_sem.at[3])
    peers = (
        (has_left, {"slab": k - 1}),
        (has_right, {"slab": k + 1}),
        (has_low, {"energy": e - 1}),
        (has_high, {"energy": e + 1}),
        (k >= HOP, {"slab": k - HOP}),
        (k < slabs - HOP, {"slab": k + HOP}),
    )
    greet(peers)
    for table in tables:
        table.start()
    for load in load_sigma:
        load.start()

    def near_copy(slot, target):
        return pltpu.make_async_remote_copy(
            src_ref=phonon_hbm.at[0, 0],
            dst_ref=near_v.at[slot],
            send_sem=near_send.at[slot],
            recv_sem=near_recv.at[slot],
            device_id={"energy": target},
            device_id_type=MESH,
        )

    up, down = near_copy(0, e + 1), near_copy(1, e - 1)

    def remote(source, target, sent, received, slab):
        return pltpu.make_async_remote_copy(
            src_ref=source,
            dst_ref=target,
            send_sem=sent,
            recv_sem=received,
            device_id={"slab": slab},
            device_id_type=MESH,
        )

    sends = [detours(k, way, slabs) for way in range(2)]
    rides = [relayed(k, way) for way in range(2)]
    relays = [detours(rides[way], way, slabs) for way in range(2)]
    handed = [relayed(k + step, way) for way, step in ((0, -1), (1, 1))]
    hands = [there & detours(handed[way], way, slabs) for way, there in enumerate((has_left, has_right))]
    gets = [there & detours(k + step, way, slabs) for way, (there, step) in enumerate(((has_left, -1), (has_right, 1)))]
    beside = (k + 1, k - 1)
    goes, comes = (has_right, has_left), (has_left, has_right)
    got_v, back_v = (from_left_v, from_right_v), (back_left_v, back_right_v)
    units = (slice(0, 9), slice(12, 15), slice(9, 12), slice(15, 18))
    halves = (slice(0, GROUP), slice(GROUP, 2 * GROUP))
    direct, spill, returned, centre = [[], []], [[], []], [[], []], [[], []]
    for way in range(2):
        for n, these in enumerate(units):
            direct[way].append(
                remote(
                    list_v.at[way, these],
                    got_v[way].at[these],
                    unit_send.at[way, n],
                    unit_recv.at[way, n],
                    beside[way],
                )
            )
        for h, these in enumerate(halves):
            spill[way].append(
                remote(
                    list_v.at[way, LIST - (h + 1) * GROUP : LIST - h * GROUP],
                    spill_v.at[way, these],
                    spill_send.at[way, h],
                    spill_recv.at[way, h],
                    k + turned(k, way),
                )
            )
            returned[way].append(
                remote(
                    got_v[way].at[SHARED + h * GROUP : SHARED + (h + 1) * GROUP],
                    back_v[way].at[halves[1 - h]],
                    back_send.at[way, h],
                    back_recv.at[way, h],
                    handed[way] + (1, -1)[way],
                )
            )
        for n, (these, row, count) in enumerate(centre_plan(width)):
            centre[way].append(
                remote(
                    own_v.at[these, row : row + count],
                    cent_v.at[way, these, row : row + count],
                    cent_send.at[way, n],
                    cent_recv.at[way, n],
                    beside[way],
                )
            )

    def live_reach(slab, q, offset):
        live = (q < count_ref[slab]) & (off_ref[q, slab] == offset)
        return jnp.where(live, range_ref[q, slab], 0)

    def combine(wanted, with_phonon, first=0, last=width // TILE):
        reach = [[live_reach(k, q, offset) for q in range(slots)] for _, offset in wanted]

        def step(t, carry):
            rows = pl.ds(pl.multiple_of(t * TILE, TILE), TILE)
            col_ids = lax.broadcasted_iota(jnp.int32, (TILE, width), 1)
            m = lax.div(t, UNIT // TILE)
            unit_rows = pl.ds(pl.multiple_of(t * TILE - m * UNIT, TILE), TILE)
            inside = [
                [col_ids < jnp.where(t * TILE < reach[n][q], reach[n][q], 0) for q in range(slots)]
                for n in range(len(wanted))
            ]
            for part in range(2):
                terms = [sigma_v[q, part, rows, :].astype(F32) for q in range(slots)]
                for n, (at, _) in enumerate(wanted):
                    kept = [jnp.where(inside[n][q], terms[q], 0.0) for q in range(slots)]
                    total = functools.reduce(jnp.add, kept)
                    if with_phonon:
                        low = near_v[0, part, rows, :].astype(F32)
                        high = near_v[1, part, rows, :].astype(F32)
                        total = total + (0.5 * (low + high)).astype(BF16).astype(F32)
                    total = total.astype(BF16)
                    lanes = slice(part * CHUNK, (part + 1) * CHUNK)
                    for c in range(chunks):
                        value = total[:, c * CHUNK : (c + 1) * CHUNK]
                        if with_phonon:
                            own_v[c, rows, lanes] = value
                        else:
                            mine_v[at, m, c, unit_rows, lanes] = value
            return carry

        lax.fori_loop(first, last, step, 0, unroll=4)

    def layout(slab, way):
        blocks = []
        for offset in OFFSETS[2 * way : 2 * way + 2]:
            reach = functools.reduce(jnp.maximum, [live_reach(slab, q, offset) for q in range(slots)])
            blocks.append(extent(reach))
        return blocks

    def pack(way, first, last):
        (_, across_a, size_a), (_, across_b, size_b) = layout(k, way)

        def step(p, carry):
            in_a = p < size_a
            unit = jnp.where(in_a, p, jnp.maximum(p - size_a, 0))
            across = jnp.where(in_a, across_a, across_b)
            row = jnp.where(across == 3, lax.div(unit, 3), jnp.where(across == 2, lax.div(unit, 2), unit))
            col = jnp.clip(unit - row * across, 0, chunks - 1)
            row = jnp.clip(row, 0, width // UNIT - 1)
            at = 2 * way + jnp.where(in_a, 0, 1)
            keep = jnp.where(p < size_a + size_b, 1.0, 0.0).astype(BF16)
            list_v[way, p] = mine_v[at, row, col] * keep
            return carry

        lax.fori_loop(first, last, step, 0, unroll=4)

    for table in tables:
        table.wait()
    tiles = width // TILE // chunks
    for way in range(2):
        wanted = [(2 * way + n, OFFSETS[2 * way + n]) for n in range(2)]
        if way == 0:
            for c in range(chunks):
                load_sigma[c].wait()
                combine(wanted, False, c * tiles, (c + 1) * tiles)
            load_green.start()
        else:
            combine(wanted, False)
        pack(way, 0, LIST)
        if way == 0:
            greeted(peers)
        start(sends[way], spill[way][0])
        start(goes[way], direct[way][0])
        if way == 0:
            start(has_high, up)
            start(has_low, down)
    for way in range(2):
        start(sends[way], spill[way][1])

    for way in range(2):

        @pl.when(jnp.logical_not(comes[way]))
        def _():
            got_v[way][...] = jnp.zeros_like(got_v[way])
            cent_v[way] = jnp.zeros_like(cent_v[way])

        @pl.when(jnp.logical_not(gets[way]))
        def _():
            back_v[way][...] = jnp.zeros_like(back_v[way])

        @pl.when(jnp.logical_not(relays[way]))
        def _():
            spill_v[way] = jnp.zeros_like(spill_v[way])

    for there, slot in ((has_low, 0), (has_high, 1)):

        @pl.when(jnp.logical_not(there))
        def _():
            near_v[slot] = jnp.zeros_like(near_v[slot])

    load_green.wait()
    prepare(green_v, b_v, a_v, side_v)

    arrived(has_low, up)
    arrived(has_high, down)
    combine([(4, 0)], True)

    def merge(h):
        for way in range(2):
            arrived(relays[way], spill[way][h])
            for j in range(h * GROUP, (h + 1) * GROUP):
                list_v[way, SHARED + j] = list_v[way, SHARED + j] + spill_v[way, j]

    merge(0)
    for way in range(2):
        start(goes[way], direct[way][1], direct[way][2])

    for n, (at, partner) in enumerate(((2, 0), (0, 2))):
        for r in range(2):
            rows = slice(r * width // 2, (r + 1) * width // 2)
            these = slice(rows.start // UNIT, rows.stop // UNIT)
            x = None
            for c in range(chunks):
                term = dot(mine_v[at, these, c].reshape(width // 2, 2 * CHUNK), b_chunk(b_v, partner, c))
                x = term if x is None else x + term
            part_v[0, rows] = x if n == 0 else part_v[0, rows] + x
    merge(1)
    for way in range(2):
        start(goes[way], direct[way][3], *centre[way])
    def hand_back(n, h):
        for way in range(2):
            arrived(comes[way], direct[way][n])
            start(hands[way], returned[way][h])

    hand_back(1, 0)
    for r in range(chunks):
        rows = slice(r * CHUNK, (r + 1) * CHUNK)
        x = part_v[0, rows]
        for c in range(chunks):
            x = x + dot(own_v[c, rows], b_chunk(b_v, 1, c))
        put(y_v, 0, x)
        term = dot(a_v[r], y_v[: 2 * CHUNK])
        acc_v[...] = term if r == 0 else acc_v[...] + term

    hand_back(3, 1)

    def multiply(way, source, first, last, down_n, across_n, before, partner, fresh, top=0):
        for m in range(top // UNIT, width // UNIT):
            for c in range(chunks):
                position = before + m * across_n + c
                there = (m < down_n) & (c < across_n) & (position >= first) & (position < last)
                keep = jnp.where(there, 1.0, 0.0).astype(BF16)
                position = jnp.clip(position - first, 0, last - first - 1)
                block_v[c, m * UNIT : (m + 1) * UNIT] = source[position] * keep
        for row in range(top, width, width // 2):
            rows = slice(row, row + width // 2)
            x = None
            for c in range(chunks):
                term = dot(block_v[c, rows], b_chunk(b_v, partner, c))
                x = term if x is None else x + term
            part_v[way, rows] = x if fresh else part_v[way, rows] + x

    blocks = [
        layout(jnp.maximum(k - 1, 0), 0),
        layout(jnp.minimum(k + 1, slabs - 1), 1),
    ]
    for way in range(2):
        (down_a, across_a, size_a), (down_b, across_b, _) = blocks[way]
        partner_a, partner_b = ((1, 2), (1, 0))[way]
        arrived(comes[way], direct[way][0], direct[way][2])
        multiply(way, got_v[way], 0, DIRECT, down_a, across_a, 0, partner_a, True)
        multiply(way, got_v[way], 0, DIRECT, down_b, across_b, size_a, partner_b, False)

    def late():
        for way in range(2):
            (_, _, size_a), (down_b, across_b, _) = blocks[way]
            arrived(gets[way], *returned[way])
            multiply(
                way, back_v[way], DIRECT, LIST, down_b, across_b, size_a, (2, 0)[way], False, width // 2
            )

    finish(
        centre,
        comes,
        lambda way, c, rows: cent_v[way, c, rows],
        late,
        b_v,
        side_v,
        y_v,
        part_v,
        acc_v,
        out_ref,
    )

    gone(has_high, up)
    gone(has_low, down)
    for way in range(2):
        gone(goes[way], *direct[way], *centre[way])
        gone(sends[way], *spill[way])
        gone(hands[way], *returned[way])


def solution(mesh):
    slabs, energies = mesh.shape["slab"], mesh.shape["energy"]

    def body(green, sigma, phonon, pair_off, pair_count, pair_range):
        width = green.shape[-1]
        slots = sigma.shape[2]
        chunks = width // CHUNK
        pieces = len(centre_plan(width))
        hbm = pl.BlockSpec(memory_space=pltpu.HBM)
        vmem = pl.BlockSpec(memory_space=pltpu.VMEM)
        split = (chunks, width, 2 * CHUNK)
        unit = (UNIT, 2 * CHUNK)
        operands = (pair_off.T, pair_count, pair_range.T, green, sigma, phonon)
        operands = [pltpu.with_memory_space_constraint(v, pltpu.HBM) for v in operands]
        taken = [
            pltpu.SMEM((slots, slabs), jnp.int32),
            pltpu.SMEM((slabs,), jnp.int32),
            pltpu.SMEM((slots, slabs), jnp.int32),
            pltpu.VMEM((3, 2, width, width), BF16),
            pltpu.VMEM((slots, 2, width, width), BF16),
            pltpu.VMEM((2, 2, width, width), BF16),
        ]
        factors = [
            pltpu.VMEM((3, 2 * width, 2 * width), BF16),
            pltpu.VMEM(split, BF16),
            pltpu.VMEM((width // LAST, width, 4 * LAST), BF16),
            pltpu.VMEM((4 * CHUNK, 2 * width), BF16),
            pltpu.VMEM((2, width, 2 * width), F32),
            pltpu.VMEM((width, 2 * width), F32),
            pltpu.SemaphoreType.DMA((4 + chunks,)),
            pltpu.SemaphoreType.DMA((2,)),
            pltpu.SemaphoreType.DMA((2,)),
        ]

        def flags(count):
            return [pltpu.SemaphoreType.DMA((2, count))] * 2

        def call(what, number, name, blocks, semaphores, *operands):
            return pl.pallas_call(
                functools.partial(what, slabs, energies),
                out_shape=jax.ShapeDtypeStruct((1, 1, 2, width, width), F32),
                in_specs=[hbm] * 6,
                out_specs=vmem,
                scratch_shapes=taken + blocks + factors + semaphores,
                compiler_params=pltpu.CompilerParams(
                    collective_id=number, has_side_effects=True, vmem_limit_bytes=48 * 1024 * 1024
                ),
                name=name,
            )(*operands)

        straight = functools.partial(
            call,
            straight_kernel,
            0,
            "straight",
            [pltpu.VMEM((5,) + split, BF16), pltpu.VMEM((2, 3) + split, BF16)],
            flags(chunks + 1 + pieces),
        )
        around = functools.partial(
            call,
            around_kernel,
            1,
            "around",
            [
                pltpu.VMEM((4, width // UNIT, chunks) + unit, BF16),
                pltpu.VMEM(split, BF16),
                pltpu.VMEM((2, LIST) + unit, BF16),
                pltpu.VMEM((DIRECT,) + unit, BF16),
                pltpu.VMEM((DIRECT,) + unit, BF16),
                pltpu.VMEM((LIST - DIRECT,) + unit, BF16),
                pltpu.VMEM((LIST - DIRECT,) + unit, BF16),
                pltpu.VMEM((2, LIST - DIRECT) + unit, BF16),
                pltpu.VMEM((2,) + split, BF16),
                pltpu.VMEM(split, BF16),
            ],
            flags(4) + flags(2) + flags(2) + flags(pieces),
        )
        crowded = pl.pallas_call(
            crowded_kernel,
            out_shape=jax.ShapeDtypeStruct((1,), jnp.int32),
            in_specs=[vmem] * 3,
            out_specs=pl.BlockSpec(memory_space=pltpu.SMEM),
            name="crowded",
        )(pair_off.T, pair_count[None], pair_range.T)
        return lax.cond(crowded[0] > 0, straight, around, *operands)

    wide = P("energy", "slab", None, None, None, None)
    slim = P("energy", "slab", None, None, None)
    return jax.shard_map(
        body,
        mesh=mesh,
        in_specs=(wide, wide, slim, P(), P(), P()),
        out_specs=slim,
        check_vma=False,
    )
```

```python
import functools

import jax
import jax.numpy as jnp
from jax import lax
from jax.experimental import pallas as pl
from jax.experimental.pallas import tpu as pltpu
from jax.sharding import PartitionSpec as P

MESH = pl.DeviceIdType.MESH
F32 = jnp.float32
BF16 = jnp.bfloat16
TILE = 16
CHUNK = 128
LAST = 64
UNIT = 96
GROUP = 3
LIST = 24
DIRECT = 18
SHARED = 12
HOP = 4
OFFSETS = (1, 2, -1, -2)


def extent(reach):
    steps = [(reach >= n * UNIT).astype(jnp.int32) for n in range(1, 5)]
    down = steps[0] + steps[1] + steps[2] + steps[3]
    across = steps[0] + steps[1] + steps[2]
    return down, across, down * across


def turned(slab, way):
    place = lax.rem(slab, HOP)
    paired = jnp.where(lax.rem(lax.div(slab, HOP), 2) == 0, HOP, -HOP)
    if way == 0:
        return jnp.where(place == HOP - 1, -HOP, jnp.where(place == 1, paired, HOP))
    return jnp.where(place == 0, HOP, jnp.where(place == 2, paired, -HOP))


def detours(slab, way, slabs):
    low, high = (0, slabs - 2) if way == 0 else (1, slabs - 1)
    relay = slab + turned(slab, way)
    return (slab >= low) & (slab <= high) & (relay >= low) & (relay <= high)


def relayed(relay, way):
    turn = turned(relay, way)
    return relay + jnp.where(lax.rem(relay, HOP) == 1 + way, turn, -turn)


def crowded_kernel(off_ref, count_ref, range_ref, out_ref):
    off, reach = off_ref[...], range_ref[...]
    slots, slabs = off.shape
    live = lax.broadcasted_iota(jnp.int32, off.shape, 0) < count_ref[...]
    slab = lax.broadcasted_iota(jnp.int32, (1, slabs), 1)
    crowded = jnp.zeros((1, slabs), F32)
    for way in range(2):
        filled = jnp.zeros((1, slabs), jnp.int32)
        for offset in OFFSETS[2 * way : 2 * way + 2]:
            widest = jnp.max(jnp.where(live & (off == offset), reach, 0), axis=0, keepdims=True)
            filled = filled + extent(widest)[2]
        above = jnp.concatenate([filled[:, HOP:], filled[:, :HOP]], axis=1)
        below = jnp.concatenate([filled[:, -HOP:], filled[:, :-HOP]], axis=1)
        relay = jnp.where(turned(slab, way) > 0, above, below)
        room = jnp.where(filled > DIRECT + GROUP, SHARED, SHARED + GROUP)
        stuck = (relay > room) | jnp.logical_not(detours(slab, way, slabs))
        crowded = crowded + ((filled > DIRECT) & stuck).astype(F32)
    out_ref[0] = jnp.max(crowded).astype(jnp.int32)


def dot(a, b):
    return jnp.dot(a, b, preferred_element_type=F32)


def start(there, *copies):
    @pl.when(there)
    def _():
        for copy in copies:
            copy.start()


def arrived(there, *copies):
    @pl.when(there)
    def _():
        for copy in copies:
            copy.wait_recv()


def gone(there, *copies):
    @pl.when(there)
    def _():
        for copy in copies:
            copy.wait_send()


def greet(peers):
    barrier = pltpu.get_barrier_semaphore()
    for there, who in peers:

        @pl.when(there)
        def _():
            pl.semaphore_signal(barrier, inc=1, device_id=who, device_id_type=MESH)


def greeted(peers):
    barrier = pltpu.get_barrier_semaphore()
    pl.semaphore_wait(barrier, sum(there.astype(jnp.int32) for there, _ in peers))


def prepare(green_v, b_v, a_v, side_v):
    width = green_v.shape[-1]
    for at in range(3):
        for part in range(2):
            flipped = green_v[at, part].astype(F32).T
            plain = flipped.astype(BF16)
            minus = (-flipped).astype(BF16)
            for c in range(width // CHUNK):
                source = slice(c * CHUNK, (c + 1) * CHUNK)
                real = slice(2 * c * CHUNK, (2 * c + 1) * CHUNK)
                imag = slice((2 * c + 1) * CHUNK, (2 * c + 2) * CHUNK)
                if part == 0:
                    b_v[at, real, :width] = plain[source]
                    b_v[at, imag, width:] = plain[source]
                else:
                    b_v[at, real, width:] = minus[source]
                    b_v[at, imag, :width] = plain[source]
    for c in range(width // CHUNK):
        for part in range(2):
            a_v[c, :, part * CHUNK : (part + 1) * CHUNK] = green_v[1, part, :, c * CHUNK : (c + 1) * CHUNK]
    for h in range(width // LAST):
        for n, at in enumerate((0, 2)):
            side_v[h, :, 2 * n * LAST : 2 * (n + 1) * LAST] = jnp.concatenate(
                [green_v[at, part, :, h * LAST : (h + 1) * LAST] for part in range(2)], axis=1
            )


def b_chunk(b_v, at, c):
    return b_v[at, 2 * c * CHUNK : 2 * (c + 1) * CHUNK]


def put(y_v, at, x):
    rows, width = x.shape[0], x.shape[1] // 2
    real = x[:, :width].astype(BF16)
    imag = x[:, width:].astype(BF16)
    y_v[at : at + rows, :width] = real
    y_v[at : at + rows, width:] = imag
    y_v[at + rows : at + 2 * rows, :width] = -imag
    y_v[at + rows : at + 2 * rows, width:] = real


def centre_plan(width):
    whole, half, most = slice(None), width // 2, width - LAST
    plan = [(whole, 0, CHUNK), (whole, CHUNK, half - CHUNK), (whole, half, most - half)]
    return plan + [(slice(c, c + 1), most, LAST) for c in range(width // CHUNK)]


def finish(centre, comes, cent, late, b_v, side_v, y_v, part_v, acc_v, out_ref):
    width = acc_v.shape[0]
    chunks = width // CHUNK
    plan = centre_plan(width)
    for n, (these, row, count) in enumerate(plan):
        rows = slice(row, row + count)
        final = n == len(plan) - 1
        complete = these == slice(None) or final
        if row == width // 2:
            late()
        for way in range(2):
            arrived(comes[way], centre[way][n])
            x = part_v[way, rows]
            for c in range(chunks)[these]:
                x = x + dot(cent(way, c, rows), b_chunk(b_v, (0, 2)[way], c))
            if complete:
                for h in range(count // LAST):
                    put(y_v, 4 * h * LAST + 2 * way * LAST, x[h * LAST : (h + 1) * LAST])
            else:
                part_v[way, rows] = x
        if complete and not final:
            total = acc_v[...]
            for h in range(count // LAST):
                total = total + dot(side_v[row // LAST + h], y_v[4 * h * LAST : 4 * (h + 1) * LAST])
            acc_v[...] = total
    for m in range(chunks):
        rows = slice(m * CHUNK, (m + 1) * CHUNK)
        total = acc_v[rows] + dot(side_v[width // LAST - 1, rows], y_v[: 4 * LAST])
        for part in range(2):
            out_ref[0, 0, part, rows] = total[:, part * width : (part + 1) * width]


def straight_kernel(
    slabs,
    energies,
    off_hbm,
    count_hbm,
    range_hbm,
    green_hbm,
    sigma_hbm,
    phonon_hbm,
    out_ref,
    off_ref,
    count_ref,
    range_ref,
    green_v,
    sigma_v,
    near_v,
    mine_v,
    got_v,
    b_v,
    a_v,
    side_v,
    y_v,
    part_v,
    acc_v,
    local_sem,
    near_send,
    near_recv,
    send_sem,
    recv_sem,
):
    k = lax.axis_index("slab")
    e = lax.axis_index("energy")
    width = green_v.shape[-1]
    slots = sigma_v.shape[0]
    chunks = width // CHUNK
    has_low, has_high = e > 0, e < energies - 1
    has_left, has_right = k > 0, k < slabs - 1
    goes, comes = (has_right, has_left), (has_left, has_right)

    tables = [
        pltpu.make_async_copy(source, held, local_sem.at[n])
        for n, (source, held) in enumerate(
            ((off_hbm, off_ref), (count_hbm, count_ref), (range_hbm, range_ref))
        )
    ]
    load_sigma = []
    for c in range(chunks):
        rows = slice(c * CHUNK, (c + 1) * CHUNK)
        load_sigma.append(
            pltpu.make_async_copy(
                sigma_hbm.at[0, 0, :, :, rows], sigma_v.at[:, :, rows], local_sem.at[4 + c]
            )
        )
    load_green = pltpu.make_async_copy(green_hbm.at[0, 0], green_v, local_sem.at[3])

    peers = (
        (has_left, {"slab": k - 1}),
        (has_right, {"slab": k + 1}),
        (has_low, {"energy": e - 1}),
        (has_high, {"energy": e + 1}),
    )
    greet(peers)
    for table in tables:
        table.start()
    for load in load_sigma:
        load.start()

    def near_copy(slot, target):
        return pltpu.make_async_remote_copy(
            src_ref=phonon_hbm.at[0, 0],
            dst_ref=near_v.at[slot],
            send_sem=near_send.at[slot],
            recv_sem=near_recv.at[slot],
            device_id={"energy": target},
            device_id_type=MESH,
        )

    up, down = near_copy(0, e + 1), near_copy(1, e - 1)

    whole = slice(None)
    plan = [(0, whole, c * CHUNK, CHUNK) for c in range(chunks)]
    plan += [(1, whole, 0, width)]
    first_centre = len(plan)
    plan += [(2,) + piece for piece in centre_plan(width)]
    sent = [[], []]
    for way in range(2):
        for n, (slot, these, row, count) in enumerate(plan):
            source = 4 if slot == 2 else 2 * way + slot
            sent[way].append(
                pltpu.make_async_remote_copy(
                    src_ref=mine_v.at[source, these, row : row + count],
                    dst_ref=got_v.at[way, slot, these, row : row + count],
                    send_sem=send_sem.at[way, n],
                    recv_sem=recv_sem.at[way, n],
                    device_id={"slab": (k + 1, k - 1)[way]},
                    device_id_type=MESH,
                )
            )

    def combine(at, offset, with_phonon, first=0, last=width // TILE):
        reach = []
        for q in range(slots):
            live = (q < count_ref[k]) & (off_ref[q, k] == offset)
            reach.append(jnp.where(live, range_ref[q, k], 0))

        def step(t, carry):
            rows = pl.ds(pl.multiple_of(t * TILE, TILE), TILE)
            col_ids = lax.broadcasted_iota(jnp.int32, (TILE, width), 1)
            inside = [col_ids < jnp.where(t * TILE < reach[q], reach[q], 0) for q in range(slots)]
            for part in range(2):
                kept = [
                    jnp.where(inside[q], sigma_v[q, part, rows, :].astype(F32), 0.0) for q in range(slots)
                ]
                total = functools.reduce(jnp.add, kept)
                if with_phonon:
                    low = near_v[0, part, rows, :].astype(F32)
                    high = near_v[1, part, rows, :].astype(F32)
                    total = total + (0.5 * (low + high)).astype(BF16).astype(F32)
                total = total.astype(BF16)
                for c in range(chunks):
                    mine_v[at, c, rows, part * CHUNK : (part + 1) * CHUNK] = total[
                        :, c * CHUNK : (c + 1) * CHUNK
                    ]
            return carry

        lax.fori_loop(first, last, step, 0, unroll=4)

    for table in tables:
        table.wait()
    tiles = CHUNK // TILE
    for c in range(chunks):
        load_sigma[c].wait()
        for way in range(2):
            combine(2 * way, (1, -1)[way], False, c * tiles, (c + 1) * tiles)
            if c == 0 and way == 0:
                greeted(peers)
            start(goes[way], sent[way][c])
        if c == 0:
            start(has_high, up)
            start(has_low, down)
    load_green.start()
    for way in range(2):
        combine(2 * way + 1, (2, -2)[way], False)
        start(goes[way], sent[way][chunks])

    for way in range(2):

        @pl.when(jnp.logical_not(comes[way]))
        def _():
            got_v[way] = jnp.zeros_like(got_v[way])

    for there, slot in ((has_low, 0), (has_high, 1)):

        @pl.when(jnp.logical_not(there))
        def _():
            near_v[slot] = jnp.zeros_like(near_v[slot])

    load_green.wait()
    prepare(green_v, b_v, a_v, side_v)

    arrived(has_low, up)
    arrived(has_high, down)
    combine(4, 0, True)
    for way in range(2):
        start(goes[way], *sent[way][first_centre:])

    for r in range(chunks):
        rows = slice(r * CHUNK, (r + 1) * CHUNK)
        x = None
        for at, partner in ((2, 0), (4, 1), (0, 2)):
            for c in range(chunks):
                term = dot(mine_v[at, c, rows], b_chunk(b_v, partner, c))
                x = term if x is None else x + term
        put(y_v, 0, x)
        term = dot(a_v[r], y_v[: 2 * CHUNK])
        acc_v[...] = term if r == 0 else acc_v[...] + term

    for slot in range(2):
        for way in range(2):
            arrived(comes[way], *sent[way][chunks * slot : chunks + slot])
            partner = ((1, 2), (1, 0))[way][slot]
            for r in range(chunks):
                rows = slice(r * CHUNK, (r + 1) * CHUNK)
                x = None
                for c in range(chunks):
                    term = dot(got_v[way, slot, c, rows], b_chunk(b_v, partner, c))
                    x = term if x is None else x + term
                part_v[way, rows] = x if slot == 0 else part_v[way, rows] + x
    centre = [copies[first_centre:] for copies in sent]
    finish(
        centre,
        comes,
        lambda way, c, rows: got_v[way, 2, c, rows],
        lambda: None,
        b_v,
        side_v,
        y_v,
        part_v,
        acc_v,
        out_ref,
    )

    gone(has_high, up)
    gone(has_low, down)
    gone(has_right, *sent[0])
    gone(has_left, *sent[1])


def around_kernel(
    slabs,
    energies,
    off_hbm,
    count_hbm,
    range_hbm,
    green_hbm,
    sigma_hbm,
    phonon_hbm,
    out_ref,
    off_ref,
    count_ref,
    range_ref,
    green_v,
    sigma_v,
    near_v,
    mine_v,
    own_v,
    list_v,
    from_left_v,
    from_right_v,
    back_left_v,
    back_right_v,
    spill_v,
    cent_v,
    block_v,
    b_v,
    a_v,
    side_v,
    y_v,
    part_v,
    acc_v,
    local_sem,
    near_send,
    near_recv,
    unit_send,
    unit_recv,
    spill_send,
    spill_recv,
    back_send,
    back_recv,
    cent_send,
    cent_recv,
):
    k = lax.axis_index("slab")
    e = lax.axis_index("energy")
    width = green_v.shape[-1]
    slots = sigma_v.shape[2]
    chunks = width // CHUNK
    has_low, has_high = e > 0, e < energies - 1

    has_left, has_right = k > 0, k < slabs - 1

    tables = [
        pltpu.make_async_copy(source, held, local_sem.at[n])
        for n, (source, held) in enumerate(
            ((off_hbm, off_ref), (count_hbm, count_ref), (range_hbm, range_ref))
        )
    ]
    load_sigma = []
    for m in range(width // UNIT):
        for c in range(chunks):
            rows, columns = slice(m * UNIT, (m + 1) * UNIT), slice(c * CHUNK, (c + 1) * CHUNK)
            load_sigma.append(
                pltpu.make_async_copy(
                    sigma_hbm.at[0, 0, :, :, rows, columns],
                    sigma_v.at[m, c],
                    local_sem.at[4 + len(load_sigma)],
                )
            )
    load_green = pltpu.make_async_copy(green_hbm.at[0, 0], green_v, local_sem.at[3])
    peers = (
        (has_left, {"slab": k - 1}),
        (has_right, {"slab": k + 1}),
        (has_low, {"energy": e - 1}),
        (has_high, {"energy": e + 1}),
        (k >= HOP, {"slab": k - HOP}),
        (k < slabs - HOP, {"slab": k + HOP}),
    )
    greet(peers)
    for table in tables:
        table.start()
    for load in load_sigma:
        load.start()

    def near_copy(slot, target):
        return pltpu.make_async_remote_copy(
            src_ref=phonon_hbm.at[0, 0],
            dst_ref=near_v.at[slot],
            send_sem=near_send.at[slot],
            recv_sem=near_recv.at[slot],
            device_id={"energy": target},
            device_id_type=MESH,
        )

    up, down = near_copy(0, e + 1), near_copy(1, e - 1)

    def remote(source, target, sent, received, slab):
        return pltpu.make_async_remote_copy(
            src_ref=source,
            dst_ref=target,
            send_sem=sent,
            recv_sem=received,
            device_id={"slab": slab},
            device_id_type=MESH,
        )

    sends = [detours(k, way, slabs) for way in range(2)]
    rides = [relayed(k, way) for way in range(2)]
    relays = [detours(rides[way], way, slabs) for way in range(2)]
    handed = [relayed(k + step, way) for way, step in ((0, -1), (1, 1))]
    hands = [there & detours(handed[way], way, slabs) for way, there in enumerate((has_left, has_right))]
    gets = [there & detours(k + step, way, slabs) for way, (there, step) in enumerate(((has_left, -1), (has_right, 1)))]
    beside = (k + 1, k - 1)
    goes, comes = (has_right, has_left), (has_left, has_right)
    got_v, back_v = (from_left_v, from_right_v), (back_left_v, back_right_v)
    units = (slice(0, 9), slice(12, 15), slice(9, 12), slice(15, 18))
    halves = (slice(0, GROUP), slice(GROUP, 2 * GROUP))
    direct, spill, returned, centre = [[], []], [[], []], [[], []], [[], []]
    for way in range(2):
        for n, these in enumerate(units):
            direct[way].append(
                remote(
                    list_v.at[way, these],
                    got_v[way].at[these],
                    unit_send.at[way, n],
                    unit_recv.at[way, n],
                    beside[way],
                )
            )
        for h, these in enumerate(halves):
            spill[way].append(
                remote(
                    list_v.at[way, LIST - (h + 1) * GROUP : LIST - h * GROUP],
                    spill_v.at[way, these],
                    spill_send.at[way, h],
                    spill_recv.at[way, h],
                    k + turned(k, way),
                )
            )
            returned[way].append(
                remote(
                    got_v[way].at[SHARED + h * GROUP : SHARED + (h + 1) * GROUP],
                    back_v[way].at[halves[1 - h]],
                    back_send.at[way, h],
                    back_recv.at[way, h],
                    handed[way] + (1, -1)[way],
                )
            )
        for n, (these, row, count) in enumerate(centre_plan(width)):
            centre[way].append(
                remote(
                    own_v.at[these, row : row + count],
                    cent_v.at[way, these, row : row + count],
                    cent_send.at[way, n],
                    cent_recv.at[way, n],
                    beside[way],
                )
            )

    def live_reach(slab, q, offset):
        live = (q < count_ref[slab]) & (off_ref[q, slab] == offset)
        return jnp.where(live, range_ref[q, slab], 0)

    def unit_sum(m, c, reach):
        column = c * CHUNK + lax.broadcasted_iota(jnp.int32, (UNIT, CHUNK), 1)
        inside = [column < jnp.where(m * UNIT < reach[q], reach[q], 0) for q in range(slots)]
        return [
            functools.reduce(
                jnp.add,
                [jnp.where(inside[q], sigma_v[m, c, q, part].astype(F32), 0.0) for q in range(slots)],
            )
            for part in range(2)
        ]

    def reaches(offset):
        return [live_reach(k, q, offset) for q in range(slots)]

    def sum_sides():
        wanted = [reaches(-1), reaches(1)]

        def step(m, carry):
            for c in range(chunks):
                for at in range(2):
                    for part, value in enumerate(unit_sum(m, c, wanted[at])):
                        mine_v[at, m, c, :, part * CHUNK : (part + 1) * CHUNK] = value.astype(BF16)
            return carry

        lax.fori_loop(0, width // UNIT, step, 0)

    def sum_own():
        reach = reaches(0)

        def step(m, carry):
            rows = pl.ds(pl.multiple_of(m * UNIT, UNIT), UNIT)
            for c in range(chunks):
                columns = slice(c * CHUNK, (c + 1) * CHUNK)
                for part, value in enumerate(unit_sum(m, c, reach)):
                    low = near_v[0, part, rows, columns].astype(F32)
                    high = near_v[1, part, rows, columns].astype(F32)
                    value = value + (0.5 * (low + high)).astype(BF16).astype(F32)
                    own_v[c, rows, part * CHUNK : (part + 1) * CHUNK] = value.astype(BF16)
            return carry

        lax.fori_loop(0, width // UNIT, step, 0)

    def layout(slab, way):
        blocks = []
        for offset in OFFSETS[2 * way : 2 * way + 2]:
            reach = functools.reduce(jnp.maximum, [live_reach(slab, q, offset) for q in range(slots)])
            blocks.append(extent(reach))
        return blocks

    def pack(way, first, last):
        (_, across_a, size_a), (_, across_b, size_b) = layout(k, way)
        reach_a, reach_b = [reaches(offset) for offset in OFFSETS[2 * way : 2 * way + 2]]

        def step(p, carry):
            in_a = p < size_a
            unit = jnp.where(in_a, p, jnp.maximum(p - size_a, 0))
            across = jnp.where(in_a, across_a, across_b)
            row = jnp.where(across == 3, lax.div(unit, 3), jnp.where(across == 2, lax.div(unit, 2), unit))
            col = jnp.clip(unit - row * across, 0, chunks - 1)
            row = jnp.clip(row, 0, width // UNIT - 1)
            used = p < size_a + size_b
            reach = [
                jnp.where(used, jnp.where(in_a, reach_a[q], reach_b[q]), 0) for q in range(slots)
            ]
            for part, value in enumerate(unit_sum(row, col, reach)):
                list_v[way, p, :, part * CHUNK : (part + 1) * CHUNK] = value.astype(BF16)
            return carry

        lax.fori_loop(first, last, step, 0, unroll=3)

    for table in tables:
        table.wait()
    for load in load_sigma:
        load.wait()
    load_green.start()
    for way in range(2):
        pack(way, 0, 9)
        if way == 0:
            greeted(peers)
        start(goes[way], direct[way][0])
    for way in range(2):
        pack(way, DIRECT, LIST)
        start(sends[way], spill[way][0])
    start(has_high, up)
    start(has_low, down)
    for way in range(2):
        start(sends[way], spill[way][1])
        pack(way, 9, DIRECT)

    for way in range(2):

        @pl.when(jnp.logical_not(comes[way]))
        def _():
            got_v[way][...] = jnp.zeros_like(got_v[way])
            cent_v[way] = jnp.zeros_like(cent_v[way])

        @pl.when(jnp.logical_not(gets[way]))
        def _():
            back_v[way][...] = jnp.zeros_like(back_v[way])

        @pl.when(jnp.logical_not(relays[way]))
        def _():
            spill_v[way] = jnp.zeros_like(spill_v[way])

    for there, slot in ((has_low, 0), (has_high, 1)):

        @pl.when(jnp.logical_not(there))
        def _():
            near_v[slot] = jnp.zeros_like(near_v[slot])

    sum_sides()
    load_green.wait()
    prepare(green_v, b_v, a_v, side_v)

    arrived(has_low, up)
    arrived(has_high, down)
    sum_own()

    def merge(h):
        for way in range(2):
            arrived(relays[way], spill[way][h])
            for j in range(h * GROUP, (h + 1) * GROUP):
                list_v[way, SHARED + j] = list_v[way, SHARED + j] + spill_v[way, j]

    merge(0)
    for way in range(2):
        start(goes[way], direct[way][1], direct[way][2])

    for at, partner in enumerate((0, 2)):
        for r in range(2):
            rows = slice(r * width // 2, (r + 1) * width // 2)
            these = slice(rows.start // UNIT, rows.stop // UNIT)
            x = None
            for c in range(chunks):
                term = dot(mine_v[at, these, c].reshape(width // 2, 2 * CHUNK), b_chunk(b_v, partner, c))
                x = term if x is None else x + term
            part_v[0, rows] = x if at == 0 else part_v[0, rows] + x
    merge(1)
    for way in range(2):
        start(goes[way], direct[way][3], *centre[way])
    def hand_back(n, h):
        for way in range(2):
            arrived(comes[way], direct[way][n])
            start(hands[way], returned[way][h])

    hand_back(1, 0)
    for r in range(chunks):
        rows = slice(r * CHUNK, (r + 1) * CHUNK)
        x = part_v[0, rows]
        for c in range(chunks):
            x = x + dot(own_v[c, rows], b_chunk(b_v, 1, c))
        put(y_v, 0, x)
        term = dot(a_v[r], y_v[: 2 * CHUNK])
        acc_v[...] = term if r == 0 else acc_v[...] + term

    hand_back(3, 1)

    def multiply(way, source, first, last, down_n, across_n, before, partner, fresh, top=0):
        for m in range(top // UNIT, width // UNIT):
            for c in range(chunks):
                position = before + m * across_n + c
                there = (m < down_n) & (c < across_n) & (position >= first) & (position < last)
                keep = jnp.where(there, 1.0, 0.0).astype(BF16)
                position = jnp.clip(position - first, 0, last - first - 1)
                block_v[c, m * UNIT : (m + 1) * UNIT] = source[position] * keep
        for row in range(top, width, width // 2):
            rows = slice(row, row + width // 2)
            x = None
            for c in range(chunks):
                term = dot(block_v[c, rows], b_chunk(b_v, partner, c))
                x = term if x is None else x + term
            part_v[way, rows] = x if fresh else part_v[way, rows] + x

    blocks = [
        layout(jnp.maximum(k - 1, 0), 0),
        layout(jnp.minimum(k + 1, slabs - 1), 1),
    ]
    for way in range(2):
        (down_a, across_a, size_a), (down_b, across_b, _) = blocks[way]
        partner_a, partner_b = ((1, 2), (1, 0))[way]
        arrived(comes[way], direct[way][0], direct[way][2])
        multiply(way, got_v[way], 0, DIRECT, down_a, across_a, 0, partner_a, True)
        multiply(way, got_v[way], 0, DIRECT, down_b, across_b, size_a, partner_b, False)

    def late():
        for way in range(2):
            (_, _, size_a), (down_b, across_b, _) = blocks[way]
            arrived(gets[way], *returned[way])
            multiply(
                way, back_v[way], DIRECT, LIST, down_b, across_b, size_a, (2, 0)[way], False, width // 2
            )

    finish(
        centre,
        comes,
        lambda way, c, rows: cent_v[way, c, rows],
        late,
        b_v,
        side_v,
        y_v,
        part_v,
        acc_v,
        out_ref,
    )

    gone(has_high, up)
    gone(has_low, down)
    for way in range(2):
        gone(goes[way], *direct[way], *centre[way])
        gone(sends[way], *spill[way])
        gone(hands[way], *returned[way])


def solution(mesh):
    slabs, energies = mesh.shape["slab"], mesh.shape["energy"]

    def body(green, sigma, phonon, pair_off, pair_count, pair_range):
        width = green.shape[-1]
        slots = sigma.shape[2]
        chunks = width // CHUNK
        pieces = len(centre_plan(width))
        hbm = pl.BlockSpec(memory_space=pltpu.HBM)
        vmem = pl.BlockSpec(memory_space=pltpu.VMEM)
        split = (chunks, width, 2 * CHUNK)
        unit = (UNIT, 2 * CHUNK)
        operands = (pair_off.T, pair_count, pair_range.T, green, sigma, phonon)
        operands = [pltpu.with_memory_space_constraint(v, pltpu.HBM) for v in operands]
        taken = [
            pltpu.SMEM((slots, slabs), jnp.int32),
            pltpu.SMEM((slabs,), jnp.int32),
            pltpu.SMEM((slots, slabs), jnp.int32),
            pltpu.VMEM((3, 2, width, width), BF16),
        ]
        near = pltpu.VMEM((2, 2, width, width), BF16)
        factors = [
            pltpu.VMEM((3, 2 * width, 2 * width), BF16),
            pltpu.VMEM(split, BF16),
            pltpu.VMEM((width // LAST, width, 4 * LAST), BF16),
            pltpu.VMEM((4 * CHUNK, 2 * width), BF16),
            pltpu.VMEM((2, width, 2 * width), F32),
            pltpu.VMEM((width, 2 * width), F32),
            pltpu.SemaphoreType.DMA((4 + chunks * (width // UNIT),)),
            pltpu.SemaphoreType.DMA((2,)),
            pltpu.SemaphoreType.DMA((2,)),
        ]

        def flags(count):
            return [pltpu.SemaphoreType.DMA((2, count))] * 2

        def call(what, number, name, blocks, semaphores, *operands):
            return pl.pallas_call(
                functools.partial(what, slabs, energies),
                out_shape=jax.ShapeDtypeStruct((1, 1, 2, width, width), F32),
                in_specs=[hbm] * 6,
                out_specs=vmem,
                scratch_shapes=taken + blocks + factors + semaphores,
                compiler_params=pltpu.CompilerParams(
                    collective_id=number, has_side_effects=True, vmem_limit_bytes=48 * 1024 * 1024
                ),
                name=name,
            )(*operands)

        straight = functools.partial(
            call,
            straight_kernel,
            0,
            "straight",
            [
                pltpu.VMEM((slots, 2, width, width), BF16),
                near,
                pltpu.VMEM((5,) + split, BF16),
                pltpu.VMEM((2, 3) + split, BF16),
            ],
            flags(chunks + 1 + pieces),
        )
        around = functools.partial(
            call,
            around_kernel,
            1,
            "around",
            [
                pltpu.VMEM((width // UNIT, chunks, slots, 2, UNIT, CHUNK), BF16),
                near,
                pltpu.VMEM((2, width // UNIT, chunks) + unit, BF16),
                pltpu.VMEM(split, BF16),
                pltpu.VMEM((2, LIST) + unit, BF16),
                pltpu.VMEM((DIRECT,) + unit, BF16),
                pltpu.VMEM((DIRECT,) + unit, BF16),
                pltpu.VMEM((LIST - DIRECT,) + unit, BF16),
                pltpu.VMEM((LIST - DIRECT,) + unit, BF16),
                pltpu.VMEM((2, LIST - DIRECT) + unit, BF16),
                pltpu.VMEM((2,) + split, BF16),
                pltpu.VMEM(split, BF16),
            ],
            flags(4) + flags(2) + flags(2) + flags(pieces),
        )
        crowded = pl.pallas_call(
            crowded_kernel,
            out_shape=jax.ShapeDtypeStruct((1,), jnp.int32),
            in_specs=[vmem] * 3,
            out_specs=pl.BlockSpec(memory_space=pltpu.SMEM),
            name="crowded",
        )(pair_off.T, pair_count[None], pair_range.T)
        return lax.cond(crowded[0] > 0, straight, around, *operands)

    wide = P("energy", "slab", None, None, None, None)
    slim = P("energy", "slab", None, None, None)
    return jax.shard_map(
        body,
        mesh=mesh,
        in_specs=(wide, wide, slim, P(), P(), P()),
        out_specs=slim,
        check_vma=False,
    )
```

```python
import functools

import jax
import jax.numpy as jnp
from jax import lax
from jax.experimental import pallas as pl
from jax.experimental.pallas import tpu as pltpu
from jax.sharding import PartitionSpec as P

MESH = pl.DeviceIdType.MESH
F32 = jnp.float32
BF16 = jnp.bfloat16
TILE = 16
CHUNK = 128
LAST = 64
UNIT = 96
GROUP = 3
LIST = 24
DIRECT = 18
SHARED = 12
HOP = 4
OFFSETS = (1, 2, -1, -2)


def extent(reach):
    steps = [(reach >= n * UNIT).astype(jnp.int32) for n in range(1, 5)]
    down = steps[0] + steps[1] + steps[2] + steps[3]
    across = steps[0] + steps[1] + steps[2]
    return down, across, down * across


def turned(slab, way):
    place = lax.rem(slab, HOP)
    paired = jnp.where(lax.rem(lax.div(slab, HOP), 2) == 0, HOP, -HOP)
    if way == 0:
        return jnp.where(place == HOP - 1, -HOP, jnp.where(place == 1, paired, HOP))
    return jnp.where(place == 0, HOP, jnp.where(place == 2, paired, -HOP))


def detours(slab, way, slabs):
    low, high = (0, slabs - 2) if way == 0 else (1, slabs - 1)
    relay = slab + turned(slab, way)
    return (slab >= low) & (slab <= high) & (relay >= low) & (relay <= high)


def relayed(relay, way):
    turn = turned(relay, way)
    return relay + jnp.where(lax.rem(relay, HOP) == 1 + way, turn, -turn)


def crowded_kernel(off_ref, count_ref, range_ref, out_ref):
    off, reach = off_ref[...], range_ref[...]
    slots, slabs = off.shape
    live = lax.broadcasted_iota(jnp.int32, off.shape, 0) < count_ref[...]
    slab = lax.broadcasted_iota(jnp.int32, (1, slabs), 1)
    crowded = jnp.zeros((1, slabs), F32)
    for way in range(2):
        filled = jnp.zeros((1, slabs), jnp.int32)
        for offset in OFFSETS[2 * way : 2 * way + 2]:
            widest = jnp.max(jnp.where(live & (off == offset), reach, 0), axis=0, keepdims=True)
            filled = filled + extent(widest)[2]
        above = jnp.concatenate([filled[:, HOP:], filled[:, :HOP]], axis=1)
        below = jnp.concatenate([filled[:, -HOP:], filled[:, :-HOP]], axis=1)
        relay = jnp.where(turned(slab, way) > 0, above, below)
        room = jnp.where(filled > DIRECT + GROUP, SHARED, SHARED + GROUP)
        stuck = (relay > room) | jnp.logical_not(detours(slab, way, slabs))
        crowded = crowded + ((filled > DIRECT) & stuck).astype(F32)
    out_ref[0] = jnp.max(crowded).astype(jnp.int32)


def dot(a, b):
    return jnp.dot(a, b, preferred_element_type=F32)


def start(there, *copies):
    @pl.when(there)
    def _():
        for copy in copies:
            copy.start()


def arrived(there, *copies):
    @pl.when(there)
    def _():
        for copy in copies:
            copy.wait_recv()


def gone(there, *copies):
    @pl.when(there)
    def _():
        for copy in copies:
            copy.wait_send()


def greet(peers):
    barrier = pltpu.get_barrier_semaphore()
    for there, who in peers:

        @pl.when(there)
        def _():
            pl.semaphore_signal(barrier, inc=1, device_id=who, device_id_type=MESH)


def greeted(peers):
    barrier = pltpu.get_barrier_semaphore()
    pl.semaphore_wait(barrier, sum(there.astype(jnp.int32) for there, _ in peers))


def prepare(green_v, b_v, a_v, side_v):
    width = green_v.shape[-1]
    for at in range(3):
        for part in range(2):
            flipped = green_v[at, part].astype(F32).T
            plain = flipped.astype(BF16)
            minus = (-flipped).astype(BF16)
            for c in range(width // CHUNK):
                source = slice(c * CHUNK, (c + 1) * CHUNK)
                real = slice(2 * c * CHUNK, (2 * c + 1) * CHUNK)
                imag = slice((2 * c + 1) * CHUNK, (2 * c + 2) * CHUNK)
                if part == 0:
                    b_v[at, real, :width] = plain[source]
                    b_v[at, imag, width:] = plain[source]
                else:
                    b_v[at, real, width:] = minus[source]
                    b_v[at, imag, :width] = plain[source]
    for c in range(width // CHUNK):
        for part in range(2):
            a_v[c, :, part * CHUNK : (part + 1) * CHUNK] = green_v[1, part, :, c * CHUNK : (c + 1) * CHUNK]
    for h in range(width // LAST):
        for n, at in enumerate((0, 2)):
            side_v[h, :, 2 * n * LAST : 2 * (n + 1) * LAST] = jnp.concatenate(
                [green_v[at, part, :, h * LAST : (h + 1) * LAST] for part in range(2)], axis=1
            )


def b_chunk(b_v, at, c):
    return b_v[at, 2 * c * CHUNK : 2 * (c + 1) * CHUNK]


def put(y_v, at, x):
    rows, width = x.shape[0], x.shape[1] // 2
    real = x[:, :width].astype(BF16)
    imag = x[:, width:].astype(BF16)
    y_v[at : at + rows, :width] = real
    y_v[at : at + rows, width:] = imag
    y_v[at + rows : at + 2 * rows, :width] = -imag
    y_v[at + rows : at + 2 * rows, width:] = real


def centre_plan(width):
    whole, half, most = slice(None), width // 2, width - LAST
    plan = [(whole, 0, CHUNK), (whole, CHUNK, half - CHUNK), (whole, half, most - half)]
    return plan + [(slice(c, c + 1), most, LAST) for c in range(width // CHUNK)]


def finish(centre, comes, cent, late, b_v, side_v, y_v, part_v, acc_v, out_ref):
    width = acc_v.shape[0]
    chunks = width // CHUNK
    plan = centre_plan(width)
    for n, (these, row, count) in enumerate(plan):
        rows = slice(row, row + count)
        final = n == len(plan) - 1
        complete = these == slice(None) or final
        if row == width // 2:
            late()
        for way in range(2):
            arrived(comes[way], centre[way][n])
            x = part_v[way, rows]
            for c in range(chunks)[these]:
                x = x + dot(cent(way, c, rows), b_chunk(b_v, (0, 2)[way], c))
            if complete:
                for h in range(count // LAST):
                    put(y_v, 4 * h * LAST + 2 * way * LAST, x[h * LAST : (h + 1) * LAST])
            else:
                part_v[way, rows] = x
        if complete and not final:
            total = acc_v[...]
            for h in range(count // LAST):
                total = total + dot(side_v[row // LAST + h], y_v[4 * h * LAST : 4 * (h + 1) * LAST])
            acc_v[...] = total
    for m in range(chunks):
        rows = slice(m * CHUNK, (m + 1) * CHUNK)
        total = acc_v[rows] + dot(side_v[width // LAST - 1, rows], y_v[: 4 * LAST])
        for part in range(2):
            out_ref[0, 0, part, rows] = total[:, part * width : (part + 1) * width]


def straight_kernel(
    slabs,
    energies,
    off_hbm,
    count_hbm,
    range_hbm,
    green_hbm,
    sigma_hbm,
    phonon_hbm,
    out_ref,
    off_ref,
    count_ref,
    range_ref,
    green_v,
    sigma_v,
    near_v,
    mine_v,
    got_v,
    b_v,
    a_v,
    side_v,
    y_v,
    part_v,
    acc_v,
    local_sem,
    near_send,
    near_recv,
    send_sem,
    recv_sem,
):
    k = lax.axis_index("slab")
    e = lax.axis_index("energy")
    width = green_v.shape[-1]
    slots = sigma_v.shape[0]
    chunks = width // CHUNK
    has_low, has_high = e > 0, e < energies - 1
    has_left, has_right = k > 0, k < slabs - 1
    goes, comes = (has_right, has_left), (has_left, has_right)

    tables = [
        pltpu.make_async_copy(source, held, local_sem.at[n])
        for n, (source, held) in enumerate(
            ((off_hbm, off_ref), (count_hbm, count_ref), (range_hbm, range_ref))
        )
    ]
    load_sigma = []
    for c in range(chunks):
        rows = slice(c * CHUNK, (c + 1) * CHUNK)
        load_sigma.append(
            pltpu.make_async_copy(
                sigma_hbm.at[0, 0, :, :, rows], sigma_v.at[:, :, rows], local_sem.at[4 + c]
            )
        )
    load_green = pltpu.make_async_copy(green_hbm.at[0, 0], green_v, local_sem.at[3])

    peers = (
        (has_left, {"slab": k - 1}),
        (has_right, {"slab": k + 1}),
        (has_low, {"energy": e - 1}),
        (has_high, {"energy": e + 1}),
    )
    greet(peers)
    for table in tables:
        table.start()
    for load in load_sigma:
        load.start()

    def near_copy(slot, target):
        return pltpu.make_async_remote_copy(
            src_ref=phonon_hbm.at[0, 0],
            dst_ref=near_v.at[slot],
            send_sem=near_send.at[slot],
            recv_sem=near_recv.at[slot],
            device_id={"energy": target},
            device_id_type=MESH,
        )

    up, down = near_copy(0, e + 1), near_copy(1, e - 1)

    whole = slice(None)
    plan = [(0, whole, c * CHUNK, CHUNK) for c in range(chunks)]
    plan += [(1, whole, 0, width)]
    first_centre = len(plan)
    plan += [(2,) + piece for piece in centre_plan(width)]
    sent = [[], []]
    for way in range(2):
        for n, (slot, these, row, count) in enumerate(plan):
            source = 4 if slot == 2 else 2 * way + slot
            sent[way].append(
                pltpu.make_async_remote_copy(
                    src_ref=mine_v.at[source, these, row : row + count],
                    dst_ref=got_v.at[way, slot, these, row : row + count],
                    send_sem=send_sem.at[way, n],
                    recv_sem=recv_sem.at[way, n],
                    device_id={"slab": (k + 1, k - 1)[way]},
                    device_id_type=MESH,
                )
            )

    def combine(at, offset, with_phonon, first=0, last=width // TILE):
        reach = []
        for q in range(slots):
            live = (q < count_ref[k]) & (off_ref[q, k] == offset)
            reach.append(jnp.where(live, range_ref[q, k], 0))

        def step(t, carry):
            rows = pl.ds(pl.multiple_of(t * TILE, TILE), TILE)
            col_ids = lax.broadcasted_iota(jnp.int32, (TILE, width), 1)
            inside = [col_ids < jnp.where(t * TILE < reach[q], reach[q], 0) for q in range(slots)]
            for part in range(2):
                kept = [
                    jnp.where(inside[q], sigma_v[q, part, rows, :].astype(F32), 0.0) for q in range(slots)
                ]
                total = functools.reduce(jnp.add, kept)
                if with_phonon:
                    low = near_v[0, part, rows, :].astype(F32)
                    high = near_v[1, part, rows, :].astype(F32)
                    total = total + (0.5 * (low + high)).astype(BF16).astype(F32)
                total = total.astype(BF16)
                for c in range(chunks):
                    mine_v[at, c, rows, part * CHUNK : (part + 1) * CHUNK] = total[
                        :, c * CHUNK : (c + 1) * CHUNK
                    ]
            return carry

        lax.fori_loop(first, last, step, 0, unroll=4)

    for table in tables:
        table.wait()
    tiles = CHUNK // TILE
    for c in range(chunks):
        load_sigma[c].wait()
        for way in range(2):
            combine(2 * way, (1, -1)[way], False, c * tiles, (c + 1) * tiles)
            if c == 0 and way == 0:
                greeted(peers)
            start(goes[way], sent[way][c])
        if c == 0:
            start(has_high, up)
            start(has_low, down)
    load_green.start()
    for way in range(2):
        combine(2 * way + 1, (2, -2)[way], False)
        start(goes[way], sent[way][chunks])

    for way in range(2):

        @pl.when(jnp.logical_not(comes[way]))
        def _():
            got_v[way] = jnp.zeros_like(got_v[way])

    for there, slot in ((has_low, 0), (has_high, 1)):

        @pl.when(jnp.logical_not(there))
        def _():
            near_v[slot] = jnp.zeros_like(near_v[slot])

    load_green.wait()
    prepare(green_v, b_v, a_v, side_v)

    arrived(has_low, up)
    arrived(has_high, down)
    combine(4, 0, True)
    for way in range(2):
        start(goes[way], *sent[way][first_centre:])

    for r in range(chunks):
        rows = slice(r * CHUNK, (r + 1) * CHUNK)
        x = None
        for at, partner in ((2, 0), (4, 1), (0, 2)):
            for c in range(chunks):
                term = dot(mine_v[at, c, rows], b_chunk(b_v, partner, c))
                x = term if x is None else x + term
        put(y_v, 0, x)
        term = dot(a_v[r], y_v[: 2 * CHUNK])
        acc_v[...] = term if r == 0 else acc_v[...] + term

    for slot in range(2):
        for way in range(2):
            arrived(comes[way], *sent[way][chunks * slot : chunks + slot])
            partner = ((1, 2), (1, 0))[way][slot]
            for r in range(chunks):
                rows = slice(r * CHUNK, (r + 1) * CHUNK)
                x = None
                for c in range(chunks):
                    term = dot(got_v[way, slot, c, rows], b_chunk(b_v, partner, c))
                    x = term if x is None else x + term
                part_v[way, rows] = x if slot == 0 else part_v[way, rows] + x
    centre = [copies[first_centre:] for copies in sent]
    finish(
        centre,
        comes,
        lambda way, c, rows: got_v[way, 2, c, rows],
        lambda: None,
        b_v,
        side_v,
        y_v,
        part_v,
        acc_v,
        out_ref,
    )

    gone(has_high, up)
    gone(has_low, down)
    gone(has_right, *sent[0])
    gone(has_left, *sent[1])


def around_kernel(
    slabs,
    energies,
    off_hbm,
    count_hbm,
    range_hbm,
    green_hbm,
    sigma_hbm,
    phonon_hbm,
    out_ref,
    off_ref,
    count_ref,
    range_ref,
    green_v,
    sigma_v,
    near_v,
    mine_v,
    own_v,
    list_v,
    from_left_v,
    from_right_v,
    back_left_v,
    back_right_v,
    spill_v,
    cent_v,
    block_v,
    b_v,
    a_v,
    side_v,
    y_v,
    part_v,
    acc_v,
    local_sem,
    near_send,
    near_recv,
    unit_send,
    unit_recv,
    spill_send,
    spill_recv,
    back_send,
    back_recv,
    cent_send,
    cent_recv,
):
    k = lax.axis_index("slab")
    e = lax.axis_index("energy")
    width = green_v.shape[-1]
    slots = sigma_v.shape[2]
    chunks = width // CHUNK
    has_low, has_high = e > 0, e < energies - 1

    has_left, has_right = k > 0, k < slabs - 1

    tables = [
        pltpu.make_async_copy(source, held, local_sem.at[n])
        for n, (source, held) in enumerate(
            ((off_hbm, off_ref), (count_hbm, count_ref), (range_hbm, range_ref))
        )
    ]
    load_sigma = []
    for m in range(width // UNIT):
        for c in range(chunks):
            rows, columns = slice(m * UNIT, (m + 1) * UNIT), slice(c * CHUNK, (c + 1) * CHUNK)
            load_sigma.append(
                pltpu.make_async_copy(
                    sigma_hbm.at[0, 0, :, :, rows, columns],
                    sigma_v.at[m, c],
                    local_sem.at[4 + len(load_sigma)],
                )
            )
    load_green = pltpu.make_async_copy(green_hbm.at[0, 0], green_v, local_sem.at[3])
    peers = (
        (has_left, {"slab": k - 1}),
        (has_right, {"slab": k + 1}),
        (has_low, {"energy": e - 1}),
        (has_high, {"energy": e + 1}),
        (k >= HOP, {"slab": k - HOP}),
        (k < slabs - HOP, {"slab": k + HOP}),
    )
    greet(peers)
    for table in tables:
        table.start()
    for load in load_sigma:
        load.start()

    def near_copy(slot, target):
        return pltpu.make_async_remote_copy(
            src_ref=phonon_hbm.at[0, 0],
            dst_ref=near_v.at[slot],
            send_sem=near_send.at[slot],
            recv_sem=near_recv.at[slot],
            device_id={"energy": target},
            device_id_type=MESH,
        )

    up, down = near_copy(0, e + 1), near_copy(1, e - 1)

    def remote(source, target, sent, received, slab):
        return pltpu.make_async_remote_copy(
            src_ref=source,
            dst_ref=target,
            send_sem=sent,
            recv_sem=received,
            device_id={"slab": slab},
            device_id_type=MESH,
        )

    sends = [detours(k, way, slabs) for way in range(2)]
    rides = [relayed(k, way) for way in range(2)]
    relays = [detours(rides[way], way, slabs) for way in range(2)]
    handed = [relayed(k + step, way) for way, step in ((0, -1), (1, 1))]
    hands = [there & detours(handed[way], way, slabs) for way, there in enumerate((has_left, has_right))]
    gets = [there & detours(k + step, way, slabs) for way, (there, step) in enumerate(((has_left, -1), (has_right, 1)))]
    beside = (k + 1, k - 1)
    goes, comes = (has_right, has_left), (has_left, has_right)
    got_v, back_v = (from_left_v, from_right_v), (back_left_v, back_right_v)
    units = (slice(0, 9), slice(12, 15), slice(9, 12), slice(15, 18))
    halves = (slice(0, GROUP), slice(GROUP, 2 * GROUP))
    direct, spill, returned, centre = [[], []], [[], []], [[], []], [[], []]
    for way in range(2):
        for n, these in enumerate(units):
            direct[way].append(
                remote(
                    list_v.at[way, these],
                    got_v[way].at[these],
                    unit_send.at[way, n],
                    unit_recv.at[way, n],
                    beside[way],
                )
            )
        for h, these in enumerate(halves):
            spill[way].append(
                remote(
                    list_v.at[way, LIST - (h + 1) * GROUP : LIST - h * GROUP],
                    spill_v.at[way, these],
                    spill_send.at[way, h],
                    spill_recv.at[way, h],
                    k + turned(k, way),
                )
            )
            returned[way].append(
                remote(
                    got_v[way].at[SHARED + h * GROUP : SHARED + (h + 1) * GROUP],
                    back_v[way].at[halves[1 - h]],
                    back_send.at[way, h],
                    back_recv.at[way, h],
                    handed[way] + (1, -1)[way],
                )
            )
        for n, (these, row, count) in enumerate(centre_plan(width)):
            centre[way].append(
                remote(
                    own_v.at[these, row : row + count],
                    cent_v.at[way, these, row : row + count],
                    cent_send.at[way, n],
                    cent_recv.at[way, n],
                    beside[way],
                )
            )

    def live_reach(slab, q, offset):
        live = (q < count_ref[slab]) & (off_ref[q, slab] == offset)
        return jnp.where(live, range_ref[q, slab], 0)

    def unit_sum(m, c, reach):
        column = c * CHUNK + lax.broadcasted_iota(jnp.int32, (UNIT, CHUNK), 1)
        inside = [column < jnp.where(m * UNIT < reach[q], reach[q], 0) for q in range(slots)]
        return [
            functools.reduce(
                jnp.add,
                [jnp.where(inside[q], sigma_v[m, c, q, part].astype(F32), 0.0) for q in range(slots)],
            )
            for part in range(2)
        ]

    def reaches(offset):
        return [live_reach(k, q, offset) for q in range(slots)]

    def sum_sides():
        wanted = [reaches(-1), reaches(1)]

        def step(m, carry):
            for c in range(chunks):
                for at in range(2):
                    for part, value in enumerate(unit_sum(m, c, wanted[at])):
                        mine_v[at, m, c, :, part * CHUNK : (part + 1) * CHUNK] = value.astype(BF16)
            return carry

        lax.fori_loop(0, width // UNIT, step, 0)

    def sum_own():
        reach = reaches(0)

        def step(m, carry):
            rows = pl.ds(pl.multiple_of(m * UNIT, UNIT), UNIT)
            for c in range(chunks):
                columns = slice(c * CHUNK, (c + 1) * CHUNK)
                for part, value in enumerate(unit_sum(m, c, reach)):
                    low = near_v[0, part, rows, columns].astype(F32)
                    high = near_v[1, part, rows, columns].astype(F32)
                    value = value + (0.5 * (low + high)).astype(BF16).astype(F32)
                    own_v[c, rows, part * CHUNK : (part + 1) * CHUNK] = value.astype(BF16)
            return carry

        lax.fori_loop(0, width // UNIT, step, 0)

    def layout(slab, way):
        blocks = []
        for offset in OFFSETS[2 * way : 2 * way + 2]:
            reach = functools.reduce(jnp.maximum, [live_reach(slab, q, offset) for q in range(slots)])
            blocks.append(extent(reach))
        return blocks

    def pack(way, first, last):
        (_, across_a, size_a), (_, across_b, size_b) = layout(k, way)
        reach_a, reach_b = [reaches(offset) for offset in OFFSETS[2 * way : 2 * way + 2]]

        def step(p, carry):
            in_a = p < size_a
            unit = jnp.where(in_a, p, jnp.maximum(p - size_a, 0))
            across = jnp.where(in_a, across_a, across_b)
            row = jnp.where(across == 3, lax.div(unit, 3), jnp.where(across == 2, lax.div(unit, 2), unit))
            col = jnp.clip(unit - row * across, 0, chunks - 1)
            row = jnp.clip(row, 0, width // UNIT - 1)
            used = p < size_a + size_b
            reach = [
                jnp.where(used, jnp.where(in_a, reach_a[q], reach_b[q]), 0) for q in range(slots)
            ]
            for part, value in enumerate(unit_sum(row, col, reach)):
                list_v[way, p, :, part * CHUNK : (part + 1) * CHUNK] = value.astype(BF16)
            return carry

        lax.fori_loop(first, last, step, 0, unroll=3)

    for table in tables:
        table.wait()
    for load in load_sigma:
        load.wait()
    load_green.start()
    for way in range(2):
        pack(way, DIRECT, LIST)
    greeted(peers)
    for h in range(2):
        for way in range(2):
            start(sends[way], spill[way][h])
    for way in range(2):
        pack(way, 0, 9)
        start(goes[way], direct[way][0])
    start(has_high, up)
    start(has_low, down)
    for way in range(2):
        pack(way, 9, DIRECT)

    for way in range(2):

        @pl.when(jnp.logical_not(comes[way]))
        def _():
            got_v[way][...] = jnp.zeros_like(got_v[way])
            cent_v[way] = jnp.zeros_like(cent_v[way])

        @pl.when(jnp.logical_not(gets[way]))
        def _():
            back_v[way][...] = jnp.zeros_like(back_v[way])

        @pl.when(jnp.logical_not(relays[way]))
        def _():
            spill_v[way] = jnp.zeros_like(spill_v[way])

    for there, slot in ((has_low, 0), (has_high, 1)):

        @pl.when(jnp.logical_not(there))
        def _():
            near_v[slot] = jnp.zeros_like(near_v[slot])

    sum_sides()
    load_green.wait()
    prepare(green_v, b_v, a_v, side_v)

    arrived(has_low, up)
    arrived(has_high, down)
    sum_own()

    def merge(way, h):
        arrived(relays[way], spill[way][h])
        for j in range(h * GROUP, (h + 1) * GROUP):
            list_v[way, SHARED + j] = list_v[way, SHARED + j] + spill_v[way, j]

    for way in range(2):
        merge(way, 0)
        start(goes[way], direct[way][1], direct[way][2])

    for at, partner in enumerate((0, 2)):
        for r in range(2):
            rows = slice(r * width // 2, (r + 1) * width // 2)
            these = slice(rows.start // UNIT, rows.stop // UNIT)
            x = None
            for c in range(chunks):
                term = dot(mine_v[at, these, c].reshape(width // 2, 2 * CHUNK), b_chunk(b_v, partner, c))
                x = term if x is None else x + term
            part_v[0, rows] = x if at == 0 else part_v[0, rows] + x
    for way in range(2):
        merge(way, 1)
        start(goes[way], direct[way][3], *centre[way])
    def hand_back(n, h):
        for way in range(2):
            arrived(comes[way], direct[way][n])
            start(hands[way], returned[way][h])

    hand_back(1, 0)
    for r in range(chunks):
        rows = slice(r * CHUNK, (r + 1) * CHUNK)
        x = part_v[0, rows]
        for c in range(chunks):
            x = x + dot(own_v[c, rows], b_chunk(b_v, 1, c))
        put(y_v, 0, x)
        term = dot(a_v[r], y_v[: 2 * CHUNK])
        acc_v[...] = term if r == 0 else acc_v[...] + term

    hand_back(3, 1)

    def multiply(way, source, first, last, down_n, across_n, before, partner, fresh, top=0):
        for m in range(top // UNIT, width // UNIT):
            for c in range(chunks):
                position = before + m * across_n + c
                there = (m < down_n) & (c < across_n) & (position >= first) & (position < last)
                keep = jnp.where(there, 1.0, 0.0).astype(BF16)
                position = jnp.clip(position - first, 0, last - first - 1)
                block_v[c, m * UNIT : (m + 1) * UNIT] = source[position] * keep
        for row in range(top, width, width // 2):
            rows = slice(row, row + width // 2)
            x = None
            for c in range(chunks):
                term = dot(block_v[c, rows], b_chunk(b_v, partner, c))
                x = term if x is None else x + term
            part_v[way, rows] = x if fresh else part_v[way, rows] + x

    blocks = [
        layout(jnp.maximum(k - 1, 0), 0),
        layout(jnp.minimum(k + 1, slabs - 1), 1),
    ]
    for way in range(2):
        (down_a, across_a, size_a), (down_b, across_b, _) = blocks[way]
        partner_a, partner_b = ((1, 2), (1, 0))[way]
        arrived(comes[way], direct[way][0], direct[way][2])
        multiply(way, got_v[way], 0, DIRECT, down_a, across_a, 0, partner_a, True)
        multiply(way, got_v[way], 0, DIRECT, down_b, across_b, size_a, partner_b, False)

    def late():
        for way in range(2):
            (_, _, size_a), (down_b, across_b, _) = blocks[way]
            arrived(gets[way], *returned[way])
            multiply(
                way, back_v[way], DIRECT, LIST, down_b, across_b, size_a, (2, 0)[way], False, width // 2
            )

    finish(
        centre,
        comes,
        lambda way, c, rows: cent_v[way, c, rows],
        late,
        b_v,
        side_v,
        y_v,
        part_v,
        acc_v,
        out_ref,
    )

    gone(has_high, up)
    gone(has_low, down)
    for way in range(2):
        gone(goes[way], *direct[way], *centre[way])
        gone(sends[way], *spill[way])
        gone(hands[way], *returned[way])


def solution(mesh):
    slabs, energies = mesh.shape["slab"], mesh.shape["energy"]

    def body(green, sigma, phonon, pair_off, pair_count, pair_range):
        width = green.shape[-1]
        slots = sigma.shape[2]
        chunks = width // CHUNK
        pieces = len(centre_plan(width))
        hbm = pl.BlockSpec(memory_space=pltpu.HBM)
        vmem = pl.BlockSpec(memory_space=pltpu.VMEM)
        split = (chunks, width, 2 * CHUNK)
        unit = (UNIT, 2 * CHUNK)
        operands = (pair_off.T, pair_count, pair_range.T, green, sigma, phonon)
        operands = [pltpu.with_memory_space_constraint(v, pltpu.HBM) for v in operands]
        taken = [
            pltpu.SMEM((slots, slabs), jnp.int32),
            pltpu.SMEM((slabs,), jnp.int32),
            pltpu.SMEM((slots, slabs), jnp.int32),
            pltpu.VMEM((3, 2, width, width), BF16),
        ]
        near = pltpu.VMEM((2, 2, width, width), BF16)
        factors = [
            pltpu.VMEM((3, 2 * width, 2 * width), BF16),
            pltpu.VMEM(split, BF16),
            pltpu.VMEM((width // LAST, width, 4 * LAST), BF16),
            pltpu.VMEM((4 * CHUNK, 2 * width), BF16),
            pltpu.VMEM((2, width, 2 * width), F32),
            pltpu.VMEM((width, 2 * width), F32),
            pltpu.SemaphoreType.DMA((4 + chunks * (width // UNIT),)),
            pltpu.SemaphoreType.DMA((2,)),
            pltpu.SemaphoreType.DMA((2,)),
        ]

        def flags(count):
            return [pltpu.SemaphoreType.DMA((2, count))] * 2

        def call(what, number, name, blocks, semaphores, *operands):
            return pl.pallas_call(
                functools.partial(what, slabs, energies),
                out_shape=jax.ShapeDtypeStruct((1, 1, 2, width, width), F32),
                in_specs=[hbm] * 6,
                out_specs=vmem,
                scratch_shapes=taken + blocks + factors + semaphores,
                compiler_params=pltpu.CompilerParams(
                    collective_id=number, has_side_effects=True, vmem_limit_bytes=48 * 1024 * 1024
                ),
                name=name,
            )(*operands)

        straight = functools.partial(
            call,
            straight_kernel,
            0,
            "straight",
            [
                pltpu.VMEM((slots, 2, width, width), BF16),
                near,
                pltpu.VMEM((5,) + split, BF16),
                pltpu.VMEM((2, 3) + split, BF16),
            ],
            flags(chunks + 1 + pieces),
        )
        around = functools.partial(
            call,
            around_kernel,
            1,
            "around",
            [
                pltpu.VMEM((width // UNIT, chunks, slots, 2, UNIT, CHUNK), BF16),
                near,
                pltpu.VMEM((2, width // UNIT, chunks) + unit, BF16),
                pltpu.VMEM(split, BF16),
                pltpu.VMEM((2, LIST) + unit, BF16),
                pltpu.VMEM((DIRECT,) + unit, BF16),
                pltpu.VMEM((DIRECT,) + unit, BF16),
                pltpu.VMEM((LIST - DIRECT,) + unit, BF16),
                pltpu.VMEM((LIST - DIRECT,) + unit, BF16),
                pltpu.VMEM((2, LIST - DIRECT) + unit, BF16),
                pltpu.VMEM((2,) + split, BF16),
                pltpu.VMEM(split, BF16),
            ],
            flags(4) + flags(2) + flags(2) + flags(pieces),
        )
        crowded = pl.pallas_call(
            crowded_kernel,
            out_shape=jax.ShapeDtypeStruct((1,), jnp.int32),
            in_specs=[vmem] * 3,
            out_specs=pl.BlockSpec(memory_space=pltpu.SMEM),
            name="crowded",
        )(pair_off.T, pair_count[None], pair_range.T)
        return lax.cond(crowded[0] > 0, straight, around, *operands)

    wide = P("energy", "slab", None, None, None, None)
    slim = P("energy", "slab", None, None, None)
    return jax.shard_map(
        body,
        mesh=mesh,
        in_specs=(wide, wide, slim, P(), P(), P()),
        out_specs=slim,
        check_vma=False,
    )
```

```python
import functools

import jax
import jax.numpy as jnp
from jax import lax
from jax.experimental import pallas as pl
from jax.experimental.pallas import tpu as pltpu
from jax.sharding import PartitionSpec as P

MESH = pl.DeviceIdType.MESH
F32 = jnp.float32
BF16 = jnp.bfloat16
TILE = 16
CHUNK = 128
LAST = 64
UNIT = 96
GROUP = 3
LIST = 24
DIRECT = 18
SHARED = 12
HOP = 4
OFFSETS = (1, 2, -1, -2)


def extent(reach):
    steps = [(reach >= n * UNIT).astype(jnp.int32) for n in range(1, 5)]
    down = steps[0] + steps[1] + steps[2] + steps[3]
    across = steps[0] + steps[1] + steps[2]
    return down, across, down * across


def turned(slab, way):
    place = lax.rem(slab, HOP)
    paired = jnp.where(lax.rem(lax.div(slab, HOP), 2) == 0, HOP, -HOP)
    if way == 0:
        return jnp.where(place == HOP - 1, -HOP, jnp.where(place == 1, paired, HOP))
    return jnp.where(place == 0, HOP, jnp.where(place == 2, paired, -HOP))


def detours(slab, way, slabs):
    low, high = (0, slabs - 2) if way == 0 else (1, slabs - 1)
    relay = slab + turned(slab, way)
    return (slab >= low) & (slab <= high) & (relay >= low) & (relay <= high)


def relayed(relay, way):
    turn = turned(relay, way)
    return relay + jnp.where(lax.rem(relay, HOP) == 1 + way, turn, -turn)


def crowded_kernel(off_ref, count_ref, range_ref, out_ref):
    off, reach = off_ref[...], range_ref[...]
    slots, slabs = off.shape
    live = lax.broadcasted_iota(jnp.int32, off.shape, 0) < count_ref[...]
    slab = lax.broadcasted_iota(jnp.int32, (1, slabs), 1)
    crowded = jnp.zeros((1, slabs), F32)
    for way in range(2):
        filled = jnp.zeros((1, slabs), jnp.int32)
        for offset in OFFSETS[2 * way : 2 * way + 2]:
            widest = jnp.max(jnp.where(live & (off == offset), reach, 0), axis=0, keepdims=True)
            filled = filled + extent(widest)[2]
        above = jnp.concatenate([filled[:, HOP:], filled[:, :HOP]], axis=1)
        below = jnp.concatenate([filled[:, -HOP:], filled[:, :-HOP]], axis=1)
        relay = jnp.where(turned(slab, way) > 0, above, below)
        room = jnp.where(filled > DIRECT + GROUP, SHARED, SHARED + GROUP)
        stuck = (relay > room) | jnp.logical_not(detours(slab, way, slabs))
        crowded = crowded + ((filled > DIRECT) & stuck).astype(F32)
    out_ref[0] = jnp.max(crowded).astype(jnp.int32)


def dot(a, b):
    return jnp.dot(a, b, preferred_element_type=F32)


def start(there, *copies):
    @pl.when(there)
    def _():
        for copy in copies:
            copy.start()


def arrived(there, *copies):
    @pl.when(there)
    def _():
        for copy in copies:
            copy.wait_recv()


def gone(there, *copies):
    @pl.when(there)
    def _():
        for copy in copies:
            copy.wait_send()


def greet(peers):
    barrier = pltpu.get_barrier_semaphore()
    for there, who in peers:

        @pl.when(there)
        def _():
            pl.semaphore_signal(barrier, inc=1, device_id=who, device_id_type=MESH)


def greeted(peers):
    barrier = pltpu.get_barrier_semaphore()
    pl.semaphore_wait(barrier, sum(there.astype(jnp.int32) for there, _ in peers))


def prepare(green_v, b_v, a_v, side_v):
    width = green_v.shape[-1]
    for at in range(3):
        for part in range(2):
            flipped = green_v[at, part].astype(F32).T
            plain = flipped.astype(BF16)
            minus = (-flipped).astype(BF16)
            for c in range(width // CHUNK):
                source = slice(c * CHUNK, (c + 1) * CHUNK)
                real = slice(2 * c * CHUNK, (2 * c + 1) * CHUNK)
                imag = slice((2 * c + 1) * CHUNK, (2 * c + 2) * CHUNK)
                if part == 0:
                    b_v[at, real, :width] = plain[source]
                    b_v[at, imag, width:] = plain[source]
                else:
                    b_v[at, real, width:] = minus[source]
                    b_v[at, imag, :width] = plain[source]
    for c in range(width // CHUNK):
        for part in range(2):
            a_v[c, :, part * CHUNK : (part + 1) * CHUNK] = green_v[1, part, :, c * CHUNK : (c + 1) * CHUNK]
    for h in range(width // LAST):
        for n, at in enumerate((0, 2)):
            side_v[h, :, 2 * n * LAST : 2 * (n + 1) * LAST] = jnp.concatenate(
                [green_v[at, part, :, h * LAST : (h + 1) * LAST] for part in range(2)], axis=1
            )


def b_chunk(b_v, at, c):
    return b_v[at, 2 * c * CHUNK : 2 * (c + 1) * CHUNK]


def put(y_v, at, x):
    rows, width = x.shape[0], x.shape[1] // 2
    real = x[:, :width].astype(BF16)
    imag = x[:, width:].astype(BF16)
    y_v[at : at + rows, :width] = real
    y_v[at : at + rows, width:] = imag
    y_v[at + rows : at + 2 * rows, :width] = -imag
    y_v[at + rows : at + 2 * rows, width:] = real


def centre_plan(width):
    whole, half, most = slice(None), width // 2, width - LAST
    plan = [(whole, 0, CHUNK), (whole, CHUNK, half - CHUNK), (whole, half, most - half)]
    return plan + [(slice(c, c + 1), most, LAST) for c in range(width // CHUNK)]


def finish(centre, comes, cent, late, b_v, side_v, y_v, part_v, acc_v, out_ref):
    width = acc_v.shape[0]
    chunks = width // CHUNK
    plan = centre_plan(width)
    for n, (these, row, count) in enumerate(plan):
        rows = slice(row, row + count)
        final = n == len(plan) - 1
        complete = these == slice(None) or final
        if row == width // 2:
            late()
        for way in range(2):
            arrived(comes[way], centre[way][n])
            x = part_v[way, rows]
            for c in range(chunks)[these]:
                x = x + dot(cent(way, c, rows), b_chunk(b_v, (0, 2)[way], c))
            if complete:
                for h in range(count // LAST):
                    put(y_v, 4 * h * LAST + 2 * way * LAST, x[h * LAST : (h + 1) * LAST])
            else:
                part_v[way, rows] = x
        if complete and not final:
            total = acc_v[...]
            for h in range(count // LAST):
                total = total + dot(side_v[row // LAST + h], y_v[4 * h * LAST : 4 * (h + 1) * LAST])
            acc_v[...] = total
    for m in range(chunks):
        rows = slice(m * CHUNK, (m + 1) * CHUNK)
        total = acc_v[rows] + dot(side_v[width // LAST - 1, rows], y_v[: 4 * LAST])
        for part in range(2):
            out_ref[0, 0, part, rows] = total[:, part * width : (part + 1) * width]


def straight_kernel(
    slabs,
    energies,
    off_hbm,
    count_hbm,
    range_hbm,
    green_hbm,
    sigma_hbm,
    phonon_hbm,
    out_ref,
    off_ref,
    count_ref,
    range_ref,
    green_v,
    sigma_v,
    near_v,
    mine_v,
    got_v,
    b_v,
    a_v,
    side_v,
    y_v,
    part_v,
    acc_v,
    local_sem,
    near_send,
    near_recv,
    send_sem,
    recv_sem,
):
    k = lax.axis_index("slab")
    e = lax.axis_index("energy")
    width = green_v.shape[-1]
    slots = sigma_v.shape[0]
    chunks = width // CHUNK
    has_low, has_high = e > 0, e < energies - 1
    has_left, has_right = k > 0, k < slabs - 1
    goes, comes = (has_right, has_left), (has_left, has_right)

    tables = [
        pltpu.make_async_copy(source, held, local_sem.at[n])
        for n, (source, held) in enumerate(
            ((off_hbm, off_ref), (count_hbm, count_ref), (range_hbm, range_ref))
        )
    ]
    load_sigma = []
    for c in range(chunks):
        rows = slice(c * CHUNK, (c + 1) * CHUNK)
        load_sigma.append(
            pltpu.make_async_copy(
                sigma_hbm.at[0, 0, :, :, rows], sigma_v.at[:, :, rows], local_sem.at[4 + c]
            )
        )
    load_green = pltpu.make_async_copy(green_hbm.at[0, 0], green_v, local_sem.at[3])

    peers = (
        (has_left, {"slab": k - 1}),
        (has_right, {"slab": k + 1}),
        (has_low, {"energy": e - 1}),
        (has_high, {"energy": e + 1}),
    )
    greet(peers)
    for table in tables:
        table.start()
    for load in load_sigma:
        load.start()

    def near_copy(slot, target):
        return pltpu.make_async_remote_copy(
            src_ref=phonon_hbm.at[0, 0],
            dst_ref=near_v.at[slot],
            send_sem=near_send.at[slot],
            recv_sem=near_recv.at[slot],
            device_id={"energy": target},
            device_id_type=MESH,
        )

    up, down = near_copy(0, e + 1), near_copy(1, e - 1)

    whole = slice(None)
    plan = [(0, whole, c * CHUNK, CHUNK) for c in range(chunks)]
    plan += [(1, whole, 0, width)]
    first_centre = len(plan)
    plan += [(2,) + piece for piece in centre_plan(width)]
    sent = [[], []]
    for way in range(2):
        for n, (slot, these, row, count) in enumerate(plan):
            source = 4 if slot == 2 else 2 * way + slot
            sent[way].append(
                pltpu.make_async_remote_copy(
                    src_ref=mine_v.at[source, these, row : row + count],
                    dst_ref=got_v.at[way, slot, these, row : row + count],
                    send_sem=send_sem.at[way, n],
                    recv_sem=recv_sem.at[way, n],
                    device_id={"slab": (k + 1, k - 1)[way]},
                    device_id_type=MESH,
                )
            )

    def combine(at, offset, with_phonon, first=0, last=width // TILE):
        reach = []
        for q in range(slots):
            live = (q < count_ref[k]) & (off_ref[q, k] == offset)
            reach.append(jnp.where(live, range_ref[q, k], 0))

        def step(t, carry):
            rows = pl.ds(pl.multiple_of(t * TILE, TILE), TILE)
            col_ids = lax.broadcasted_iota(jnp.int32, (TILE, width), 1)
            inside = [col_ids < jnp.where(t * TILE < reach[q], reach[q], 0) for q in range(slots)]
            for part in range(2):
                kept = [
                    jnp.where(inside[q], sigma_v[q, part, rows, :].astype(F32), 0.0) for q in range(slots)
                ]
                total = functools.reduce(jnp.add, kept)
                if with_phonon:
                    low = near_v[0, part, rows, :].astype(F32)
                    high = near_v[1, part, rows, :].astype(F32)
                    total = total + (0.5 * (low + high)).astype(BF16).astype(F32)
                total = total.astype(BF16)
                for c in range(chunks):
                    mine_v[at, c, rows, part * CHUNK : (part + 1) * CHUNK] = total[
                        :, c * CHUNK : (c + 1) * CHUNK
                    ]
            return carry

        lax.fori_loop(first, last, step, 0, unroll=4)

    for table in tables:
        table.wait()
    tiles = CHUNK // TILE
    for c in range(chunks):
        load_sigma[c].wait()
        for way in range(2):
            combine(2 * way, (1, -1)[way], False, c * tiles, (c + 1) * tiles)
            if c == 0 and way == 0:
                greeted(peers)
            start(goes[way], sent[way][c])
        if c == 0:
            start(has_high, up)
            start(has_low, down)
    load_green.start()
    for way in range(2):
        combine(2 * way + 1, (2, -2)[way], False)
        start(goes[way], sent[way][chunks])

    for way in range(2):

        @pl.when(jnp.logical_not(comes[way]))
        def _():
            got_v[way] = jnp.zeros_like(got_v[way])

    for there, slot in ((has_low, 0), (has_high, 1)):

        @pl.when(jnp.logical_not(there))
        def _():
            near_v[slot] = jnp.zeros_like(near_v[slot])

    load_green.wait()
    prepare(green_v, b_v, a_v, side_v)

    arrived(has_low, up)
    arrived(has_high, down)
    combine(4, 0, True)
    for way in range(2):
        start(goes[way], *sent[way][first_centre:])

    for r in range(chunks):
        rows = slice(r * CHUNK, (r + 1) * CHUNK)
        x = None
        for at, partner in ((2, 0), (4, 1), (0, 2)):
            for c in range(chunks):
                term = dot(mine_v[at, c, rows], b_chunk(b_v, partner, c))
                x = term if x is None else x + term
        put(y_v, 0, x)
        term = dot(a_v[r], y_v[: 2 * CHUNK])
        acc_v[...] = term if r == 0 else acc_v[...] + term

    for slot in range(2):
        for way in range(2):
            arrived(comes[way], *sent[way][chunks * slot : chunks + slot])
            partner = ((1, 2), (1, 0))[way][slot]
            for r in range(chunks):
                rows = slice(r * CHUNK, (r + 1) * CHUNK)
                x = None
                for c in range(chunks):
                    term = dot(got_v[way, slot, c, rows], b_chunk(b_v, partner, c))
                    x = term if x is None else x + term
                part_v[way, rows] = x if slot == 0 else part_v[way, rows] + x
    centre = [copies[first_centre:] for copies in sent]
    finish(
        centre,
        comes,
        lambda way, c, rows: got_v[way, 2, c, rows],
        lambda: None,
        b_v,
        side_v,
        y_v,
        part_v,
        acc_v,
        out_ref,
    )

    gone(has_high, up)
    gone(has_low, down)
    gone(has_right, *sent[0])
    gone(has_left, *sent[1])


def around_kernel(
    slabs,
    energies,
    off_hbm,
    count_hbm,
    range_hbm,
    green_hbm,
    sigma_hbm,
    phonon_hbm,
    out_ref,
    off_ref,
    count_ref,
    range_ref,
    green_v,
    sigma_v,
    near_v,
    mine_v,
    own_v,
    list_v,
    from_left_v,
    from_right_v,
    back_left_v,
    back_right_v,
    spill_v,
    cent_v,
    block_v,
    b_v,
    a_v,
    side_v,
    y_v,
    part_v,
    acc_v,
    local_sem,
    near_send,
    near_recv,
    unit_send,
    unit_recv,
    spill_send,
    spill_recv,
    back_send,
    back_recv,
    cent_send,
    cent_recv,
):
    k = lax.axis_index("slab")
    e = lax.axis_index("energy")
    width = green_v.shape[-1]
    slots = sigma_v.shape[2]
    chunks = width // CHUNK
    has_low, has_high = e > 0, e < energies - 1

    has_left, has_right = k > 0, k < slabs - 1

    tables = [
        pltpu.make_async_copy(source, held, local_sem.at[n])
        for n, (source, held) in enumerate(
            ((off_hbm, off_ref), (count_hbm, count_ref), (range_hbm, range_ref))
        )
    ]
    load_sigma = []
    for m in range(width // UNIT):
        for c in range(chunks):
            rows, columns = slice(m * UNIT, (m + 1) * UNIT), slice(c * CHUNK, (c + 1) * CHUNK)
            load_sigma.append(
                pltpu.make_async_copy(
                    sigma_hbm.at[0, 0, :, :, rows, columns],
                    sigma_v.at[m, c],
                    local_sem.at[4 + len(load_sigma)],
                )
            )
    load_green = pltpu.make_async_copy(green_hbm.at[0, 0], green_v, local_sem.at[3])
    peers = (
        (has_left, {"slab": k - 1}),
        (has_right, {"slab": k + 1}),
        (has_low, {"energy": e - 1}),
        (has_high, {"energy": e + 1}),
        (k >= HOP, {"slab": k - HOP}),
        (k < slabs - HOP, {"slab": k + HOP}),
    )
    greet(peers)
    for table in tables:
        table.start()
    for load in load_sigma:
        load.start()

    def near_copy(slot, target):
        return pltpu.make_async_remote_copy(
            src_ref=phonon_hbm.at[0, 0],
            dst_ref=near_v.at[slot],
            send_sem=near_send.at[slot],
            recv_sem=near_recv.at[slot],
            device_id={"energy": target},
            device_id_type=MESH,
        )

    up, down = near_copy(0, e + 1), near_copy(1, e - 1)

    def remote(source, target, sent, received, slab):
        return pltpu.make_async_remote_copy(
            src_ref=source,
            dst_ref=target,
            send_sem=sent,
            recv_sem=received,
            device_id={"slab": slab},
            device_id_type=MESH,
        )

    sends = [detours(k, way, slabs) for way in range(2)]
    rides = [relayed(k, way) for way in range(2)]
    relays = [detours(rides[way], way, slabs) for way in range(2)]
    handed = [relayed(k + step, way) for way, step in ((0, -1), (1, 1))]
    hands = [there & detours(handed[way], way, slabs) for way, there in enumerate((has_left, has_right))]
    gets = [there & detours(k + step, way, slabs) for way, (there, step) in enumerate(((has_left, -1), (has_right, 1)))]
    beside = (k + 1, k - 1)
    goes, comes = (has_right, has_left), (has_left, has_right)
    got_v, back_v = (from_left_v, from_right_v), (back_left_v, back_right_v)
    units = (slice(0, 9), slice(12, 15), slice(9, 12), slice(15, 18))
    halves = (slice(0, GROUP), slice(GROUP, 2 * GROUP))
    direct, spill, returned, centre = [[], []], [[], []], [[], []], [[], []]
    for way in range(2):
        for n, these in enumerate(units):
            direct[way].append(
                remote(
                    list_v.at[way, these],
                    got_v[way].at[these],
                    unit_send.at[way, n],
                    unit_recv.at[way, n],
                    beside[way],
                )
            )
        for h, these in enumerate(halves):
            spill[way].append(
                remote(
                    list_v.at[way, LIST - (h + 1) * GROUP : LIST - h * GROUP],
                    spill_v.at[way, these],
                    spill_send.at[way, h],
                    spill_recv.at[way, h],
                    k + turned(k, way),
                )
            )
            returned[way].append(
                remote(
                    got_v[way].at[SHARED + h * GROUP : SHARED + (h + 1) * GROUP],
                    back_v[way].at[halves[1 - h]],
                    back_send.at[way, h],
                    back_recv.at[way, h],
                    handed[way] + (1, -1)[way],
                )
            )
        for n, (these, row, count) in enumerate(centre_plan(width)):
            centre[way].append(
                remote(
                    own_v.at[these, row : row + count],
                    cent_v.at[way, these, row : row + count],
                    cent_send.at[way, n],
                    cent_recv.at[way, n],
                    beside[way],
                )
            )

    def live_reach(slab, q, offset):
        live = (q < count_ref[slab]) & (off_ref[q, slab] == offset)
        return jnp.where(live, range_ref[q, slab], 0)

    def unit_sum(m, c, reach):
        column = c * CHUNK + lax.broadcasted_iota(jnp.int32, (UNIT, CHUNK), 1)
        inside = [column < jnp.where(m * UNIT < reach[q], reach[q], 0) for q in range(slots)]
        return [
            functools.reduce(
                jnp.add,
                [jnp.where(inside[q], sigma_v[m, c, q, part].astype(F32), 0.0) for q in range(slots)],
            )
            for part in range(2)
        ]

    def reaches(offset):
        return [live_reach(k, q, offset) for q in range(slots)]

    def sum_sides():
        wanted = [reaches(-1), reaches(1)]

        def step(m, carry):
            for c in range(chunks):
                for at in range(2):
                    for part, value in enumerate(unit_sum(m, c, wanted[at])):
                        mine_v[at, m, c, :, part * CHUNK : (part + 1) * CHUNK] = value.astype(BF16)
            return carry

        lax.fori_loop(0, width // UNIT, step, 0)

    def sum_own():
        reach = reaches(0)

        def step(m, carry):
            rows = pl.ds(pl.multiple_of(m * UNIT, UNIT), UNIT)
            for c in range(chunks):
                columns = slice(c * CHUNK, (c + 1) * CHUNK)
                for part, value in enumerate(unit_sum(m, c, reach)):
                    low = near_v[0, part, rows, columns].astype(F32)
                    high = near_v[1, part, rows, columns].astype(F32)
                    value = value + (0.5 * (low + high)).astype(BF16).astype(F32)
                    own_v[c, rows, part * CHUNK : (part + 1) * CHUNK] = value.astype(BF16)
            return carry

        lax.fori_loop(0, width // UNIT, step, 0)

    def layout(slab, way):
        blocks = []
        for offset in OFFSETS[2 * way : 2 * way + 2]:
            reach = functools.reduce(jnp.maximum, [live_reach(slab, q, offset) for q in range(slots)])
            blocks.append(extent(reach))
        return blocks

    def pack(way, first, last):
        (_, across_a, size_a), (_, across_b, size_b) = layout(k, way)
        reach_a, reach_b = [reaches(offset) for offset in OFFSETS[2 * way : 2 * way + 2]]

        def step(p, carry):
            in_a = p < size_a
            unit = jnp.where(in_a, p, jnp.maximum(p - size_a, 0))
            across = jnp.where(in_a, across_a, across_b)
            row = jnp.where(across == 3, lax.div(unit, 3), jnp.where(across == 2, lax.div(unit, 2), unit))
            col = jnp.clip(unit - row * across, 0, chunks - 1)
            row = jnp.clip(row, 0, width // UNIT - 1)
            used = p < size_a + size_b
            reach = [
                jnp.where(used, jnp.where(in_a, reach_a[q], reach_b[q]), 0) for q in range(slots)
            ]
            for part, value in enumerate(unit_sum(row, col, reach)):
                list_v[way, p, :, part * CHUNK : (part + 1) * CHUNK] = value.astype(BF16)
            return carry

        lax.fori_loop(first, last, step, 0, unroll=3)

    for table in tables:
        table.wait()
    for load in load_sigma:
        load.wait()
    load_green.start()
    for way in range(2):
        pack(way, DIRECT, LIST)
    greeted(peers)
    for h in range(2):
        for way in range(2):
            start(sends[way], spill[way][h])
    for way in range(2):
        pack(way, 0, 9)
        start(goes[way], direct[way][0])
    start(has_high, up)
    start(has_low, down)
    for way in range(2):
        pack(way, 9, DIRECT)

    for way in range(2):

        @pl.when(jnp.logical_not(comes[way]))
        def _():
            got_v[way][...] = jnp.zeros_like(got_v[way])
            cent_v[way] = jnp.zeros_like(cent_v[way])

        @pl.when(jnp.logical_not(gets[way]))
        def _():
            back_v[way][...] = jnp.zeros_like(back_v[way])

        @pl.when(jnp.logical_not(relays[way]))
        def _():
            spill_v[way] = jnp.zeros_like(spill_v[way])

    for there, slot in ((has_low, 0), (has_high, 1)):

        @pl.when(jnp.logical_not(there))
        def _():
            near_v[slot] = jnp.zeros_like(near_v[slot])

    sum_sides()
    load_green.wait()
    prepare(green_v, b_v, a_v, side_v)

    arrived(has_low, up)
    arrived(has_high, down)
    sum_own()

    def merge(way, h):
        arrived(relays[way], spill[way][h])
        for j in range(h * GROUP, (h + 1) * GROUP):
            list_v[way, SHARED + j] = list_v[way, SHARED + j] + spill_v[way, j]

    for way in range(2):
        merge(way, 0)
        start(goes[way], direct[way][1], direct[way][2])

    for at, partner in enumerate((0, 2)):
        for r in range(2):
            rows = slice(r * width // 2, (r + 1) * width // 2)
            these = slice(rows.start // UNIT, rows.stop // UNIT)
            x = None
            for c in range(chunks):
                term = dot(mine_v[at, these, c].reshape(width // 2, 2 * CHUNK), b_chunk(b_v, partner, c))
                x = term if x is None else x + term
            part_v[0, rows] = x if at == 0 else part_v[0, rows] + x
    for way in range(2):
        merge(way, 1)
        start(goes[way], direct[way][3], *centre[way])
    def hand_back(way, n, h):
        arrived(comes[way], direct[way][n])
        start(hands[way], returned[way][h])

    for way in range(2):
        hand_back(way, 1, 0)
    for r in range(chunks):
        rows = slice(r * CHUNK, (r + 1) * CHUNK)
        x = part_v[0, rows]
        for c in range(chunks):
            x = x + dot(own_v[c, rows], b_chunk(b_v, 1, c))
        put(y_v, 0, x)
        term = dot(a_v[r], y_v[: 2 * CHUNK])
        acc_v[...] = term if r == 0 else acc_v[...] + term


    def multiply(way, source, first, last, down_n, across_n, before, partner, fresh, top=0):
        for m in range(top // UNIT, width // UNIT):
            for c in range(chunks):
                position = before + m * across_n + c
                there = (m < down_n) & (c < across_n) & (position >= first) & (position < last)
                keep = jnp.where(there, 1.0, 0.0).astype(BF16)
                position = jnp.clip(position - first, 0, last - first - 1)
                block_v[c, m * UNIT : (m + 1) * UNIT] = source[position] * keep
        for row in range(top, width, width // 2):
            rows = slice(row, row + width // 2)
            x = None
            for c in range(chunks):
                term = dot(block_v[c, rows], b_chunk(b_v, partner, c))
                x = term if x is None else x + term
            part_v[way, rows] = x if fresh else part_v[way, rows] + x

    blocks = [
        layout(jnp.maximum(k - 1, 0), 0),
        layout(jnp.minimum(k + 1, slabs - 1), 1),
    ]
    first_row = lax.rem(k, HOP) == 0
    for order, here in (((1, 0), first_row), ((0, 1), jnp.logical_not(first_row))):

        @pl.when(here)
        def _():
            for way in order:
                (down_a, across_a, size_a), (down_b, across_b, _) = blocks[way]
                partner_a, partner_b = ((1, 2), (1, 0))[way]
                hand_back(way, 3, 1)
                arrived(comes[way], direct[way][0], direct[way][2])
                multiply(way, got_v[way], 0, DIRECT, down_a, across_a, 0, partner_a, True)
                multiply(way, got_v[way], 0, DIRECT, down_b, across_b, size_a, partner_b, False)


    def late():
        for way in range(2):
            (_, _, size_a), (down_b, across_b, _) = blocks[way]
            arrived(gets[way], *returned[way])
            multiply(
                way, back_v[way], DIRECT, LIST, down_b, across_b, size_a, (2, 0)[way], False, width // 2
            )

    finish(
        centre,
        comes,
        lambda way, c, rows: cent_v[way, c, rows],
        late,
        b_v,
        side_v,
        y_v,
        part_v,
        acc_v,
        out_ref,
    )

    gone(has_high, up)
    gone(has_low, down)
    for way in range(2):
        gone(goes[way], *direct[way], *centre[way])
        gone(sends[way], *spill[way])
        gone(hands[way], *returned[way])


def solution(mesh):
    slabs, energies = mesh.shape["slab"], mesh.shape["energy"]

    def body(green, sigma, phonon, pair_off, pair_count, pair_range):
        width = green.shape[-1]
        slots = sigma.shape[2]
        chunks = width // CHUNK
        pieces = len(centre_plan(width))
        hbm = pl.BlockSpec(memory_space=pltpu.HBM)
        vmem = pl.BlockSpec(memory_space=pltpu.VMEM)
        split = (chunks, width, 2 * CHUNK)
        unit = (UNIT, 2 * CHUNK)
        operands = (pair_off.T, pair_count, pair_range.T, green, sigma, phonon)
        operands = [pltpu.with_memory_space_constraint(v, pltpu.HBM) for v in operands]
        taken = [
            pltpu.SMEM((slots, slabs), jnp.int32),
            pltpu.SMEM((slabs,), jnp.int32),
            pltpu.SMEM((slots, slabs), jnp.int32),
            pltpu.VMEM((3, 2, width, width), BF16),
        ]
        near = pltpu.VMEM((2, 2, width, width), BF16)
        factors = [
            pltpu.VMEM((3, 2 * width, 2 * width), BF16),
            pltpu.VMEM(split, BF16),
            pltpu.VMEM((width // LAST, width, 4 * LAST), BF16),
            pltpu.VMEM((4 * CHUNK, 2 * width), BF16),
            pltpu.VMEM((2, width, 2 * width), F32),
            pltpu.VMEM((width, 2 * width), F32),
            pltpu.SemaphoreType.DMA((4 + chunks * (width // UNIT),)),
            pltpu.SemaphoreType.DMA((2,)),
            pltpu.SemaphoreType.DMA((2,)),
        ]

        def flags(count):
            return [pltpu.SemaphoreType.DMA((2, count))] * 2

        def call(what, number, name, blocks, semaphores, *operands):
            return pl.pallas_call(
                functools.partial(what, slabs, energies),
                out_shape=jax.ShapeDtypeStruct((1, 1, 2, width, width), F32),
                in_specs=[hbm] * 6,
                out_specs=vmem,
                scratch_shapes=taken + blocks + factors + semaphores,
                compiler_params=pltpu.CompilerParams(
                    collective_id=number, has_side_effects=True, vmem_limit_bytes=48 * 1024 * 1024
                ),
                name=name,
            )(*operands)

        straight = functools.partial(
            call,
            straight_kernel,
            0,
            "straight",
            [
                pltpu.VMEM((slots, 2, width, width), BF16),
                near,
                pltpu.VMEM((5,) + split, BF16),
                pltpu.VMEM((2, 3) + split, BF16),
            ],
            flags(chunks + 1 + pieces),
        )
        around = functools.partial(
            call,
            around_kernel,
            1,
            "around",
            [
                pltpu.VMEM((width // UNIT, chunks, slots, 2, UNIT, CHUNK), BF16),
                near,
                pltpu.VMEM((2, width // UNIT, chunks) + unit, BF16),
                pltpu.VMEM(split, BF16),
                pltpu.VMEM((2, LIST) + unit, BF16),
                pltpu.VMEM((DIRECT,) + unit, BF16),
                pltpu.VMEM((DIRECT,) + unit, BF16),
                pltpu.VMEM((LIST - DIRECT,) + unit, BF16),
                pltpu.VMEM((LIST - DIRECT,) + unit, BF16),
                pltpu.VMEM((2, LIST - DIRECT) + unit, BF16),
                pltpu.VMEM((2,) + split, BF16),
                pltpu.VMEM(split, BF16),
            ],
            flags(4) + flags(2) + flags(2) + flags(pieces),
        )
        crowded = pl.pallas_call(
            crowded_kernel,
            out_shape=jax.ShapeDtypeStruct((1,), jnp.int32),
            in_specs=[vmem] * 3,
            out_specs=pl.BlockSpec(memory_space=pltpu.SMEM),
            name="crowded",
        )(pair_off.T, pair_count[None], pair_range.T)
        return lax.cond(crowded[0] > 0, straight, around, *operands)

    wide = P("energy", "slab", None, None, None, None)
    slim = P("energy", "slab", None, None, None)
    return jax.shard_map(
        body,
        mesh=mesh,
        in_specs=(wide, wide, slim, P(), P(), P()),
        out_specs=slim,
        check_vma=False,
    )
```
